8 devices in a mesh: ey: 4 (over z, y, x), ex: 2 (over core).
Axes of the slice: x: 2, y: 2, z: 1, core: 2. Of those that a mesh axis runs over, the one named last changes fastest.
Arguments:
- x: bfloat16 [512, 2048], P(('ey', 'ex'))
- kv_k: bfloat16 [512, 256, 4, 128], P(('ey', 'ex'))
- kv_v: bfloat16 [512, 256, 4, 128], P(('ey', 'ex'))
- lens: int32 [512], P(('ey', 'ex'))
- topk_idx: int32 [512, 8], P(('ey', 'ex'))
- gates: float32 [512, 8], P(('ey', 'ex'))
- ln1: bfloat16 [2048], replicated
- wq: bfloat16 [2048, 4096], replicated
- wo: bfloat16 [4096, 2048], replicated
- ln2: bfloat16 [2048], replicated
- ws1: bfloat16 [2048, 768], replicated
- ws3: bfloat16 [2048, 768], replicated
- ws2: bfloat16 [768, 2048], replicated
- w1: bfloat16 [128, 2048, 768], P(('ey', 'ex'))
- w3: bfloat16 [128, 2048, 768], P(('ey', 'ex'))
- w2: bfloat16 [128, 768, 2048], P(('ey', 'ex'))
Outputs:
- output: bfloat16 [512, 2048], P(('ey', 'ex'))
All inputs are finite; a program needn't handle non-finite values.
Results may differ from the reference program's by a relative error of at most 0.0116285.
Values are sent between devices in bfloat16 or wider.
A program may use at most 1 GiB of HBM per device.

```python
import jax
import jax.numpy as jnp
from jax import lax

DEVICES = 8
B_DEV = 64
L = 256
D = 2048
HEADS = 32
KV_HEADS = 4
HEAD = 128
F = 768
FS = 768
E = 128
TOP = 8
EPS = 1e-6
B = DEVICES * B_DEV
E_DEV = E // DEVICES
CAP = B_DEV - B_DEV // 8
GROUP = HEADS // KV_HEADS


def _normal(key, shape, scale):
    return (scale * jax.random.normal(key, shape, jnp.float32)).astype(jnp.bfloat16)


def _route_ids(key):
    expert_ids = jnp.arange(E)
    cold_dev = (expert_ids >= 2 * E_DEV) & (expert_ids < 3 * E_DEV)
    weight = jnp.where(expert_ids >= E - 2, 1, jnp.where(cold_dev, E * 37 // 5, E)).astype(jnp.uint32)
    arrival = (jax.random.bits(key, (B, E), jnp.uint32) >> 12) * weight[None, :]
    return jnp.argsort(arrival, axis=-1)[:, :TOP].astype(jnp.int32)


def setup_inputs(seed: int = 0) -> dict:
    ks = jax.random.split(jax.random.PRNGKey(seed), 16)
    dk = jax.random.split(jax.random.fold_in(jax.random.PRNGKey(seed), 7), 3)
    dev = jnp.arange(B) // B_DEV
    far = (dev % 4) == 0
    far_len = jax.random.randint(dk[0], (B,), 3 * L // 4, L, jnp.int32)
    near_len = jax.random.randint(dk[1], (B,), 0, L // 16, jnp.int32)
    lens = jnp.clip(jnp.where(far, far_len, near_len), 1, L).astype(jnp.int32)
    topk_idx = _route_ids(dk[2])
    gates = 2.5 * jax.nn.softmax(0.5 * jax.random.normal(ks[5], (B, TOP), jnp.float32), axis=-1)
    return {
        "x": _normal(ks[0], (B, D), 1.0),
        "kv_k": _normal(ks[1], (B, L, KV_HEADS, HEAD), 2.0),
        "kv_v": _normal(ks[2], (B, L, KV_HEADS, HEAD), 1.0),
        "lens": lens,
        "topk_idx": topk_idx.astype(jnp.int32),
        "gates": gates,
        "ln1": (1.0 + 0.1 * jax.random.normal(ks[6], (D,), jnp.float32)).astype(jnp.bfloat16),
        "wq": _normal(ks[7], (D, HEADS * HEAD), D ** -0.5),
        "wo": _normal(ks[8], (HEADS * HEAD, D), (HEADS * HEAD) ** -0.5),
        "ln2": (1.0 + 0.1 * jax.random.normal(ks[9], (D,), jnp.float32)).astype(jnp.bfloat16),
        "ws1": _normal(ks[10], (D, FS), D ** -0.5),
        "ws3": _normal(ks[11], (D, FS), D ** -0.5),
        "ws2": _normal(ks[12], (FS, D), FS ** -0.5),
        "w1": _normal(ks[13], (E, D, F), D ** -0.5),
        "w3": _normal(ks[14], (E, D, F), D ** -0.5),
        "w2": _normal(ks[15], (E, F, D), F ** -0.5),
    }


def _rms(v, w):
    v32 = v.astype(jnp.float32)
    r = lax.rsqrt(jnp.mean(v32 * v32, axis=-1, keepdims=True) + EPS)
    return (v32 * r * w.astype(jnp.float32)).astype(jnp.bfloat16)


def _swiglu(a, w1, w3, w2):
    z1 = jnp.dot(a, w1, preferred_element_type=jnp.float32)
    z3 = jnp.dot(a, w3, preferred_element_type=jnp.float32)
    g = (jax.nn.silu(z1) * z3).astype(jnp.bfloat16)
    return jnp.dot(g, w2, preferred_element_type=jnp.float32)


def _attend(args):
    q, k, v, n = args
    s = jnp.einsum("kgh,lkh->kgl", q.astype(jnp.float32), k.astype(jnp.float32)) * HEAD ** -0.5
    s = jnp.where(jnp.arange(L) < n, s, -jnp.inf)
    p = jax.nn.softmax(s, axis=-1).astype(jnp.bfloat16)
    return jnp.einsum("kgl,lkh->kgh", p.astype(jnp.float32), v.astype(jnp.float32)).astype(jnp.bfloat16)


def reference(x, kv_k, kv_v, lens, topk_idx, gates, ln1, wq, wo, ln2, ws1, ws3, ws2, w1, w3, w2):
    a = _rms(x, ln1)
    q = jnp.dot(a, wq, preferred_element_type=jnp.float32).astype(jnp.bfloat16)
    o = lax.map(_attend, (q.reshape(B, KV_HEADS, GROUP, HEAD), kv_k, kv_v, lens))
    attn = jnp.dot(o.reshape(B, HEADS * HEAD), wo, preferred_element_type=jnp.float32)
    h = (x.astype(jnp.float32) + attn).astype(jnp.bfloat16)
    u = _rms(h, ln2)
    shared = _swiglu(u, ws1, ws3, ws2)
    blk = topk_idx.reshape(DEVICES, B_DEV * TOP)
    oh = jax.nn.one_hot(blk, E, dtype=jnp.int32)
    rank = jnp.sum((jnp.cumsum(oh, axis=1) - oh) * oh, axis=-1)
    src = jnp.arange(DEVICES)[:, None]
    slot = jnp.where(rank < CAP, (blk * DEVICES + src) * CAP + rank, E * DEVICES * CAP).reshape(-1)
    tok = jnp.arange(B * TOP) // TOP
    tok_buf = jnp.full((E * DEVICES * CAP,), B, jnp.int32).at[slot].set(tok, mode="drop")
    gate_buf = jnp.zeros((E * DEVICES * CAP,), jnp.float32).at[slot].set(gates.reshape(-1), mode="drop")

    def expert(acc, xs):
        t, g, e1, e3, e2 = xs
        rows = jnp.take(u, t, axis=0, mode="fill", fill_value=0)
        out = _swiglu(rows, e1, e3, e2).astype(jnp.bfloat16).astype(jnp.float32)
        return acc.at[t].add(g[:, None] * out, mode="drop"), None

    routed, _ = lax.scan(expert, jnp.zeros((B, D), jnp.float32),
                         (tok_buf.reshape(E, DEVICES * CAP), gate_buf.reshape(E, DEVICES * CAP), w1, w3, w2))
    return (h.astype(jnp.float32) + shared + routed).astype(jnp.bfloat16)
```

```python
import functools

import jax
import jax.numpy as jnp
from jax import lax
from jax.experimental import pallas as pl
from jax.experimental.pallas import tpu as pltpu
from jax.sharding import PartitionSpec as P

EPS = 1e-6
GRP = ("ey", "ex")
MESH = pl.DeviceIdType.MESH
NEG = -1e30
F32 = jnp.float32
BF16 = jnp.bfloat16
VLIM = 62 * 1024 * 1024


def _vm():
    return pl.BlockSpec(memory_space=pltpu.VMEM)


def _sm():
    return pl.BlockSpec(memory_space=pltpu.SMEM)


def _any():
    return pl.BlockSpec(memory_space=pl.ANY)


def _rms(v, w):
    v32 = v.astype(F32)
    r = lax.rsqrt(jnp.mean(v32 * v32, axis=-1, keepdims=True) + EPS)
    return (v32 * r * w.astype(F32)).astype(BF16)


SEQ = 4
KVBUF = 6
STEP = 64


def _attn_kernel(lens, x, ln1, ln2, idx, gates, kk, vv, wq, wo, h_out, u_out, pk_out,
                 wqb, wob, kb, vb, qs, os, ob, bias, hf, wq_sem, wo_sem, k_sem, v_sem):
    b, d = x.shape
    heads_dim = wqb.shape[1]
    hd = 128
    nh = heads_dim // hd
    rows = kk.shape[1]
    kvh = 4
    seqlen = rows // kvh
    ncls = seqlen // STEP
    crow = STEP * kvh
    ngrp = b // SEQ
    nwq = wq_sem.shape[0]
    nwo = wo_sem.shape[0]
    cq = heads_dim // nwq
    co = d // nwo

    def wq_copy(i):
        c = pl.ds(pl.multiple_of(i * cq, cq), cq)
        return pltpu.make_async_copy(wq.at[:, c], wqb.at[:, c], wq_sem.at[i])

    def wo_copy(i):
        c = pl.ds(pl.multiple_of(i * co, co), co)
        return pltpu.make_async_copy(wo.at[:, c], wob.at[:, c], wo_sem.at[i])

    def gmax(g):
        m = lens[g * SEQ]
        for s in range(1, SEQ):
            m = jnp.maximum(m, lens[g * SEQ + s])
        return m

    def kv_copies(g, slot, n):
        src = (pl.ds(g * SEQ, SEQ), pl.ds(0, n * crow))
        dst = (slot, slice(None), pl.ds(0, n * crow))
        return (pltpu.make_async_copy(kk.at[src], kb.at[dst], k_sem.at[slot]),
                pltpu.make_async_copy(vv.at[src], vb.at[dst], v_sem.at[slot]))

    def by_class(g, f):
        cls = (gmax(g) + STEP - 1) // STEP
        for n in range(1, ncls + 1):
            pl.when(cls == n)(functools.partial(f, n))

    def start_kv(g):
        slot = lax.rem(g, KVBUF)

        def go(n):
            for c in kv_copies(g, slot, n):
                c.start()
        by_class(g, go)

    for i in range(nwq):
        wq_copy(i).start()
    lax.fori_loop(0, min(KVBUF, ngrp), lambda g, _: (start_kv(g), 0)[1], 0)
    for i in range(nwo // 2):
        wo_copy(i).start()

    pk_out[...] = jnp.concatenate(
        [idx[...].astype(F32), gates[...], jnp.zeros((b, 128 - 2 * idx.shape[1]), F32)], axis=1)
    col = lax.broadcasted_iota(jnp.int32, (nh, rows), 1)
    row = lax.broadcasted_iota(jnp.int32, (nh, rows), 0)
    bias[...] = jnp.where(lax.rem(col, kvh) == row // (nh // kvh), 0.0, NEG)

    a = _rms(x[...], ln1[...])

    def qstep(i, _):
        wq_copy(i).wait()
        w = wqb[:, pl.ds(pl.multiple_of(i * cq, cq), cq)]
        q = jnp.dot(a, w, preferred_element_type=F32).astype(BF16).astype(F32)
        for j in range(cq // hd):
            qs[pl.ds(i * (cq // hd) + j, b, stride=nh), :] = q[:, j * hd:(j + 1) * hd]
        return 0

    lax.fori_loop(0, nwq, qstep, 0)
    for i in range(nwo // 2, nwo):
        wo_copy(i).start()

    def group(g, _):
        slot = lax.rem(g, KVBUF)

        def go(n):
            for c in kv_copies(g, slot, n):
                c.wait()
            w = n * crow
            lane = lax.broadcasted_iota(jnp.int32, (nh, w), 1)
            for s in range(SEQ):
                sb = g * SEQ + s
                r = pl.ds(pl.multiple_of(sb * nh, nh), nh)
                q = qs[r, :].astype(BF16)
                k = kb[slot, s, 0:w, :]
                sc = lax.dot_general(q, k, (((1,), (1,)), ((), ())), preferred_element_type=F32)
                sc = sc * (hd ** -0.5) + bias[:, 0:w]
                sc = jnp.where(lane < lens[sb] * kvh, sc, NEG)
                m = jnp.max(sc, axis=1, keepdims=True)
                p = jnp.exp(sc - m)
                p = (p / jnp.sum(p, axis=1, keepdims=True)).astype(BF16)
                o = jnp.dot(p, vb[slot, s, 0:w, :], preferred_element_type=F32)
                os[r, :] = o.astype(BF16).astype(F32)
        by_class(g, go)
        pl.when(g + KVBUF < ngrp)(lambda: start_kv(g + KVBUF))
        return 0

    lax.fori_loop(0, ngrp, group, 0)

    for j in range(nh):
        ob[:, j * hd:(j + 1) * hd] = os[pl.ds(j, b, stride=nh), :].astype(BF16)

    def ostep(i, _):
        wo_copy(i).wait()
        c = pl.ds(pl.multiple_of(i * co, co), co)
        attn = jnp.dot(ob[...], wob[:, c], preferred_element_type=F32)
        hf[:, c] = (x[:, c].astype(F32) + attn).astype(BF16)
        return 0

    lax.fori_loop(0, nwo, ostep, 0)
    h = hf[...]
    h_out[...] = h
    u_out[...] = _rms(h, ln2[...])


def _attention(x, kv_k, kv_v, lens, idx, gates, ln1, ln2, wq, wo):
    b, d = x.shape
    _, l, kvh, hd = kv_k.shape
    hdim = wq.shape[1]
    nh = hdim // hd
    rows = l * kvh
    kk = kv_k.reshape(b, rows, hd)
    vv = kv_v.reshape(b, rows, hd)
    return pl.pallas_call(
        _attn_kernel,
        name="attn",
        out_shape=(jax.ShapeDtypeStruct((b, d), BF16), jax.ShapeDtypeStruct((b, d), BF16),
                   jax.ShapeDtypeStruct((b, 128), F32)),
        in_specs=[_sm(), _vm(), _vm(), _vm(), _vm(), _vm(), _any(), _any(), _any(), _any()],
        out_specs=(_vm(), _vm(), _vm()),
        scratch_shapes=[
            pltpu.VMEM((d, hdim), BF16),
            pltpu.VMEM((hdim, d), BF16),
            pltpu.VMEM((KVBUF, SEQ, rows, hd), BF16),
            pltpu.VMEM((KVBUF, SEQ, rows, hd), BF16),
            pltpu.VMEM((b * nh, hd), F32),
            pltpu.VMEM((b * nh, hd), F32),
            pltpu.VMEM((b, hdim), BF16),
            pltpu.VMEM((nh, rows), F32),
            pltpu.VMEM((b, d), BF16),
            pltpu.SemaphoreType.DMA((8,)),
            pltpu.SemaphoreType.DMA((8,)),
            pltpu.SemaphoreType.DMA((KVBUF,)),
            pltpu.SemaphoreType.DMA((KVBUF,)),
        ],
        compiler_params=pltpu.CompilerParams(vmem_limit_bytes=VLIM),
    )(lens, x, ln1.reshape(1, d), ln2.reshape(1, d), idx, gates, kk, vv, wq, wo)


def _places():
    cy = lax.axis_index("ey")
    cx = lax.axis_index("ex")
    xn = cy + 1 - 2 * lax.rem(cy, 2)
    yn = lax.rem(cy + 2, 4)
    dg = 3 - cy
    return cy, cx, (xn, yn, dg)


def _barrier(cy, cx, others):
    bar = pltpu.get_barrier_semaphore()
    for o in others:
        pl.semaphore_signal(bar, inc=1, device_id=(o, cx), device_id_type=MESH)
    pl.semaphore_signal(bar, inc=1, device_id=(cy, 1 - cx), device_id_type=MESH)
    pl.semaphore_wait(bar, len(others) + 1)


def _gather_kernel(u, pk, ua, pka, s_sem, r_sem, fs_sem, fr_sem):
    cy, cx, others = _places()
    _barrier(cy, cx, others)
    me = 2 * cy + cx

    def both(src_u, src_p, slot, dev, ss, rs, i):
        return (
            pltpu.make_async_remote_copy(
                src_ref=src_u, dst_ref=ua.at[slot], send_sem=ss.at[0, i], recv_sem=rs.at[0, i],
                device_id=dev, device_id_type=MESH),
            pltpu.make_async_remote_copy(
                src_ref=src_p, dst_ref=pka.at[slot], send_sem=ss.at[1, i], recv_sem=rs.at[1, i],
                device_id=dev, device_id_type=MESH))

    sends = []
    for i in (2, 0, 1):
        sends.append((i, both(u, pk, me, (others[i], cx), s_sem, r_sem, i)))
    for _, cs in sends:
        for c in cs:
            c.start()
    mine = both(u, pk, me, (cy, 1 - cx), fs_sem, fr_sem, 3)
    for c in mine:
        c.start()
    ua[me] = u[...]
    pka[me] = pk[...]
    fwds = [mine]
    for i in (0, 1, 2):
        slot = 2 * others[i] + cx
        for c in both(u, pk, slot, (others[i], cx), s_sem, r_sem, i):
            c.wait_recv()
        f = both(ua.at[slot], pka.at[slot], slot, (cy, 1 - cx), fs_sem, fr_sem, i)
        for c in f:
            c.start()
        fwds.append(f)
    for f in fwds:
        for c in f:
            c.wait()
    for _, cs in sends:
        for c in cs:
            c.wait_send()


def _all_gather(u, pk):
    b, d = u.shape
    return pl.pallas_call(
        _gather_kernel,
        name="gather",
        out_shape=(jax.ShapeDtypeStruct((8, b, d), BF16), jax.ShapeDtypeStruct((8, b, 128), F32)),
        in_specs=[_vm(), _vm()],
        out_specs=(_vm(), _vm()),
        scratch_shapes=[
            pltpu.SemaphoreType.DMA((2, 3)),
            pltpu.SemaphoreType.DMA((2, 3)),
            pltpu.SemaphoreType.DMA((2, 4)),
            pltpu.SemaphoreType.DMA((2, 4)),
        ],
        compiler_params=pltpu.CompilerParams(collective_id=0, has_side_effects=True),
    )(u, pk)


TILE = 128
WBUF = 4


def _silu_mul(z1, z3):
    return (z1 * jax.nn.sigmoid(z1) * z3).astype(BF16)


def _expert_kernel(first, ua, pka, h, u, ws1, ws3, ws2, w1, w3, w2, acc, hs,
                   b1, b3, b2, tmap, posk, posb, gateb, xt, gt, rt, cnt, sem):
    ntok, d = ua.shape
    ne = w1.shape[0]
    f = w1.shape[2]
    top = 8
    blk = ntok // 8
    cap = blk - blk // 8
    fc = 256
    dc = 512

    def copies(e, slot):
        return (pltpu.make_async_copy(w1.at[e], b1.at[slot], sem.at[0, slot]),
                pltpu.make_async_copy(w3.at[e], b3.at[slot], sem.at[1, slot]),
                pltpu.make_async_copy(w2.at[e], b2.at[slot], sem.at[2, slot]))

    shared = (pltpu.make_async_copy(ws1, b1.at[WBUF - 1], sem.at[0, WBUF - 1]),
              pltpu.make_async_copy(ws3, b3.at[WBUF - 1], sem.at[1, WBUF - 1]),
              pltpu.make_async_copy(ws2, b2.at[WBUF - 1], sem.at[2, WBUF - 1]))
    for c in shared:
        c.start()
    for e in range(WBUF - 1):
        for c in copies(e, e):
            c.start()

    e0 = first[0]
    tmap[...] = jnp.transpose(pka[...])
    ids = e0 + lax.broadcasted_iota(jnp.int32, (ne, ntok), 0)
    ids = ids.astype(F32)
    member = jnp.zeros((ne, ntok), F32)
    gate = jnp.zeros((ne, ntok), F32)
    for j in range(top):
        hit = tmap[j:j + 1, :] == ids
        member = member + jnp.where(hit, 1.0, 0.0)
        gate = gate + jnp.where(hit, tmap[top + j:top + j + 1, :], 0.0)
    ti = lax.broadcasted_iota(jnp.int32, (ntok, ntok), 0)
    tj = lax.broadcasted_iota(jnp.int32, (ntok, ntok), 1)
    tri = ti < tj
    tri_b = (tri & (ti // blk == tj // blk)).astype(F32).astype(BF16)
    rank = jnp.dot(member.astype(BF16), tri_b, preferred_element_type=F32)
    keep = jnp.where(rank < cap, member, 0.0)
    pos = jnp.dot(keep.astype(BF16), tri.astype(F32).astype(BF16), preferred_element_type=F32)
    pk = jnp.where(keep > 0, pos, -1.0)
    gk = gate * keep
    posk[...] = pk
    for e in range(ne):
        cnt[e] = jnp.sum(keep[e:e + 1, :]).astype(jnp.int32)
    both = jnp.concatenate([pk, gk, jnp.zeros((128 - 2 * ne, ntok), F32)], axis=0)
    cols = jnp.transpose(both)
    for e in range(ne):
        posb[e] = jnp.broadcast_to(cols[:, e:e + 1], (ntok, 128))
        gateb[e] = jnp.broadcast_to(cols[:, ne + e:ne + e + 1], (ntok, 128))

    def zero(i, _):
        acc[pl.ds(pl.multiple_of(i * 64, 64), 64), :] = jnp.zeros((64, d), F32)
        return 0
    lax.fori_loop(0, ntok // 64, zero, 0)

    for c in shared:
        c.wait()
    for c in range(f // fc):
        s = slice(c * fc, (c + 1) * fc)
        z1 = jnp.dot(u[...], b1[WBUF - 1, :, s], preferred_element_type=F32)
        z3 = jnp.dot(u[...], b3[WBUF - 1, :, s], preferred_element_type=F32)
        gt[0:blk, s] = _silu_mul(z1, z3)
    for c in range(d // dc):
        s = slice(c * dc, (c + 1) * dc)
        hs[:, s] = h[:, s].astype(F32) + jnp.dot(gt[0:blk, :], b2[WBUF - 1, :, s], preferred_element_type=F32)
    for c in copies(WBUF - 1, WBUF - 1):
        c.start()

    def ffn(slot):
        for c in range(f // fc):
            s = slice(c * fc, (c + 1) * fc)
            z1 = jnp.dot(xt[...], b1[slot, :, s], preferred_element_type=F32)
            z3 = jnp.dot(xt[...], b3[slot, :, s], preferred_element_type=F32)
            gt[:, s] = _silu_mul(z1, z3)
        for c in range(d // dc):
            s = slice(c * dc, (c + 1) * dc)
            rt[:, s] = jnp.dot(gt[...], b2[slot, :, s], preferred_element_type=F32).astype(BF16)

    def expert(e, _):
        slot = lax.rem(e, WBUF)
        for c in copies(e, slot):
            c.wait()
        n = cnt[e]

        def packed(t, _):
            base = t * TILE
            want = (lax.broadcasted_iota(jnp.int32, (TILE, ntok), 0) + base).astype(F32)
            sel = (posk[pl.ds(e, 1), :] == want).astype(F32).astype(BF16)
            for c in range(d // dc):
                s = slice(c * dc, (c + 1) * dc)
                xt[:, s] = jnp.dot(sel, ua[:, s], preferred_element_type=F32).astype(BF16)
            ffn(slot)
            wantc = (lax.broadcasted_iota(jnp.int32, (ntok, TILE), 1) + base).astype(F32)
            selt = (posb[e] == wantc).astype(F32).astype(BF16)
            for c in range(d // 256):
                s = slice(c * 256, (c + 1) * 256)
                y = jnp.dot(selt, rt[:, s], preferred_element_type=F32)
                g = gateb[e]
                acc[:, c * 256:c * 256 + 128] += g * y[:, 0:128]
                acc[:, c * 256 + 128:(c + 1) * 256] += g * y[:, 128:256]
            return 0

        def dense(t, _):
            rows = pl.ds(pl.multiple_of(t * TILE, TILE), TILE)
            xt[...] = ua[rows, :]
            ffn(slot)
            g = gateb[e, rows, :]
            for c in range(d // 128):
                s = slice(c * 128, (c + 1) * 128)
                acc[rows, s] += g * rt[:, s].astype(F32)
            return 0

        many = n > 2 * TILE
        lax.fori_loop(0, jnp.where(many, 0, (n + TILE - 1) // TILE), packed, 0)
        lax.fori_loop(0, jnp.where(many, ntok // TILE, 0), dense, 0)

        @pl.when(e + WBUF < ne)
        def _():
            for c in copies(e + WBUF, slot):
                c.start()
        return 0

    lax.fori_loop(0, ne, expert, 0)


def _experts(first, ua, pka, h, u, ws1, ws3, ws2, w1, w3, w2):
    ntok, d = ua.shape
    b = u.shape[0]
    ne, _, f = w1.shape
    return pl.pallas_call(
        _expert_kernel,
        name="experts",
        out_shape=(jax.ShapeDtypeStruct((ntok, d), F32), jax.ShapeDtypeStruct((b, d), F32)),
        in_specs=[_sm(), _vm(), _vm(), _vm(), _vm()] + [_any()] * 6,
        out_specs=(_vm(), _vm()),
        scratch_shapes=[
            pltpu.VMEM((WBUF, d, f), BF16),
            pltpu.VMEM((WBUF, d, f), BF16),
            pltpu.VMEM((WBUF, f, d), BF16),
            pltpu.VMEM((128, ntok), F32),
            pltpu.VMEM((ne, ntok), F32),
            pltpu.VMEM((ne, ntok, 128), F32),
            pltpu.VMEM((ne, ntok, 128), F32),
            pltpu.VMEM((TILE, d), BF16),
            pltpu.VMEM((TILE, f), BF16),
            pltpu.VMEM((TILE, d), BF16),
            pltpu.SMEM((ne,), jnp.int32),
            pltpu.SemaphoreType.DMA((3, WBUF)),
        ],
        compiler_params=pltpu.CompilerParams(vmem_limit_bytes=VLIM),
    )(first, ua, pka, h, u, ws1, ws3, ws2, w1, w3, w2)


CH = 4


def _return_kernel(acc, hs, y, rbuf, sbuf, gbuf, ds_sem, dr_sem, s_sem, r_sem):
    cy, cx, others = _places()
    _barrier(cy, cx, others)
    d = acc.shape[3]
    w = d // CH

    def cols(c):
        return pl.ds(c * w, w)

    def pair(c):
        return pltpu.make_async_remote_copy(
            src_ref=acc.at[:, 1 - cx, :, cols(c)], dst_ref=rbuf.at[c], send_sem=ds_sem.at[c], recv_sem=dr_sem.at[c],
            device_id=(cy, 1 - cx), device_id_type=MESH)

    def far(c, i):
        return pltpu.make_async_remote_copy(
            src_ref=sbuf.at[c, others[i]], dst_ref=gbuf.at[c, i], send_sem=s_sem.at[c, i], recv_sem=r_sem.at[c, i],
            device_id=(others[i], cx), device_id_type=MESH)

    for c in range(CH):
        pair(c).start()
    for c in range(CH):
        pair(c).wait_recv()
        for k in range(4):
            sbuf[c, k] = acc[k, cx, :, c * w:(c + 1) * w] + rbuf[c, k]
        for i in (2, 0, 1):
            far(c, i).start()
    for c in range(CH):
        for i in range(3):
            far(c, i).wait_recv()
        s = slice(c * w, (c + 1) * w)
        t = hs[:, s] + sbuf[c, cy]
        t = t + (gbuf[c, 0] + gbuf[c, 1] + gbuf[c, 2])
        y[:, s] = t.astype(BF16)
    for c in range(CH):
        pair(c).wait_send()
        for i in range(3):
            far(c, i).wait_send()


def _return(acc, hs):
    b, d = hs.shape
    w = d // CH
    return pl.pallas_call(
        _return_kernel,
        name="giveback",
        out_shape=jax.ShapeDtypeStruct((b, d), BF16),
        in_specs=[_vm(), _vm()],
        out_specs=_vm(),
        scratch_shapes=[
            pltpu.VMEM((CH, 4, b, w), F32),
            pltpu.VMEM((CH, 4, b, w), F32),
            pltpu.VMEM((CH, 3, b, w), F32),
            pltpu.SemaphoreType.DMA((CH,)),
            pltpu.SemaphoreType.DMA((CH,)),
            pltpu.SemaphoreType.DMA((CH, 3)),
            pltpu.SemaphoreType.DMA((CH, 3)),
        ],
        compiler_params=pltpu.CompilerParams(collective_id=1, has_side_effects=True, vmem_limit_bytes=VLIM),
    )(acc, hs)


def solution(mesh):
    nx = mesh.shape["ex"]

    def body(x, kv_k, kv_v, lens, idx, gates, ln1, wq, wo, ln2, ws1, ws3, ws2, w1, w3, w2):
        b, d = x.shape
        edev = w1.shape[0]
        me = lax.axis_index("ey") * nx + lax.axis_index("ex")
        h, u, pk = _attention(x, kv_k, kv_v, lens, idx, gates, ln1, ln2, wq, wo)
        ua, pka = _all_gather(u, pk)
        first = (me * edev).astype(jnp.int32).reshape(1)
        acc, hs = _experts(first, ua.reshape(8 * b, d), pka.reshape(8 * b, 128), h, u, ws1, ws3, ws2, w1, w3, w2)
        return _return(acc.reshape(4, 2, b, d), hs)

    rows = P(GRP)
    rep = P()
    return jax.shard_map(
        body, mesh=mesh,
        in_specs=(rows, rows, rows, rows, rows, rows, rep, rep, rep, rep, rep, rep, rep, rows, rows, rows),
        out_specs=rows, check_vma=False)
```

```python
import functools

import jax
import jax.numpy as jnp
from jax import lax
from jax.experimental import pallas as pl
from jax.experimental.pallas import tpu as pltpu
from jax.sharding import PartitionSpec as P

EPS = 1e-6
GRP = ("ey", "ex")
MESH = pl.DeviceIdType.MESH
NEG = -1e30
F32 = jnp.float32
BF16 = jnp.bfloat16
VLIM = 55 * 1024 * 1024


def _vm():
    return pl.BlockSpec(memory_space=pltpu.VMEM)


def _sm():
    return pl.BlockSpec(memory_space=pltpu.SMEM)


def _any():
    return pl.BlockSpec(memory_space=pl.ANY)


def _rms(v, w):
    v32 = v.astype(F32)
    r = lax.rsqrt(jnp.mean(v32 * v32, axis=-1, keepdims=True) + EPS)
    return (v32 * r * w.astype(F32)).astype(BF16)


SEQ = 8
KVBUF = 4
STEP = 64


def _attn_kernel(lens, x, ln1, ln2, idx, gates, kk, vv, wq, wo, h_out, u_out, pk_out,
                 wqb, wob, kb, vb, qs, os, ob, bias, hf, ss, ps, wq_sem, wo_sem, k_sem, v_sem):
    b, d = x.shape
    heads_dim = wqb.shape[1]
    hd = 128
    nh = heads_dim // hd
    rows = kk.shape[1]
    kvh = 4
    seqlen = rows // kvh
    ncls = seqlen // STEP
    crow = STEP * kvh
    ngrp = b // SEQ
    nwq = wq_sem.shape[0]
    nwo = wo_sem.shape[0]
    cq = heads_dim // nwq
    co = d // nwo

    def wq_copy(i):
        c = pl.ds(pl.multiple_of(i * cq, cq), cq)
        return pltpu.make_async_copy(wq.at[:, c], wqb.at[:, c], wq_sem.at[i])

    def wo_copy(i):
        c = pl.ds(pl.multiple_of(i * co, co), co)
        return pltpu.make_async_copy(wo.at[:, c], wob.at[:, c], wo_sem.at[i])

    def gmax(g):
        m = lens[g * SEQ]
        for s in range(1, SEQ):
            m = jnp.maximum(m, lens[g * SEQ + s])
        return m

    def kv_copies(g, slot, n):
        src = (pl.ds(g * SEQ, SEQ), pl.ds(0, n * crow))
        dst = (slot, slice(None), pl.ds(0, n * crow))
        return (pltpu.make_async_copy(kk.at[src], kb.at[dst], k_sem.at[slot]),
                pltpu.make_async_copy(vv.at[src], vb.at[dst], v_sem.at[slot]))

    def by_class(g, f):
        cls = (gmax(g) + STEP - 1) // STEP
        for n in range(1, ncls + 1):
            pl.when(cls == n)(functools.partial(f, n))

    def start_kv(g):
        slot = lax.rem(g, KVBUF)

        def go(n):
            for c in kv_copies(g, slot, n):
                c.start()
        by_class(g, go)

    for i in range(nwq):
        wq_copy(i).start()
    lax.fori_loop(0, min(KVBUF, ngrp), lambda g, _: (start_kv(g), 0)[1], 0)
    table = jnp.concatenate([idx[...].astype(F32), gates[...]], axis=0)
    table = jnp.concatenate([table, jnp.zeros((table.shape[0], 128 - b), F32)], axis=1)
    table = jnp.concatenate([table, jnp.zeros((128 - table.shape[0], 128), F32)], axis=0)
    pk_out[...] = jnp.transpose(table)[0:b, :]
    col = lax.broadcasted_iota(jnp.int32, (nh, rows), 1)
    row = lax.broadcasted_iota(jnp.int32, (nh, rows), 0)
    bias[...] = jnp.where(lax.rem(col, kvh) == row // (nh // kvh), 0.0, NEG)

    a = _rms(x[...], ln1[...])

    def qstep(i, _):
        wq_copy(i).wait()
        w = wqb[:, pl.ds(pl.multiple_of(i * cq, cq), cq)]
        q = jnp.dot(a, w, preferred_element_type=F32).astype(BF16).astype(F32)
        for j in range(cq // hd):
            qs[pl.ds(i * (cq // hd) + j, b, stride=nh), :] = q[:, j * hd:(j + 1) * hd]
        return 0

    lax.fori_loop(0, nwq, qstep, 0)
    per = nwo // min(KVBUF, ngrp)

    def group(g, _):
        slot = lax.rem(g, KVBUF)

        def go(n):
            for c in kv_copies(g, slot, n):
                c.wait()
            w = n * crow
            lane = lax.broadcasted_iota(jnp.int32, (nh, w), 1)
            rq = [pl.ds(pl.multiple_of((g * SEQ + s) * nh, nh), nh) for s in range(SEQ)]
            for s in range(SEQ):
                q = qs[rq[s], :].astype(BF16)
                k = kb[slot, s, 0:w, :]
                ss[s * nh:(s + 1) * nh, 0:w] = lax.dot_general(
                    q, k, (((1,), (1,)), ((), ())), preferred_element_type=F32)
            for s in range(SEQ):
                sc = ss[s * nh:(s + 1) * nh, 0:w] * (hd ** -0.5) + bias[:, 0:w]
                sc = jnp.where(lane < lens[g * SEQ + s] * kvh, sc, NEG)
                m = jnp.max(sc, axis=1, keepdims=True)
                p = jnp.exp(sc - m)
                ps[s * nh:(s + 1) * nh, 0:w] = (p * (1.0 / jnp.sum(p, axis=1, keepdims=True))).astype(BF16)
            for s in range(SEQ):
                o = jnp.dot(ps[s * nh:(s + 1) * nh, 0:w], vb[slot, s, 0:w, :], preferred_element_type=F32)
                os[rq[s], :] = o.astype(BF16).astype(F32)
        by_class(g, go)
        pl.when(g + KVBUF < ngrp)(lambda: start_kv(g + KVBUF))

        @pl.when(g + KVBUF >= ngrp)
        def _():
            for i in range(per):
                wo_copy((g + KVBUF - ngrp) * per + i).start()
        return 0

    lax.fori_loop(0, ngrp, group, 0)

    for j in range(nh):
        ob[:, j * hd:(j + 1) * hd] = os[pl.ds(j, b, stride=nh), :].astype(BF16)

    def ostep(i, _):
        wo_copy(i).wait()
        c = pl.ds(pl.multiple_of(i * co, co), co)
        attn = jnp.dot(ob[...], wob[:, c], preferred_element_type=F32)
        hf[:, c] = (x[:, c].astype(F32) + attn).astype(BF16)
        return 0

    lax.fori_loop(0, nwo, ostep, 0)
    h = hf[...]
    h_out[...] = h
    u_out[...] = _rms(h, ln2[...])


def _attention(x, kv_k, kv_v, lens, idx, gates, ln1, ln2, wq, wo):
    b, d = x.shape
    _, l, kvh, hd = kv_k.shape
    hdim = wq.shape[1]
    nh = hdim // hd
    rows = l * kvh
    kk = kv_k.reshape(b, rows, hd)
    vv = kv_v.reshape(b, rows, hd)
    return pl.pallas_call(
        _attn_kernel,
        name="attn",
        out_shape=(pltpu.VMEM((b, d), BF16), pltpu.VMEM((b, d), BF16), pltpu.VMEM((b, 128), F32)),
        in_specs=[_sm(), _vm(), _vm(), _vm(), _vm(), _vm(), _any(), _any(), _any(), _any()],
        out_specs=(_vm(), _vm(), _vm()),
        scratch_shapes=[
            pltpu.VMEM((d, hdim), BF16),
            pltpu.VMEM((hdim, d), BF16),
            pltpu.VMEM((KVBUF, SEQ, rows, hd), BF16),
            pltpu.VMEM((KVBUF, SEQ, rows, hd), BF16),
            pltpu.VMEM((b * nh, hd), F32),
            pltpu.VMEM((b * nh, hd), F32),
            pltpu.VMEM((b, hdim), BF16),
            pltpu.VMEM((nh, rows), F32),
            pltpu.VMEM((b, d), BF16),
            pltpu.VMEM((SEQ * nh, rows), F32),
            pltpu.VMEM((SEQ * nh, rows), BF16),
            pltpu.SemaphoreType.DMA((8,)),
            pltpu.SemaphoreType.DMA((8,)),
            pltpu.SemaphoreType.DMA((KVBUF,)),
            pltpu.SemaphoreType.DMA((KVBUF,)),
        ],
        compiler_params=pltpu.CompilerParams(vmem_limit_bytes=VLIM),
    )(lens, x, ln1, ln2, idx.T, gates.T, kk, vv, wq, wo)


def _places():
    cy = lax.axis_index("ey")
    cx = lax.axis_index("ex")
    xn = cy + 1 - 2 * lax.rem(cy, 2)
    yn = lax.rem(cy + 2, 4)
    dg = 3 - cy
    return cy, cx, (xn, yn, dg)


def _barrier(cy, cx, others):
    bar = pltpu.get_barrier_semaphore()
    for o in others:
        pl.semaphore_signal(bar, inc=1, device_id=(o, cx), device_id_type=MESH)
    pl.semaphore_signal(bar, inc=1, device_id=(cy, 1 - cx), device_id_type=MESH)
    pl.semaphore_wait(bar, len(others) + 1)


WBUF = 4
TILE = 128


def _silu_mul(z1, z3):
    return (z1 * jax.nn.sigmoid(z1) * z3).astype(BF16)


def _slot_copies(w1, w3, w2, b1, b3, b2, sem, e, slot):
    return (pltpu.make_async_copy(w1.at[e], b1.at[slot], sem.at[0, slot]),
            pltpu.make_async_copy(w3.at[e], b3.at[slot], sem.at[1, slot]),
            pltpu.make_async_copy(w2.at[e], b2.at[slot], sem.at[2, slot]))


def _gather_kernel(u, pk, h, ws1, ws3, ws2, w1, w3, w2, ua, posk, cols, hs, b1, b3, b2,
                   pka, v1, v3, v2, gt, tmap, s_sem, r_sem, fs_sem, fr_sem, w_sem, v_sem):
    blk, d = u.shape
    ntok = 8 * blk
    ne = w1.shape[0]
    f = w1.shape[2]
    top = 8
    cap = blk - blk // 8
    cy, cx, others = _places()
    me = 2 * cy + cx

    shared = (pltpu.make_async_copy(ws1, v1, v_sem.at[0]),
              pltpu.make_async_copy(ws3, v3, v_sem.at[1]),
              pltpu.make_async_copy(ws2, v2, v_sem.at[2]))
    for c in shared:
        c.start()
    ahead = [_slot_copies(w1, w3, w2, b1, b3, b2, w_sem, e, e) for e in range(WBUF)]
    for cs in ahead:
        for c in cs:
            c.start()

    _barrier(cy, cx, others)

    def pair(k, src, slot, dev, ss, rs, i):
        out = (ua, pka)[k]
        return pltpu.make_async_remote_copy(
            src_ref=src, dst_ref=out.at[slot], send_sem=ss.at[k, i], recv_sem=rs.at[k, i],
            device_id=dev, device_id_type=MESH)

    src = (u, pk)
    outs = (ua, pka)
    for k in (1, 0):
        for i in (2, 0, 1):
            pair(k, src[k], me, (others[i], cx), s_sem, r_sem, i).start()
        pair(k, src[k], me, (cy, 1 - cx), fs_sem, fr_sem, 3).start()
    ua[me] = u[...]
    pka[me] = pk[...]

    for c in shared:
        c.wait()
    for c in range(f // 256):
        s = slice(c * 256, (c + 1) * 256)
        z1 = jnp.dot(u[...], v1[:, s], preferred_element_type=F32)
        z3 = jnp.dot(u[...], v3[:, s], preferred_element_type=F32)
        gt[:, s] = _silu_mul(z1, z3)
    for c in range(d // 512):
        s = slice(c * 512, (c + 1) * 512)
        hs[:, s] = h[:, s].astype(F32) + jnp.dot(gt[...], v2[:, s], preferred_element_type=F32)

    def relay(k):
        for i in (0, 1, 2):
            slot = 2 * others[i] + cx
            pair(k, src[k], slot, (others[i], cx), s_sem, r_sem, i).wait_recv()
            pair(k, outs[k].at[slot], slot, (cy, 1 - cx), fs_sem, fr_sem, i).start()

    def settle(k):
        for i in (0, 1, 2):
            slot = 2 * others[i] + cx
            pair(k, outs[k].at[slot], slot, (cy, 1 - cx), fs_sem, fr_sem, i).wait()
            pair(k, src[k], me, (others[i], cx), s_sem, r_sem, i).wait_send()
        pair(k, src[k], me, (cy, 1 - cx), fs_sem, fr_sem, 3).wait()

    relay(1)
    settle(1)

    tmap[...] = jnp.transpose(pka[...].reshape(ntok, 128))
    ids = (me * ne + lax.broadcasted_iota(jnp.int32, (ne, ntok), 0)).astype(F32)
    member = jnp.zeros((ne, ntok), F32)
    gate = jnp.zeros((ne, ntok), F32)
    for j in range(top):
        hit = tmap[j:j + 1, :] == ids
        member = member + jnp.where(hit, 1.0, 0.0)
        gate = gate + jnp.where(hit, tmap[top + j:top + j + 1, :], 0.0)
    ti = lax.broadcasted_iota(jnp.int32, (ntok, ntok), 0)
    tj = lax.broadcasted_iota(jnp.int32, (ntok, ntok), 1)
    tri = ti < tj
    tri_b = (tri & (ti // blk == tj // blk)).astype(F32).astype(BF16)
    rank = jnp.dot(member.astype(BF16), tri_b, preferred_element_type=F32)
    keep = jnp.where(rank < cap, member, 0.0)
    pos = jnp.dot(keep.astype(BF16), tri.astype(F32).astype(BF16), preferred_element_type=F32)
    pkeep = jnp.where(keep > 0, pos, -1.0)
    posk[...] = pkeep
    both = jnp.concatenate([pkeep, gate * keep, jnp.zeros((128 - 2 * ne, ntok), F32)], axis=0)
    cols[...] = jnp.transpose(both)

    relay(0)
    settle(0)
    for cs in ahead:
        for c in cs:
            c.wait()


def _all_gather(u, pk, h, ws1, ws3, ws2, w1, w3, w2):
    b, d = u.shape
    ne, _, f = w1.shape
    return pl.pallas_call(
        _gather_kernel,
        name="gather",
        out_shape=(pltpu.VMEM((8, b, d), BF16),
                   pltpu.VMEM((ne, 8 * b), F32),
                   pltpu.VMEM((8 * b, 128), F32),
                   pltpu.VMEM((b, d), F32),
                   pltpu.VMEM((WBUF, d, f), BF16),
                   pltpu.VMEM((WBUF, d, f), BF16),
                   pltpu.VMEM((WBUF, f, d), BF16)),
        in_specs=[_vm(), _vm(), _vm()] + [_any()] * 6,
        out_specs=(_vm(),) * 7,
        scratch_shapes=[
            pltpu.VMEM((8, b, 128), F32),
            pltpu.VMEM((d, f), BF16),
            pltpu.VMEM((d, f), BF16),
            pltpu.VMEM((f, d), BF16),
            pltpu.VMEM((b, f), BF16),
            pltpu.VMEM((128, 8 * b), F32),
            pltpu.SemaphoreType.DMA((2, 3)),
            pltpu.SemaphoreType.DMA((2, 3)),
            pltpu.SemaphoreType.DMA((2, 4)),
            pltpu.SemaphoreType.DMA((2, 4)),
            pltpu.SemaphoreType.DMA((3, WBUF)),
            pltpu.SemaphoreType.DMA((3,)),
        ],
        compiler_params=pltpu.CompilerParams(
            collective_id=0, has_side_effects=True, vmem_limit_bytes=12 * 1024 * 1024),
    )(u, pk, h, ws1, ws3, ws2, w1, w3, w2)


def _expert_kernel(ua, posk, cols, i1, i3, i2, w1, w3, w2, acc, b1, b3, b2, xt, gt, rt, psc, gsc, cnt, sem):
    del i1, i3, i2
    ntok, d = ua.shape
    ne = w1.shape[0]
    f = w1.shape[2]
    fc = 256
    dc = 512

    def copies(e, slot):
        return _slot_copies(w1, w3, w2, b1, b3, b2, sem, e, slot)

    for e in range(ne):
        cnt[e] = (jnp.max(posk[e:e + 1, :]) + 1.0).astype(jnp.int32)

    def zero(i, _):
        acc[pl.ds(pl.multiple_of(i * 64, 64), 64), :] = jnp.zeros((64, d), F32)
        return 0
    lax.fori_loop(0, ntok // 64, zero, 0)

    def ffn(slot):
        for c in range(f // fc):
            s = slice(c * fc, (c + 1) * fc)
            z1 = jnp.dot(xt[...], b1[slot, :, s], preferred_element_type=F32)
            z3 = jnp.dot(xt[...], b3[slot, :, s], preferred_element_type=F32)
            gt[:, s] = _silu_mul(z1, z3)
        for c in range(d // dc):
            s = slice(c * dc, (c + 1) * dc)
            rt[:, s] = jnp.dot(gt[...], b2[slot, :, s], preferred_element_type=F32).astype(BF16)

    def expert(e, _):
        slot = lax.rem(e, WBUF)

        @pl.when(e >= WBUF)
        def _():
            for c in copies(e, slot):
                c.wait()
        n = cnt[e]
        lane = lax.broadcasted_iota(jnp.int32, (ntok, 128), 1)
        psc[...] = jnp.broadcast_to(
            jnp.sum(jnp.where(lane == e, cols[...], 0.0), axis=1, keepdims=True), (ntok, 128))
        gsc[...] = jnp.broadcast_to(
            jnp.sum(jnp.where(lane == e + ne, cols[...], 0.0), axis=1, keepdims=True), (ntok, 128))

        def packed(t, _):
            base = t * TILE
            want = (lax.broadcasted_iota(jnp.int32, (TILE, ntok), 0) + base).astype(F32)
            sel = (posk[pl.ds(e, 1), :] == want).astype(F32).astype(BF16)
            for c in range(d // dc):
                s = slice(c * dc, (c + 1) * dc)
                xt[:, s] = jnp.dot(sel, ua[:, s], preferred_element_type=F32).astype(BF16)
            ffn(slot)
            wantc = (lax.broadcasted_iota(jnp.int32, (ntok, TILE), 1) + base).astype(F32)
            selt = (psc[...] == wantc).astype(F32).astype(BF16)
            for c in range(d // 256):
                s = slice(c * 256, (c + 1) * 256)
                y = jnp.dot(selt, rt[:, s], preferred_element_type=F32)
                g = gsc[...]
                acc[:, c * 256:c * 256 + 128] += g * y[:, 0:128]
                acc[:, c * 256 + 128:(c + 1) * 256] += g * y[:, 128:256]
            return 0

        def dense(t, _):
            rows = pl.ds(pl.multiple_of(t * TILE, TILE), TILE)
            xt[...] = ua[rows, :]
            ffn(slot)
            g = gsc[rows, :]
            for c in range(d // 128):
                s = slice(c * 128, (c + 1) * 128)
                acc[rows, s] += g * rt[:, s].astype(F32)
            return 0

        many = n > 2 * TILE
        lax.fori_loop(0, jnp.where(many, 0, (n + TILE - 1) // TILE), packed, 0)
        lax.fori_loop(0, jnp.where(many, ntok // TILE, 0), dense, 0)

        @pl.when(e + WBUF < ne)
        def _():
            for c in copies(e + WBUF, slot):
                c.start()
        return 0

    lax.fori_loop(0, ne, expert, 0)


def _experts(ua, posk, cols, i1, i3, i2, w1, w3, w2):
    ntok, d = ua.shape
    ne, _, f = w1.shape
    return pl.pallas_call(
        _expert_kernel,
        name="experts",
        out_shape=(pltpu.VMEM((ntok, d), F32),
                   pltpu.VMEM((WBUF, d, f), BF16),
                   pltpu.VMEM((WBUF, d, f), BF16),
                   pltpu.VMEM((WBUF, f, d), BF16)),
        in_specs=[_vm()] * 6 + [_any()] * 3,
        out_specs=(_vm(),) * 4,
        input_output_aliases={3: 1, 4: 2, 5: 3},
        scratch_shapes=[
            pltpu.VMEM((TILE, d), BF16),
            pltpu.VMEM((TILE, f), BF16),
            pltpu.VMEM((TILE, d), BF16),
            pltpu.VMEM((ntok, 128), F32),
            pltpu.VMEM((ntok, 128), F32),
            pltpu.SMEM((ne,), jnp.int32),
            pltpu.SemaphoreType.DMA((3, WBUF)),
        ],
        compiler_params=pltpu.CompilerParams(vmem_limit_bytes=3584 * 1024),
    )(ua, posk, cols, i1, i3, i2, w1, w3, w2)[0]


CH = 4


def _return_kernel(acc, hs, y, rbuf, sbuf, gbuf, ds_sem, dr_sem, s_sem, r_sem):
    cy, cx, others = _places()
    _barrier(cy, cx, others)
    d = acc.shape[3]
    w = d // CH

    def cols(c):
        return pl.ds(c * w, w)

    def pair(c):
        return pltpu.make_async_remote_copy(
            src_ref=acc.at[:, 1 - cx, :, cols(c)], dst_ref=rbuf.at[c], send_sem=ds_sem.at[c], recv_sem=dr_sem.at[c],
            device_id=(cy, 1 - cx), device_id_type=MESH)

    def far(c, i):
        return pltpu.make_async_remote_copy(
            src_ref=sbuf.at[c, others[i]], dst_ref=gbuf.at[c, i], send_sem=s_sem.at[c, i], recv_sem=r_sem.at[c, i],
            device_id=(others[i], cx), device_id_type=MESH)

    for c in range(CH):
        pair(c).start()
    for c in range(CH):
        pair(c).wait_recv()
        for k in range(4):
            sbuf[c, k] = acc[k, cx, :, c * w:(c + 1) * w] + rbuf[c, k]
        for i in (2, 0, 1):
            far(c, i).start()
    for c in range(CH):
        for i in range(3):
            far(c, i).wait_recv()
        s = slice(c * w, (c + 1) * w)
        t = hs[:, s] + sbuf[c, cy]
        t = t + (gbuf[c, 0] + gbuf[c, 1] + gbuf[c, 2])
        y[:, s] = t.astype(BF16)
    for c in range(CH):
        pair(c).wait_send()
        for i in range(3):
            far(c, i).wait_send()


def _return(acc, hs):
    b, d = hs.shape
    w = d // CH
    return pl.pallas_call(
        _return_kernel,
        name="giveback",
        out_shape=jax.ShapeDtypeStruct((b, d), BF16),
        in_specs=[_vm(), _vm()],
        out_specs=_vm(),
        scratch_shapes=[
            pltpu.VMEM((CH, 4, b, w), F32),
            pltpu.VMEM((CH, 4, b, w), F32),
            pltpu.VMEM((CH, 3, b, w), F32),
            pltpu.SemaphoreType.DMA((CH,)),
            pltpu.SemaphoreType.DMA((CH,)),
            pltpu.SemaphoreType.DMA((CH, 3)),
            pltpu.SemaphoreType.DMA((CH, 3)),
        ],
        compiler_params=pltpu.CompilerParams(
            collective_id=1, has_side_effects=True, vmem_limit_bytes=9 * 1024 * 1024),
    )(acc, hs)


def solution(mesh):
    def body(x, kv_k, kv_v, lens, idx, gates, ln1, wq, wo, ln2, ws1, ws3, ws2, w1, w3, w2):
        b, d = x.shape
        h, u, pk = _attention(x, kv_k, kv_v, lens, idx, gates, ln1, ln2, wq, wo)
        ua, posk, cols, hs, b1, b3, b2 = _all_gather(u, pk, h, ws1, ws3, ws2, w1, w3, w2)
        acc = _experts(ua.reshape(8 * b, d), posk, cols, b1, b3, b2, w1, w3, w2)
        return _return(acc.reshape(4, 2, b, d), hs)

    rows = P(GRP)
    rep = P()
    return jax.shard_map(
        body, mesh=mesh,
        in_specs=(rows, rows, rows, rows, rows, rows, rep, rep, rep, rep, rep, rep, rep, rows, rows, rows),
        out_specs=rows, check_vma=False)
```

```python
import functools

import jax
import jax.numpy as jnp
from jax import lax
from jax.experimental import pallas as pl
from jax.experimental.pallas import tpu as pltpu
from jax.sharding import PartitionSpec as P

EPS = 1e-6
GRP = ("ey", "ex")
MESH = pl.DeviceIdType.MESH
NEG = -1e30
F32 = jnp.float32
BF16 = jnp.bfloat16
VLIM = 55 * 1024 * 1024


def _vm():
    return pl.BlockSpec(memory_space=pltpu.VMEM)


def _sm():
    return pl.BlockSpec(memory_space=pltpu.SMEM)


def _hbm():
    return pl.BlockSpec(memory_space=pltpu.HBM)


def _any():
    return pl.BlockSpec(memory_space=pl.ANY)


def _rms(v, w):
    v32 = v.astype(F32)
    r = lax.rsqrt(jnp.mean(v32 * v32, axis=-1, keepdims=True) + EPS)
    return (v32 * r * w.astype(F32)).astype(BF16)


SEQ = 8
KVBUF = 4
STEP = 64


def _attn_kernel(lens, x, ln1, ln2, idx, gates, kk, vv, wq, wo, h_out, u_out, pk_out,
                 wqb, wob, kb, vb, qs, os, ob, bias, hf, ss, ps, wq_sem, wo_sem, k_sem, v_sem):
    b, d = x.shape
    heads_dim = wqb.shape[1]
    hd = 128
    nh = heads_dim // hd
    rows = kk.shape[1]
    kvh = 4
    seqlen = rows // kvh
    ncls = seqlen // STEP
    crow = STEP * kvh
    ngrp = b // SEQ
    nwq = wq_sem.shape[0]
    nwo = wo_sem.shape[0]
    cq = heads_dim // nwq
    co = d // nwo

    def wq_copy(i):
        c = pl.ds(pl.multiple_of(i * cq, cq), cq)
        return pltpu.make_async_copy(wq.at[:, c], wqb.at[:, c], wq_sem.at[i])

    def wo_copy(i):
        c = pl.ds(pl.multiple_of(i * co, co), co)
        return pltpu.make_async_copy(wo.at[:, c], wob.at[:, c], wo_sem.at[i])

    def gmax(g):
        m = lens[g * SEQ]
        for s in range(1, SEQ):
            m = jnp.maximum(m, lens[g * SEQ + s])
        return m

    def kv_copies(g, slot, n):
        src = (pl.ds(g * SEQ, SEQ), pl.ds(0, n * crow))
        dst = (slot, slice(None), pl.ds(0, n * crow))
        return (pltpu.make_async_copy(kk.at[src], kb.at[dst], k_sem.at[slot]),
                pltpu.make_async_copy(vv.at[src], vb.at[dst], v_sem.at[slot]))

    def by_class(g, f):
        cls = (gmax(g) + STEP - 1) // STEP
        for n in range(1, ncls + 1):
            pl.when(cls == n)(functools.partial(f, n))

    def start_kv(g):
        slot = lax.rem(g, KVBUF)

        def go(n):
            for c in kv_copies(g, slot, n):
                c.start()
        by_class(g, go)

    for i in range(nwq):
        wq_copy(i).start()
    lax.fori_loop(0, min(KVBUF, ngrp), lambda g, _: (start_kv(g), 0)[1], 0)
    table = jnp.concatenate([idx[...].astype(F32), gates[...]], axis=0)
    pk_out[...] = jnp.concatenate([table, jnp.zeros((table.shape[0], 128 - b), F32)], axis=1)
    col = lax.broadcasted_iota(jnp.int32, (nh, rows), 1)
    row = lax.broadcasted_iota(jnp.int32, (nh, rows), 0)
    bias[...] = jnp.where(lax.rem(col, kvh) == row // (nh // kvh), 0.0, NEG)

    a = _rms(x[...], ln1[...])

    def qstep(i, _):
        wq_copy(i).wait()
        w = wqb[:, pl.ds(pl.multiple_of(i * cq, cq), cq)]
        q = jnp.dot(a, w, preferred_element_type=F32).astype(BF16).astype(F32)
        for j in range(cq // hd):
            qs[pl.ds(i * (cq // hd) + j, b, stride=nh), :] = q[:, j * hd:(j + 1) * hd]
        return 0

    lax.fori_loop(0, nwq, qstep, 0)
    per = nwo // min(KVBUF, ngrp)

    def group(g, _):
        slot = lax.rem(g, KVBUF)

        def go(n):
            for c in kv_copies(g, slot, n):
                c.wait()
            w = n * crow
            lane = lax.broadcasted_iota(jnp.int32, (nh, w), 1)
            rq = [pl.ds(pl.multiple_of((g * SEQ + s) * nh, nh), nh) for s in range(SEQ)]
            for s in range(SEQ):
                q = qs[rq[s], :].astype(BF16)
                k = kb[slot, s, 0:w, :]
                ss[s * nh:(s + 1) * nh, 0:w] = lax.dot_general(
                    q, k, (((1,), (1,)), ((), ())), preferred_element_type=F32)
            for s in range(SEQ):
                sc = ss[s * nh:(s + 1) * nh, 0:w] * (hd ** -0.5) + bias[:, 0:w]
                sc = jnp.where(lane < lens[g * SEQ + s] * kvh, sc, NEG)
                m = jnp.max(sc, axis=1, keepdims=True)
                p = jnp.exp(sc - m)
                ps[s * nh:(s + 1) * nh, 0:w] = (p * (1.0 / jnp.sum(p, axis=1, keepdims=True))).astype(BF16)
            for s in range(SEQ):
                o = jnp.dot(ps[s * nh:(s + 1) * nh, 0:w], vb[slot, s, 0:w, :], preferred_element_type=F32)
                os[rq[s], :] = o.astype(BF16).astype(F32)
        by_class(g, go)
        pl.when(g + KVBUF < ngrp)(lambda: start_kv(g + KVBUF))

        @pl.when(g + KVBUF >= ngrp)
        def _():
            for i in range(per):
                wo_copy((g + KVBUF - ngrp) * per + i).start()
        return 0

    lax.fori_loop(0, ngrp, group, 0)

    for j in range(nh):
        ob[:, j * hd:(j + 1) * hd] = os[pl.ds(j, b, stride=nh), :].astype(BF16)

    def ostep(i, _):
        wo_copy(i).wait()
        c = pl.ds(pl.multiple_of(i * co, co), co)
        attn = jnp.dot(ob[...], wob[:, c], preferred_element_type=F32)
        hf[:, c] = (x[:, c].astype(F32) + attn).astype(BF16)
        return 0

    lax.fori_loop(0, nwo, ostep, 0)
    h = hf[...]
    h_out[...] = h
    u_out[...] = _rms(h, ln2[...])


def _attention(x, kv_k, kv_v, lens, idx, gates, ln1, ln2, wq, wo):
    b, d = x.shape
    _, l, kvh, hd = kv_k.shape
    hdim = wq.shape[1]
    nh = hdim // hd
    rows = l * kvh
    kk = kv_k.reshape(b, rows, hd)
    vv = kv_v.reshape(b, rows, hd)
    return pl.pallas_call(
        _attn_kernel,
        name="attn",
        out_shape=(pltpu.VMEM((b, d), BF16), pltpu.VMEM((b, d), BF16), pltpu.VMEM((2 * idx.shape[1], 128), F32)),
        in_specs=[_sm(), _vm(), _vm(), _vm(), _vm(), _vm(), _any(), _any(), _any(), _any()],
        out_specs=(_vm(), _vm(), _vm()),
        scratch_shapes=[
            pltpu.VMEM((d, hdim), BF16),
            pltpu.VMEM((hdim, d), BF16),
            pltpu.VMEM((KVBUF, SEQ, rows, hd), BF16),
            pltpu.VMEM((KVBUF, SEQ, rows, hd), BF16),
            pltpu.VMEM((b * nh, hd), F32),
            pltpu.VMEM((b * nh, hd), F32),
            pltpu.VMEM((b, hdim), BF16),
            pltpu.VMEM((nh, rows), F32),
            pltpu.VMEM((b, d), BF16),
            pltpu.VMEM((SEQ * nh, rows), F32),
            pltpu.VMEM((SEQ * nh, rows), BF16),
            pltpu.SemaphoreType.DMA((8,)),
            pltpu.SemaphoreType.DMA((8,)),
            pltpu.SemaphoreType.DMA((KVBUF,)),
            pltpu.SemaphoreType.DMA((KVBUF,)),
        ],
        compiler_params=pltpu.CompilerParams(vmem_limit_bytes=VLIM),
    )(lens, x, ln1, ln2, idx.T, gates.T, kk, vv, wq, wo)


def _places():
    cy = lax.axis_index("ey")
    cx = lax.axis_index("ex")
    xn = cy + 1 - 2 * lax.rem(cy, 2)
    yn = lax.rem(cy + 2, 4)
    dg = 3 - cy
    return cy, cx, (xn, yn, dg)


def _barrier(cy, cx, others):
    bar = pltpu.get_barrier_semaphore()
    for o in others:
        pl.semaphore_signal(bar, inc=1, device_id=(o, cx), device_id_type=MESH)
    pl.semaphore_signal(bar, inc=1, device_id=(cy, 1 - cx), device_id_type=MESH)
    pl.semaphore_wait(bar, len(others) + 1)


WBUF = 4
TILE = 128


def _silu_mul(z1, z3):
    return (z1 * jax.nn.sigmoid(z1) * z3).astype(BF16)


def _slot_copies(w1, w3, w2, b1, b3, b2, sem, e, slot):
    return (pltpu.make_async_copy(w1.at[e], b1.at[slot], sem.at[0, slot]),
            pltpu.make_async_copy(w3.at[e], b3.at[slot], sem.at[1, slot]),
            pltpu.make_async_copy(w2.at[e], b2.at[slot], sem.at[2, slot]))


def _gather_kernel(u, pk, w1, w3, w2, ua, posk, cols, b1, b3, b2,
                   pka, tmap, ps_sem, pr_sem, s_sem, r_sem, fs_sem, fr_sem, os_sem, or_sem, w_sem):
    blk, d = u.shape
    ntok = 8 * blk
    ne = w1.shape[0]
    top = 8
    cap = blk - blk // 8
    half = blk // 2
    cy, cx, others = _places()
    xn, yn, dg = others
    me = 2 * cy + cx

    ahead = [_slot_copies(w1, w3, w2, b1, b3, b2, w_sem, e, e) for e in range(WBUF)]
    for cs in ahead:
        for c in cs:
            c.start()

    _barrier(cy, cx, others)

    def table(src, slot, dev, i):
        return pltpu.make_async_remote_copy(
            src_ref=src, dst_ref=pka.at[slot], send_sem=ps_sem.at[i], recv_sem=pr_sem.at[i],
            device_id=dev, device_id_type=MESH)

    def rows(k):
        return pl.ds(k * half, half)

    def part(src, slot, k, dev, ss, rs, i):
        return pltpu.make_async_remote_copy(
            src_ref=src, dst_ref=ua.at[slot, rows(k)], send_sem=ss.at[i, k], recv_sem=rs.at[i, k],
            device_id=dev, device_id_type=MESH)

    partner = (cy, 1 - cx)
    for i in range(3):
        table(pk, me, (others[i], cx), i).start()
    table(pk, me, partner, 3).start()
    direct = [(1, 0), (0, 1), (1, 1), (0, 0)]
    for i, k in direct:
        part(u.at[rows(k)], me, k, (others[i], cx), s_sem, r_sem, i).start()
    for k in range(2):
        part(u.at[rows(k)], me, k, partner, os_sem, or_sem, 0).start()
    ua[me] = u[...]
    pka[me] = pk[...]

    for i in range(3):
        slot = 2 * others[i] + cx
        table(pk, slot, (others[i], cx), i).wait_recv()
        table(pka.at[slot], slot, partner, 4 + i).start()
    for i in range(3):
        slot = 2 * others[i] + cx
        table(pka.at[slot], slot, partner, 4 + i).wait()
        table(pk, me, (others[i], cx), i).wait_send()
    table(pk, me, partner, 3).wait()

    def tables():
        tmap[...] = jnp.concatenate([pka[k, :, 0:blk] for k in range(8)], axis=1)
        ids = (me * ne + lax.broadcasted_iota(jnp.int32, (ne, ntok), 0)).astype(F32)
        member = jnp.zeros((ne, ntok), F32)
        gate = jnp.zeros((ne, ntok), F32)
        for j in range(top):
            hit = tmap[j:j + 1, :] == ids
            member = member + jnp.where(hit, 1.0, 0.0)
            gate = gate + jnp.where(hit, tmap[top + j:top + j + 1, :], 0.0)
        ti = lax.broadcasted_iota(jnp.int32, (ntok, ntok), 0)
        tj = lax.broadcasted_iota(jnp.int32, (ntok, ntok), 1)
        tri = ti < tj
        tri_b = (tri & (ti // blk == tj // blk)).astype(F32).astype(BF16)
        rank = jnp.dot(member.astype(BF16), tri_b, preferred_element_type=F32)
        keep = jnp.where(rank < cap, member, 0.0)
        pos = jnp.dot(keep.astype(BF16), tri.astype(F32).astype(BF16), preferred_element_type=F32)
        pkeep = jnp.where(keep > 0, pos, -1.0)
        posk[...] = pkeep
        both = jnp.concatenate([pkeep, gate * keep, jnp.zeros((128 - 2 * ne, ntok), F32)], axis=0)
        cols[...] = jnp.transpose(both)

    def take(slot, k, dev, i):
        part(u.at[rows(k)], slot, k, dev, s_sem, r_sem, i).wait_recv()
        part(ua.at[slot, rows(k)], slot, k, partner, fs_sem, fr_sem, i).start()

    sx, sy, sd = 2 * xn + cx, 2 * yn + cx, 2 * dg + cx
    relay = {0: (sy, xn), 1: (sx, yn)}

    def across(k):
        slot, dev = relay[k]
        return part(ua.at[slot, rows(k)], slot, k, (dev, cx), s_sem, r_sem, 2)

    tables()
    take(sy, 0, (yn, cx), 1)
    across(0).start()
    take(sx, 1, (xn, cx), 0)
    across(1).start()
    take(sy, 1, (yn, cx), 1)
    take(sx, 0, (xn, cx), 0)
    for k in range(2):
        take(sd, k, (dg, cx), 2)
    for i, slot in ((1, sy), (0, sx), (2, sd)):
        for k in range(2):
            part(ua.at[slot, rows(k)], slot, k, partner, fs_sem, fr_sem, i).wait()
    for k in range(2):
        part(u.at[rows(k)], me, k, partner, os_sem, or_sem, 0).wait()
        across(k).wait_send()
        for i in range(2):
            part(u.at[rows(k)], me, k, (others[i], cx), s_sem, r_sem, i).wait_send()
    for cs in ahead:
        for c in cs:
            c.wait()


def _all_gather(u, pk, w1, w3, w2):
    b, d = u.shape
    ne, _, f = w1.shape
    return pl.pallas_call(
        _gather_kernel,
        name="gather",
        out_shape=(pltpu.VMEM((8, b, d), BF16),
                   pltpu.VMEM((ne, 8 * b), F32),
                   pltpu.VMEM((8 * b, 128), F32),
                   pltpu.VMEM((WBUF, d, f), BF16),
                   pltpu.VMEM((WBUF, d, f), BF16),
                   pltpu.VMEM((WBUF, f, d), BF16)),
        in_specs=[_vm(), _vm()] + [_hbm()] * 3,
        out_specs=(_vm(),) * 6,
        scratch_shapes=[
            pltpu.VMEM((8, pk.shape[0], 128), F32),
            pltpu.VMEM((pk.shape[0], 8 * b), F32),
            pltpu.SemaphoreType.DMA((7,)),
            pltpu.SemaphoreType.DMA((7,)),
            pltpu.SemaphoreType.DMA((3, 2)),
            pltpu.SemaphoreType.DMA((3, 2)),
            pltpu.SemaphoreType.DMA((3, 2)),
            pltpu.SemaphoreType.DMA((3, 2)),
            pltpu.SemaphoreType.DMA((1, 2)),
            pltpu.SemaphoreType.DMA((1, 2)),
            pltpu.SemaphoreType.DMA((3, WBUF)),
        ],
        compiler_params=pltpu.CompilerParams(
            collective_id=0, has_side_effects=True, vmem_limit_bytes=4 * 1024 * 1024),
    )(u, pk, w1, w3, w2)


def _expert_kernel(ua, posk, cols, i1, i3, i2, w1, w3, w2, acc, b1, b3, b2, xt, gt, rt, psc, gsc, cnt, order, sem):
    del i1, i3, i2
    ntok, d = ua.shape
    ne = w1.shape[0]
    f = w1.shape[2]
    fc = 256
    dc = 512

    def copies(e, slot):
        return _slot_copies(w1, w3, w2, b1, b3, b2, sem, e, slot)

    for e in range(ne):
        cnt[e] = (jnp.max(posk[e:e + 1, :]) + 1.0).astype(jnp.int32)
    for e in range(ne):
        if e < WBUF:
            order[e] = e
        else:
            place = jnp.int32(WBUF)
            for o in range(WBUF, ne):
                if o != e:
                    ahead = cnt[o] >= cnt[e] if o < e else cnt[o] > cnt[e]
                    place = place + ahead.astype(jnp.int32)
            order[place] = e

    def zero(i, _):
        acc[pl.ds(pl.multiple_of(i * 64, 64), 64), :] = jnp.zeros((64, d), F32)
        return 0
    lax.fori_loop(0, ntok // 64, zero, 0)

    def ffn(slot):
        for c in range(f // fc):
            s = slice(c * fc, (c + 1) * fc)
            z1 = jnp.dot(xt[...], b1[slot, :, s], preferred_element_type=F32)
            z3 = jnp.dot(xt[...], b3[slot, :, s], preferred_element_type=F32)
            gt[:, s] = _silu_mul(z1, z3)
        for c in range(d // dc):
            s = slice(c * dc, (c + 1) * dc)
            rt[:, s] = jnp.dot(gt[...], b2[slot, :, s], preferred_element_type=F32).astype(BF16)

    def expert(step, _):
        slot = lax.rem(step, WBUF)
        e = order[step]

        @pl.when(step >= WBUF)
        def _():
            for c in copies(e, slot):
                c.wait()
        n = cnt[e]
        lane = lax.broadcasted_iota(jnp.int32, (ntok, 128), 1)
        psc[...] = jnp.broadcast_to(
            jnp.sum(jnp.where(lane == e, cols[...], 0.0), axis=1, keepdims=True), (ntok, 128))
        gsc[...] = jnp.broadcast_to(
            jnp.sum(jnp.where(lane == e + ne, cols[...], 0.0), axis=1, keepdims=True), (ntok, 128))

        def packed(t, _):
            base = t * TILE
            want = (lax.broadcasted_iota(jnp.int32, (TILE, ntok), 0) + base).astype(F32)
            sel = (posk[pl.ds(e, 1), :] == want).astype(F32).astype(BF16)
            for c in range(d // dc):
                s = slice(c * dc, (c + 1) * dc)
                xt[:, s] = jnp.dot(sel, ua[:, s], preferred_element_type=F32).astype(BF16)
            ffn(slot)
            wantc = (lax.broadcasted_iota(jnp.int32, (ntok, TILE), 1) + base).astype(F32)
            selt = (psc[...] == wantc).astype(F32).astype(BF16)
            for c in range(d // 256):
                s = slice(c * 256, (c + 1) * 256)
                y = jnp.dot(selt, rt[:, s], preferred_element_type=F32)
                g = gsc[...]
                acc[:, c * 256:c * 256 + 128] += g * y[:, 0:128]
                acc[:, c * 256 + 128:(c + 1) * 256] += g * y[:, 128:256]
            return 0

        def dense(t, _):
            rows = pl.ds(pl.multiple_of(t * TILE, TILE), TILE)
            xt[...] = ua[rows, :]
            ffn(slot)
            g = gsc[rows, :]
            for c in range(d // 128):
                s = slice(c * 128, (c + 1) * 128)
                acc[rows, s] += g * rt[:, s].astype(F32)
            return 0

        many = n > 2 * TILE
        lax.fori_loop(0, jnp.where(many, 0, (n + TILE - 1) // TILE), packed, 0)
        lax.fori_loop(0, jnp.where(many, ntok // TILE, 0), dense, 0)

        @pl.when(step + WBUF < ne)
        def _():
            for c in copies(order[step + WBUF], slot):
                c.start()
        return 0

    lax.fori_loop(0, ne, expert, 0)


def _experts(ua, posk, cols, i1, i3, i2, w1, w3, w2):
    ntok, d = ua.shape
    ne, _, f = w1.shape
    return pl.pallas_call(
        _expert_kernel,
        name="experts",
        out_shape=(pltpu.VMEM((ntok, d), F32),
                   pltpu.VMEM((WBUF, d, f), BF16),
                   pltpu.VMEM((WBUF, d, f), BF16),
                   pltpu.VMEM((WBUF, f, d), BF16)),
        in_specs=[_vm()] * 6 + [_hbm()] * 3,
        out_specs=(_vm(),) * 4,
        input_output_aliases={3: 1, 4: 2, 5: 3},
        scratch_shapes=[
            pltpu.VMEM((TILE, d), BF16),
            pltpu.VMEM((TILE, f), BF16),
            pltpu.VMEM((TILE, d), BF16),
            pltpu.VMEM((ntok, 128), F32),
            pltpu.VMEM((ntok, 128), F32),
            pltpu.SMEM((ne,), jnp.int32),
            pltpu.SMEM((ne,), jnp.int32),
            pltpu.SemaphoreType.DMA((3, WBUF)),
        ],
        compiler_params=pltpu.CompilerParams(vmem_limit_bytes=6144 * 1024),
    )(ua, posk, cols, i1, i3, i2, w1, w3, w2)[0]


CH = 4


def _return_kernel(acc, h, u, ws1, ws3, ws2, y, rbuf, sbuf, abuf, tbuf, zbuf, hs, gt, v1, v3, v2,
                   ds_sem, dr_sem, s_sem, r_sem, ts_sem, tr_sem, v_sem):
    cy, cx, others = _places()
    xn, yn, dg = others
    d = acc.shape[3]
    f = gt.shape[1]
    w = d // CH
    n1 = xn * (1 - cx) + yn * cx
    n2 = yn * (1 - cx) + xn * cx

    shared = (pltpu.make_async_copy(ws1, v1, v_sem.at[0]),
              pltpu.make_async_copy(ws3, v3, v_sem.at[1]),
              pltpu.make_async_copy(ws2, v2, v_sem.at[2]))
    for c in shared:
        c.start()
    _barrier(cy, cx, others)

    def pair(c):
        return pltpu.make_async_remote_copy(
            src_ref=acc.at[:, 1 - cx, :, pl.ds(c * w, w)], dst_ref=rbuf.at[c],
            send_sem=ds_sem.at[c], recv_sem=dr_sem.at[c],
            device_id=(cy, 1 - cx), device_id_type=MESH)

    def first(c, i):
        return pltpu.make_async_remote_copy(
            src_ref=sbuf.at[c, dg if i else n1], dst_ref=abuf.at[c, i],
            send_sem=s_sem.at[c, i], recv_sem=r_sem.at[c, i],
            device_id=(n1, cx), device_id_type=MESH)

    def second(c):
        return pltpu.make_async_remote_copy(
            src_ref=tbuf.at[c], dst_ref=zbuf.at[c], send_sem=ts_sem.at[c], recv_sem=tr_sem.at[c],
            device_id=(n2, cx), device_id_type=MESH)

    for c in range(CH):
        pair(c).start()
    for c in range(CH):
        pair(c).wait_recv()
        for k in range(4):
            sbuf[c, k] = acc[k, cx, :, c * w:(c + 1) * w] + rbuf[c, k]
        for i in (1, 0):
            first(c, i).start()

    for c in shared:
        c.wait()
    for c in range(f // 256):
        s = slice(c * 256, (c + 1) * 256)
        z1 = jnp.dot(u[...], v1[:, s], preferred_element_type=F32)
        z3 = jnp.dot(u[...], v3[:, s], preferred_element_type=F32)
        gt[:, s] = _silu_mul(z1, z3)
    for c in range(d // 512):
        s = slice(c * 512, (c + 1) * 512)
        hs[:, s] = h[:, s].astype(F32) + jnp.dot(gt[...], v2[:, s], preferred_element_type=F32)

    for c in range(CH):
        first(c, 1).wait_recv()
        tbuf[c] = sbuf[c, n2] + abuf[c, 1]
        second(c).start()
    for c in range(CH):
        first(c, 0).wait_recv()
        second(c).wait_recv()
        s = slice(c * w, (c + 1) * w)
        y[:, s] = (hs[:, s] + sbuf[c, cy] + (abuf[c, 0] + zbuf[c])).astype(BF16)
    for c in range(CH):
        pair(c).wait_send()
        for i in range(2):
            first(c, i).wait_send()
        second(c).wait_send()


def _return(acc, h, u, ws1, ws3, ws2):
    b, d = h.shape
    f = ws1.shape[1]
    w = d // CH
    return pl.pallas_call(
        _return_kernel,
        name="giveback",
        out_shape=jax.ShapeDtypeStruct((b, d), BF16),
        in_specs=[_vm()] * 3 + [_hbm()] * 3,
        out_specs=_vm(),
        scratch_shapes=[
            pltpu.VMEM((CH, 4, b, w), F32),
            pltpu.VMEM((CH, 4, b, w), F32),
            pltpu.VMEM((CH, 2, b, w), F32),
            pltpu.VMEM((CH, b, w), F32),
            pltpu.VMEM((CH, b, w), F32),
            pltpu.VMEM((b, d), F32),
            pltpu.VMEM((b, f), BF16),
            pltpu.VMEM((d, f), BF16),
            pltpu.VMEM((d, f), BF16),
            pltpu.VMEM((f, d), BF16),
            pltpu.SemaphoreType.DMA((CH,)),
            pltpu.SemaphoreType.DMA((CH,)),
            pltpu.SemaphoreType.DMA((CH, 2)),
            pltpu.SemaphoreType.DMA((CH, 2)),
            pltpu.SemaphoreType.DMA((CH,)),
            pltpu.SemaphoreType.DMA((CH,)),
            pltpu.SemaphoreType.DMA((3,)),
        ],
        compiler_params=pltpu.CompilerParams(
            collective_id=1, has_side_effects=True, vmem_limit_bytes=20 * 1024 * 1024),
    )(acc, h, u, ws1, ws3, ws2)


def solution(mesh):
    def body(x, kv_k, kv_v, lens, idx, gates, ln1, wq, wo, ln2, ws1, ws3, ws2, w1, w3, w2):
        b, d = x.shape
        h, u, pk = _attention(x, kv_k, kv_v, lens, idx, gates, ln1, ln2, wq, wo)
        ua, posk, cols, b1, b3, b2 = _all_gather(u, pk, w1, w3, w2)
        acc = _experts(ua.reshape(8 * b, d), posk, cols, b1, b3, b2, w1, w3, w2)
        return _return(acc.reshape(4, 2, b, d), h, u, ws1, ws3, ws2)

    rows = P(GRP)
    rep = P()
    return jax.shard_map(
        body, mesh=mesh,
        in_specs=(rows, rows, rows, rows, rows, rows, rep, rep, rep, rep, rep, rep, rep, rows, rows, rows),
        out_specs=rows, check_vma=False)
```

```python
import functools

import jax
import jax.numpy as jnp
from jax import lax
from jax.experimental import pallas as pl
from jax.experimental.pallas import tpu as pltpu
from jax.sharding import PartitionSpec as P

EPS = 1e-6
GRP = ("ey", "ex")
MESH = pl.DeviceIdType.MESH
NEG = -1e30
F32 = jnp.float32
BF16 = jnp.bfloat16
VLIM = 55 * 1024 * 1024


def _vm():
    return pl.BlockSpec(memory_space=pltpu.VMEM)


def _sm():
    return pl.BlockSpec(memory_space=pltpu.SMEM)


def _hbm():
    return pl.BlockSpec(memory_space=pltpu.HBM)


def _any():
    return pl.BlockSpec(memory_space=pl.ANY)


def _rms(v, w):
    v32 = v.astype(F32)
    r = lax.rsqrt(jnp.mean(v32 * v32, axis=-1, keepdims=True) + EPS)
    return (v32 * r * w.astype(F32)).astype(BF16)


SEQ = 8
KVBUF = 4
STEP = 64


def _attn_kernel(lens, x, ln1, ln2, idx, gates, kk, vv, wq, wo, h_out, u_out, pk_out,
                 wqb, wob, kb, vb, qs, os, ob, bias, hf, ss, ps, wq_sem, wo_sem, k_sem, v_sem):
    b, d = x.shape
    heads_dim = wqb.shape[1]
    hd = 128
    nh = heads_dim // hd
    rows = kk.shape[1]
    kvh = 4
    seqlen = rows // kvh
    ncls = seqlen // STEP
    crow = STEP * kvh
    ngrp = b // SEQ
    nwq = wq_sem.shape[0]
    nwo = wo_sem.shape[0]
    cq = heads_dim // nwq
    co = d // nwo

    def wq_copy(i):
        c = pl.ds(pl.multiple_of(i * cq, cq), cq)
        return pltpu.make_async_copy(wq.at[:, c], wqb.at[:, c], wq_sem.at[i])

    def wo_copy(i):
        c = pl.ds(pl.multiple_of(i * co, co), co)
        return pltpu.make_async_copy(wo.at[:, c], wob.at[:, c], wo_sem.at[i])

    def gmax(g):
        m = lens[g * SEQ]
        for s in range(1, SEQ):
            m = jnp.maximum(m, lens[g * SEQ + s])
        return m

    def kv_copies(g, slot, n):
        src = (pl.ds(g * SEQ, SEQ), pl.ds(0, n * crow))
        dst = (slot, slice(None), pl.ds(0, n * crow))
        return (pltpu.make_async_copy(kk.at[src], kb.at[dst], k_sem.at[slot]),
                pltpu.make_async_copy(vv.at[src], vb.at[dst], v_sem.at[slot]))

    def by_class(g, f):
        cls = (gmax(g) + STEP - 1) // STEP
        for n in range(1, ncls + 1):
            pl.when(cls == n)(functools.partial(f, n))

    def start_kv(g):
        slot = lax.rem(g, KVBUF)

        def go(n):
            for c in kv_copies(g, slot, n):
                c.start()
        by_class(g, go)

    for i in range(nwq):
        wq_copy(i).start()
    lax.fori_loop(0, min(KVBUF, ngrp), lambda g, _: (start_kv(g), 0)[1], 0)
    table = jnp.concatenate([idx[...].astype(F32), gates[...]], axis=0)
    pk_out[...] = jnp.concatenate([table, jnp.zeros((table.shape[0], 128 - b), F32)], axis=1)
    col = lax.broadcasted_iota(jnp.int32, (nh, rows), 1)
    row = lax.broadcasted_iota(jnp.int32, (nh, rows), 0)
    bias[...] = jnp.where(lax.rem(col, kvh) == row // (nh // kvh), 0.0, NEG)

    a = _rms(x[...], ln1[...])

    def qstep(i, _):
        wq_copy(i).wait()
        w = wqb[:, pl.ds(pl.multiple_of(i * cq, cq), cq)]
        q = jnp.dot(a, w, preferred_element_type=F32).astype(BF16).astype(F32)
        for j in range(cq // hd):
            qs[pl.ds(i * (cq // hd) + j, b, stride=nh), :] = q[:, j * hd:(j + 1) * hd]
        return 0

    lax.fori_loop(0, nwq, qstep, 0)
    per = nwo // min(KVBUF, ngrp)

    def group(g, _):
        slot = lax.rem(g, KVBUF)

        def go(n):
            for c in kv_copies(g, slot, n):
                c.wait()
            w = n * crow
            lane = lax.broadcasted_iota(jnp.int32, (nh, w), 1)
            rq = [pl.ds(pl.multiple_of((g * SEQ + s) * nh, nh), nh) for s in range(SEQ)]
            for s in range(SEQ):
                q = qs[rq[s], :].astype(BF16)
                k = kb[slot, s, 0:w, :]
                ss[s * nh:(s + 1) * nh, 0:w] = lax.dot_general(
                    q, k, (((1,), (1,)), ((), ())), preferred_element_type=F32)
            for s in range(SEQ):
                sc = ss[s * nh:(s + 1) * nh, 0:w] * (hd ** -0.5) + bias[:, 0:w]
                sc = jnp.where(lane < lens[g * SEQ + s] * kvh, sc, NEG)
                m = jnp.max(sc, axis=1, keepdims=True)
                p = jnp.exp(sc - m)
                ps[s * nh:(s + 1) * nh, 0:w] = (p * (1.0 / jnp.sum(p, axis=1, keepdims=True))).astype(BF16)
            for s in range(SEQ):
                o = jnp.dot(ps[s * nh:(s + 1) * nh, 0:w], vb[slot, s, 0:w, :], preferred_element_type=F32)
                os[rq[s], :] = o.astype(BF16).astype(F32)
        by_class(g, go)
        pl.when(g + KVBUF < ngrp)(lambda: start_kv(g + KVBUF))

        @pl.when(g + KVBUF >= ngrp)
        def _():
            for i in range(per):
                wo_copy((g + KVBUF - ngrp) * per + i).start()
        return 0

    lax.fori_loop(0, ngrp, group, 0)

    for j in range(nh):
        ob[:, j * hd:(j + 1) * hd] = os[pl.ds(j, b, stride=nh), :].astype(BF16)

    def ostep(i, _):
        wo_copy(i).wait()
        c = pl.ds(pl.multiple_of(i * co, co), co)
        attn = jnp.dot(ob[...], wob[:, c], preferred_element_type=F32)
        hf[:, c] = (x[:, c].astype(F32) + attn).astype(BF16)
        return 0

    lax.fori_loop(0, nwo, ostep, 0)
    h = hf[...]
    h_out[...] = h
    u_out[...] = _rms(h, ln2[...])


def _attention(x, kv_k, kv_v, lens, idx, gates, ln1, ln2, wq, wo):
    b, d = x.shape
    _, l, kvh, hd = kv_k.shape
    hdim = wq.shape[1]
    nh = hdim // hd
    rows = l * kvh
    kk = kv_k.reshape(b, rows, hd)
    vv = kv_v.reshape(b, rows, hd)
    return pl.pallas_call(
        _attn_kernel,
        name="attn",
        out_shape=(pltpu.VMEM((b, d), BF16), pltpu.VMEM((b, d), BF16), pltpu.VMEM((2 * idx.shape[1], 128), F32)),
        in_specs=[_sm(), _vm(), _vm(), _vm(), _vm(), _vm(), _any(), _any(), _any(), _any()],
        out_specs=(_vm(), _vm(), _vm()),
        scratch_shapes=[
            pltpu.VMEM((d, hdim), BF16),
            pltpu.VMEM((hdim, d), BF16),
            pltpu.VMEM((KVBUF, SEQ, rows, hd), BF16),
            pltpu.VMEM((KVBUF, SEQ, rows, hd), BF16),
            pltpu.VMEM((b * nh, hd), F32),
            pltpu.VMEM((b * nh, hd), F32),
            pltpu.VMEM((b, hdim), BF16),
            pltpu.VMEM((nh, rows), F32),
            pltpu.VMEM((b, d), BF16),
            pltpu.VMEM((SEQ * nh, rows), F32),
            pltpu.VMEM((SEQ * nh, rows), BF16),
            pltpu.SemaphoreType.DMA((8,)),
            pltpu.SemaphoreType.DMA((8,)),
            pltpu.SemaphoreType.DMA((KVBUF,)),
            pltpu.SemaphoreType.DMA((KVBUF,)),
        ],
        compiler_params=pltpu.CompilerParams(vmem_limit_bytes=VLIM),
    )(lens, x, ln1, ln2, idx.T, gates.T, kk, vv, wq, wo)


def _places():
    cy = lax.axis_index("ey")
    cx = lax.axis_index("ex")
    xn = cy + 1 - 2 * lax.rem(cy, 2)
    yn = lax.rem(cy + 2, 4)
    dg = 3 - cy
    return cy, cx, (xn, yn, dg)


def _barrier(cy, cx, others):
    bar = pltpu.get_barrier_semaphore()
    for o in others:
        pl.semaphore_signal(bar, inc=1, device_id=(o, cx), device_id_type=MESH)
    pl.semaphore_signal(bar, inc=1, device_id=(cy, 1 - cx), device_id_type=MESH)
    pl.semaphore_wait(bar, len(others) + 1)


WBUF = 4
TILE = 128
SMALL = 64
LANES = 16
STEP8 = 8


def _silu_mul(z1, z3):
    return (z1 * jax.nn.sigmoid(z1) * z3).astype(BF16)


def _slot_copies(w1, w3, w2, b1, b3, b2, sem, e, slot):
    return (pltpu.make_async_copy(w1.at[e], b1.at[slot], sem.at[0, slot]),
            pltpu.make_async_copy(w3.at[e], b3.at[slot], sem.at[1, slot]),
            pltpu.make_async_copy(w2.at[e], b2.at[slot], sem.at[2, slot]))


def _gather_kernel(u, pk, w1, w3, w2, ua, toks, wgts, cols, b1, b3, b2,
                   pka, tmap, ps_sem, pr_sem, s_sem, r_sem, fs_sem, fr_sem, os_sem, or_sem, w_sem):
    blk, d = u.shape
    ntok = 8 * blk
    ne = w1.shape[0]
    top = 8
    cap = blk - blk // 8
    half = blk // 2
    cy, cx, others = _places()
    xn, yn, dg = others
    me = 2 * cy + cx

    ahead = [_slot_copies(w1, w3, w2, b1, b3, b2, w_sem, e, e) for e in range(WBUF)]
    for cs in ahead:
        for c in cs:
            c.start()

    _barrier(cy, cx, others)

    def table(src, slot, dev, i):
        return pltpu.make_async_remote_copy(
            src_ref=src, dst_ref=pka.at[slot], send_sem=ps_sem.at[i], recv_sem=pr_sem.at[i],
            device_id=dev, device_id_type=MESH)

    def rows(k):
        return pl.ds(k * half, half)

    def part(src, slot, k, dev, ss, rs, i):
        return pltpu.make_async_remote_copy(
            src_ref=src, dst_ref=ua.at[slot, rows(k)], send_sem=ss.at[i, k], recv_sem=rs.at[i, k],
            device_id=dev, device_id_type=MESH)

    partner = (cy, 1 - cx)
    for i in range(3):
        table(pk, me, (others[i], cx), i).start()
    table(pk, me, partner, 3).start()
    direct = [(1, 0), (0, 1), (1, 1), (0, 0)]
    for i, k in direct:
        part(u.at[rows(k)], me, k, (others[i], cx), s_sem, r_sem, i).start()
    for k in range(2):
        part(u.at[rows(k)], me, k, partner, os_sem, or_sem, 0).start()
    ua[me] = u[...]
    pka[me] = pk[...]

    for i in range(3):
        slot = 2 * others[i] + cx
        table(pk, slot, (others[i], cx), i).wait_recv()
        table(pka.at[slot], slot, partner, 4 + i).start()
    for i in range(3):
        slot = 2 * others[i] + cx
        table(pka.at[slot], slot, partner, 4 + i).wait()
        table(pk, me, (others[i], cx), i).wait_send()
    table(pk, me, partner, 3).wait()

    def tables():
        tmap[...] = jnp.concatenate([pka[k, :, 0:blk] for k in range(8)], axis=1)
        ids = (me * ne + lax.broadcasted_iota(jnp.int32, (ne, ntok), 0)).astype(F32)
        member = jnp.zeros((ne, ntok), F32)
        gate = jnp.zeros((ne, ntok), F32)
        for j in range(top):
            hit = tmap[j:j + 1, :] == ids
            member = member + jnp.where(hit, 1.0, 0.0)
            gate = gate + jnp.where(hit, tmap[top + j:top + j + 1, :], 0.0)
        ti = lax.broadcasted_iota(jnp.int32, (ntok, ntok), 0)
        tj = lax.broadcasted_iota(jnp.int32, (ntok, ntok), 1)
        tri = ti < tj
        tri_b = (tri & (ti // blk == tj // blk)).astype(F32).astype(BF16)
        rank = jnp.dot(member.astype(BF16), tri_b, preferred_element_type=F32)
        keep = jnp.where(rank < cap, member, 0.0)
        pos = jnp.dot(keep.astype(BF16), tri.astype(F32).astype(BF16), preferred_element_type=F32)
        pkeep = jnp.where(keep > 0, pos, -1.0)
        gkeep = gate * keep
        both = jnp.concatenate([gkeep, jnp.zeros((128 - ne, ntok), F32)], axis=0)
        cols[...] = jnp.transpose(both)
        place = lax.broadcasted_iota(jnp.int32, (SMALL, ntok), 0).astype(F32)
        tok = lax.broadcasted_iota(jnp.int32, (SMALL, ntok), 1).astype(F32) - ntok
        lane = lax.broadcasted_iota(jnp.int32, (SMALL, 128), 1)
        lists = jnp.zeros((SMALL, 128), F32)
        for e in range(ne):
            hit = pkeep[e:e + 1, :] == place
            t = jnp.sum(jnp.where(hit, tok, 0.0), axis=1, keepdims=True)
            g = jnp.sum(jnp.where(hit, gkeep[e:e + 1, :], 0.0), axis=1, keepdims=True)
            lists = lists + jnp.where(lane == e, t, 0.0) + jnp.where(lane == ne + e, g, 0.0)
        lists = jnp.transpose(jnp.concatenate([lists, jnp.zeros((128 - SMALL, 128), F32)], axis=0))
        count = jnp.sum(keep, axis=1, keepdims=True)
        last = lax.broadcasted_iota(jnp.int32, (ne, 128), 1) == 127
        toks[...] = jnp.where(last, count, lists[0:ne, :] + ntok).astype(jnp.int32)
        wgts[...] = lists[ne:2 * ne, :]

    def take(slot, k, dev, i):
        part(u.at[rows(k)], slot, k, dev, s_sem, r_sem, i).wait_recv()
        part(ua.at[slot, rows(k)], slot, k, partner, fs_sem, fr_sem, i).start()

    sx, sy, sd = 2 * xn + cx, 2 * yn + cx, 2 * dg + cx
    relay = {0: (sy, xn), 1: (sx, yn)}

    def across(k):
        slot, dev = relay[k]
        return part(ua.at[slot, rows(k)], slot, k, (dev, cx), s_sem, r_sem, 2)

    tables()
    take(sy, 0, (yn, cx), 1)
    across(0).start()
    take(sx, 1, (xn, cx), 0)
    across(1).start()
    take(sy, 1, (yn, cx), 1)
    take(sx, 0, (xn, cx), 0)
    for k in range(2):
        take(sd, k, (dg, cx), 2)
    for i, slot in ((1, sy), (0, sx), (2, sd)):
        for k in range(2):
            part(ua.at[slot, rows(k)], slot, k, partner, fs_sem, fr_sem, i).wait()
    for k in range(2):
        part(u.at[rows(k)], me, k, partner, os_sem, or_sem, 0).wait()
        across(k).wait_send()
        for i in range(2):
            part(u.at[rows(k)], me, k, (others[i], cx), s_sem, r_sem, i).wait_send()
    for cs in ahead:
        for c in cs:
            c.wait()


def _all_gather(u, pk, w1, w3, w2):
    b, d = u.shape
    ne, _, f = w1.shape
    return pl.pallas_call(
        _gather_kernel,
        name="gather",
        out_shape=(pltpu.VMEM((8, b, d), BF16),
                   jax.ShapeDtypeStruct((ne, 128), jnp.int32),
                   jax.ShapeDtypeStruct((ne, 128), F32),
                   pltpu.VMEM((8 * b, 128), F32),
                   pltpu.VMEM((WBUF, d, f), BF16),
                   pltpu.VMEM((WBUF, d, f), BF16),
                   pltpu.VMEM((WBUF, f, d), BF16)),
        in_specs=[_vm(), _vm()] + [_hbm()] * 3,
        out_specs=(_vm(),) * 7,
        scratch_shapes=[
            pltpu.VMEM((8, pk.shape[0], 128), F32),
            pltpu.VMEM((pk.shape[0], 8 * b), F32),
            pltpu.SemaphoreType.DMA((7,)),
            pltpu.SemaphoreType.DMA((7,)),
            pltpu.SemaphoreType.DMA((3, 2)),
            pltpu.SemaphoreType.DMA((3, 2)),
            pltpu.SemaphoreType.DMA((3, 2)),
            pltpu.SemaphoreType.DMA((3, 2)),
            pltpu.SemaphoreType.DMA((1, 2)),
            pltpu.SemaphoreType.DMA((1, 2)),
            pltpu.SemaphoreType.DMA((3, WBUF)),
        ],
        compiler_params=pltpu.CompilerParams(
            collective_id=0, has_side_effects=True, vmem_limit_bytes=4 * 1024 * 1024),
    )(u, pk, w1, w3, w2)


def _expert_kernel(toks, wgts, ua, cols, i1, i3, i2, w1, w3, w2, acc, b1, b3, b2,
                   ua3, x3, r3, xt, gt, rt, gsc, order, sem):
    del i1, i3, i2
    ntok, d = ua.shape
    ne = w1.shape[0]
    f = w1.shape[2]
    fc = 256
    dc = 512

    def copies(e, slot):
        return _slot_copies(w1, w3, w2, b1, b3, b2, sem, e, slot)

    for e in range(ne):
        if e < WBUF:
            order[e] = e
        else:
            place = jnp.int32(WBUF)
            for o in range(WBUF, ne):
                if o != e:
                    ahead = toks[o, 127] >= toks[e, 127] if o < e else toks[o, 127] > toks[e, 127]
                    place = place + ahead.astype(jnp.int32)
            order[place] = e

    for c in range(LANES):
        ua3[pl.ds(c, ntok, stride=LANES), :] = ua[:, c * 128:(c + 1) * 128].astype(F32)
    ua3[ntok * LANES:, :] = jnp.zeros((STEP8 * LANES, 128), F32)

    def zero(i, _):
        acc[pl.ds(pl.multiple_of(i * 256, 256), 256), :] = jnp.zeros((256, 128), F32)
        return 0
    lax.fori_loop(0, ntok * LANES // 256, zero, 0)
    acc[ntok * LANES:, :] = jnp.zeros((STEP8 * LANES, 128), F32)

    def hidden(slot, m):
        for c in range(f // fc):
            s = slice(c * fc, (c + 1) * fc)
            z1 = jnp.dot(xt[0:m, :], b1[slot, :, s], preferred_element_type=F32)
            z3 = jnp.dot(xt[0:m, :], b3[slot, :, s], preferred_element_type=F32)
            gt[0:m, s] = _silu_mul(z1, z3)

    def result(slot, m, c):
        return jnp.dot(gt[0:m, :], b2[slot, :, c * dc:(c + 1) * dc], preferred_element_type=F32).astype(BF16)

    def at(t):
        return pl.ds(pl.multiple_of(t * LANES, LANES), LANES)

    def expert(step, _):
        slot = lax.rem(step, WBUF)
        e = order[step]

        @pl.when(step >= WBUF)
        def _():
            for c in copies(e, slot):
                c.wait()
        n = toks[e, 127]

        @pl.when((n > 0) & (n <= SMALL))
        def _():
            steps = (n + STEP8 - 1) // STEP8

            def fetch(i, _):
                for k in range(STEP8):
                    m = i * STEP8 + k
                    x3[at(m), :] = ua3[at(toks[e, m]), :]
                return 0
            lax.fori_loop(0, steps, fetch, 0)
            for c in range(LANES):
                xt[0:SMALL, c * 128:(c + 1) * 128] = x3[pl.ds(c, SMALL, stride=LANES), :].astype(BF16)
            hidden(slot, SMALL)
            for c in range(d // dc):
                y = result(slot, SMALL, c).astype(F32)
                for j in range(dc // 128):
                    r3[pl.ds(c * (dc // 128) + j, SMALL, stride=LANES), :] = y[:, j * 128:(j + 1) * 128]

            def add(i, _):
                where = [at(toks[e, i * STEP8 + k]) for k in range(STEP8)]
                new = [acc[where[k], :] + wgts[e, i * STEP8 + k] * r3[at(i * STEP8 + k), :] for k in range(STEP8)]
                for k in range(STEP8):
                    acc[where[k], :] = new[k]
                return 0
            lax.fori_loop(0, steps, add, 0)

        @pl.when(n > SMALL)
        def _():
            lane = lax.broadcasted_iota(jnp.int32, (ntok, 128), 1)
            gsc[...] = jnp.broadcast_to(
                jnp.sum(jnp.where(lane == e, cols[...], 0.0), axis=1, keepdims=True), (ntok, 128))

            def dense(t, _):
                rows = pl.ds(pl.multiple_of(t * TILE, TILE), TILE)
                xt[...] = ua[rows, :]
                hidden(slot, TILE)
                for c in range(d // dc):
                    rt[:, c * dc:(c + 1) * dc] = result(slot, TILE, c)
                g = gsc[rows, :]
                for c in range(LANES):
                    where = pl.ds(t * (TILE * LANES) + c, TILE, stride=LANES)
                    acc[where, :] = acc[where, :] + g * rt[:, c * 128:(c + 1) * 128].astype(F32)
                return 0
            lax.fori_loop(0, ntok // TILE, dense, 0)

        @pl.when(step + WBUF < ne)
        def _():
            for c in copies(order[step + WBUF], slot):
                c.start()
        return 0

    lax.fori_loop(0, ne, expert, 0)


def _experts(toks, wgts, ua, cols, i1, i3, i2, w1, w3, w2):
    ntok, d = ua.shape
    ne, _, f = w1.shape
    return pl.pallas_call(
        _expert_kernel,
        name="experts",
        out_shape=(pltpu.VMEM(((ntok + STEP8) * LANES, 128), F32),
                   pltpu.VMEM((WBUF, d, f), BF16),
                   pltpu.VMEM((WBUF, d, f), BF16),
                   pltpu.VMEM((WBUF, f, d), BF16)),
        in_specs=[_sm()] * 2 + [_vm()] * 5 + [_hbm()] * 3,
        out_specs=(_vm(),) * 4,
        input_output_aliases={4: 1, 5: 2, 6: 3},
        scratch_shapes=[
            pltpu.VMEM(((ntok + STEP8) * LANES, 128), F32),
            pltpu.VMEM((SMALL * LANES, 128), F32),
            pltpu.VMEM((SMALL * LANES, 128), F32),
            pltpu.VMEM((TILE, d), BF16),
            pltpu.VMEM((TILE, f), BF16),
            pltpu.VMEM((TILE, d), BF16),
            pltpu.VMEM((ntok, 128), F32),
            pltpu.SMEM((ne,), jnp.int32),
            pltpu.SemaphoreType.DMA((3, WBUF)),
        ],
        compiler_params=pltpu.CompilerParams(vmem_limit_bytes=8 * 1024 * 1024),
    )(toks, wgts, ua, cols, i1, i3, i2, w1, w3, w2)[0]


CH = 4


def _return_kernel(acc, h, u, ws1, ws3, ws2, y, rbuf, sbuf, abuf, tbuf, zbuf, tot, hs, gt, v1, v3, v2,
                   ds_sem, dr_sem, s_sem, r_sem, ts_sem, tr_sem, v_sem):
    cy, cx, others = _places()
    xn, yn, dg = others
    b, d = h.shape
    f = gt.shape[1]
    per = b // CH
    w = per * LANES
    n1 = xn * (1 - cx) + yn * cx
    n2 = yn * (1 - cx) + xn * cx

    shared = (pltpu.make_async_copy(ws1, v1, v_sem.at[0]),
              pltpu.make_async_copy(ws3, v3, v_sem.at[1]),
              pltpu.make_async_copy(ws2, v2, v_sem.at[2]))
    for c in shared:
        c.start()
    _barrier(cy, cx, others)

    def piece(k, core, c):
        return pl.ds((2 * k + core) * (b * LANES) + c * w, w)

    def pair(c, k):
        return pltpu.make_async_remote_copy(
            src_ref=acc.at[piece(k, 1 - cx, c)], dst_ref=rbuf.at[c, k],
            send_sem=ds_sem.at[c, k], recv_sem=dr_sem.at[c, k],
            device_id=(cy, 1 - cx), device_id_type=MESH)

    def first(c, i):
        return pltpu.make_async_remote_copy(
            src_ref=sbuf.at[c, dg if i else n1], dst_ref=abuf.at[c, i],
            send_sem=s_sem.at[c, i], recv_sem=r_sem.at[c, i],
            device_id=(n1, cx), device_id_type=MESH)

    def second(c):
        return pltpu.make_async_remote_copy(
            src_ref=tbuf.at[c], dst_ref=zbuf.at[c], send_sem=ts_sem.at[c], recv_sem=tr_sem.at[c],
            device_id=(n2, cx), device_id_type=MESH)

    for c in range(CH):
        for k in range(4):
            pair(c, k).start()
    for c in range(CH):
        for k in range(4):
            pair(c, k).wait_recv()
            sbuf[c, k] = acc[piece(k, cx, c), :] + rbuf[c, k]
        for i in (1, 0):
            first(c, i).start()

    for c in shared:
        c.wait()
    for c in range(f // 256):
        s = slice(c * 256, (c + 1) * 256)
        z1 = jnp.dot(u[...], v1[:, s], preferred_element_type=F32)
        z3 = jnp.dot(u[...], v3[:, s], preferred_element_type=F32)
        gt[:, s] = _silu_mul(z1, z3)
    for c in range(d // 512):
        s = slice(c * 512, (c + 1) * 512)
        hs[:, s] = h[:, s].astype(F32) + jnp.dot(gt[...], v2[:, s], preferred_element_type=F32)

    for c in range(CH):
        first(c, 1).wait_recv()
        tbuf[c] = sbuf[c, n2] + abuf[c, 1]
        second(c).start()
    for c in range(CH):
        first(c, 0).wait_recv()
        second(c).wait_recv()
        tot[...] = sbuf[c, cy] + (abuf[c, 0] + zbuf[c])
        r = slice(c * per, (c + 1) * per)
        for j in range(LANES):
            s = slice(j * 128, (j + 1) * 128)
            y[r, s] = (hs[r, s] + tot[pl.ds(j, per, stride=LANES), :]).astype(BF16)
    for c in range(CH):
        for k in range(4):
            pair(c, k).wait_send()
        for i in range(2):
            first(c, i).wait_send()
        second(c).wait_send()


def _return(acc, h, u, ws1, ws3, ws2):
    b, d = h.shape
    f = ws1.shape[1]
    w = b // CH * LANES
    return pl.pallas_call(
        _return_kernel,
        name="giveback",
        out_shape=jax.ShapeDtypeStruct((b, d), BF16),
        in_specs=[_vm()] * 3 + [_hbm()] * 3,
        out_specs=_vm(),
        scratch_shapes=[
            pltpu.VMEM((CH, 4, w, 128), F32),
            pltpu.VMEM((CH, 4, w, 128), F32),
            pltpu.VMEM((CH, 2, w, 128), F32),
            pltpu.VMEM((CH, w, 128), F32),
            pltpu.VMEM((CH, w, 128), F32),
            pltpu.VMEM((w, 128), F32),
            pltpu.VMEM((b, d), F32),
            pltpu.VMEM((b, f), BF16),
            pltpu.VMEM((d, f), BF16),
            pltpu.VMEM((d, f), BF16),
            pltpu.VMEM((f, d), BF16),
            pltpu.SemaphoreType.DMA((CH, 4)),
            pltpu.SemaphoreType.DMA((CH, 4)),
            pltpu.SemaphoreType.DMA((CH, 2)),
            pltpu.SemaphoreType.DMA((CH, 2)),
            pltpu.SemaphoreType.DMA((CH,)),
            pltpu.SemaphoreType.DMA((CH,)),
            pltpu.SemaphoreType.DMA((3,)),
        ],
        compiler_params=pltpu.CompilerParams(
            collective_id=1, has_side_effects=True, vmem_limit_bytes=20 * 1024 * 1024),
    )(acc, h, u, ws1, ws3, ws2)


def solution(mesh):
    def body(x, kv_k, kv_v, lens, idx, gates, ln1, wq, wo, ln2, ws1, ws3, ws2, w1, w3, w2):
        b, d = x.shape
        h, u, pk = _attention(x, kv_k, kv_v, lens, idx, gates, ln1, ln2, wq, wo)
        ua, toks, wgts, cols, b1, b3, b2 = _all_gather(u, pk, w1, w3, w2)
        acc = _experts(toks, wgts, ua.reshape(8 * b, d), cols, b1, b3, b2, w1, w3, w2)
        return _return(acc, h, u, ws1, ws3, ws2)

    rows = P(GRP)
    rep = P()
    return jax.shard_map(
        body, mesh=mesh,
        in_specs=(rows, rows, rows, rows, rows, rows, rep, rep, rep, rep, rep, rep, rep, rows, rows, rows),
        out_specs=rows, check_vma=False)
```

```python
import functools

import jax
import jax.numpy as jnp
from jax import lax
from jax.experimental import pallas as pl
from jax.experimental.pallas import tpu as pltpu
from jax.sharding import PartitionSpec as P

EPS = 1e-6
GRP = ("ey", "ex")
MESH = pl.DeviceIdType.MESH
NEG = -1e30
F32 = jnp.float32
BF16 = jnp.bfloat16
VLIM = 55 * 1024 * 1024


def _vm():
    return pl.BlockSpec(memory_space=pltpu.VMEM)


def _sm():
    return pl.BlockSpec(memory_space=pltpu.SMEM)


def _hbm():
    return pl.BlockSpec(memory_space=pltpu.HBM)


def _any():
    return pl.BlockSpec(memory_space=pl.ANY)


def _rms(v, w):
    v32 = v.astype(F32)
    r = lax.rsqrt(jnp.mean(v32 * v32, axis=-1, keepdims=True) + EPS)
    return (v32 * r * w.astype(F32)).astype(BF16)


SEQ = 8
KVBUF = 4
STEP = 64


def _attn_kernel(lens, x, ln1, ln2, idx, gates, kk, vv, wq, wo, h_out, u_out, pk_out,
                 wqb, wob, kb, vb, qs, os, ob, bias, hf, ss, ps, wq_sem, wo_sem, k_sem, v_sem):
    b, d = x.shape
    heads_dim = wqb.shape[1]
    hd = 128
    nh = heads_dim // hd
    rows = kk.shape[1]
    kvh = 4
    seqlen = rows // kvh
    ncls = seqlen // STEP
    crow = STEP * kvh
    ngrp = b // SEQ
    nwq = wq_sem.shape[0]
    nwo = wo_sem.shape[0]
    cq = heads_dim // nwq
    co = d // nwo

    def wq_copy(i):
        c = pl.ds(pl.multiple_of(i * cq, cq), cq)
        return pltpu.make_async_copy(wq.at[:, c], wqb.at[:, c], wq_sem.at[i])

    def wo_copy(i):
        c = pl.ds(pl.multiple_of(i * co, co), co)
        return pltpu.make_async_copy(wo.at[:, c], wob.at[:, c], wo_sem.at[i])

    def gmax(g):
        m = lens[g * SEQ]
        for s in range(1, SEQ):
            m = jnp.maximum(m, lens[g * SEQ + s])
        return m

    def kv_copies(g, slot, n):
        src = (pl.ds(g * SEQ, SEQ), pl.ds(0, n * crow))
        dst = (slot, slice(None), pl.ds(0, n * crow))
        return (pltpu.make_async_copy(kk.at[src], kb.at[dst], k_sem.at[slot]),
                pltpu.make_async_copy(vv.at[src], vb.at[dst], v_sem.at[slot]))

    def by_class(g, f):
        cls = (gmax(g) + STEP - 1) // STEP
        for n in range(1, ncls + 1):
            pl.when(cls == n)(functools.partial(f, n))

    def start_kv(g):
        slot = lax.rem(g, KVBUF)

        def go(n):
            for c in kv_copies(g, slot, n):
                c.start()
        by_class(g, go)

    for i in range(nwq):
        wq_copy(i).start()
    lax.fori_loop(0, min(KVBUF, ngrp), lambda g, _: (start_kv(g), 0)[1], 0)
    table = jnp.concatenate([idx[...].astype(F32), gates[...]], axis=0)
    pk_out[...] = jnp.concatenate([table, jnp.zeros((table.shape[0], 128 - b), F32)], axis=1)
    col = lax.broadcasted_iota(jnp.int32, (nh, rows), 1)
    row = lax.broadcasted_iota(jnp.int32, (nh, rows), 0)
    bias[...] = jnp.where(lax.rem(col, kvh) == row // (nh // kvh), 0.0, NEG)

    a = _rms(x[...], ln1[...])

    def qstep(i, _):
        wq_copy(i).wait()
        w = wqb[:, pl.ds(pl.multiple_of(i * cq, cq), cq)]
        q = jnp.dot(a, w, preferred_element_type=F32).astype(BF16).astype(F32)
        for j in range(cq // hd):
            qs[pl.ds(i * (cq // hd) + j, b, stride=nh), :] = q[:, j * hd:(j + 1) * hd]
        return 0

    lax.fori_loop(0, nwq, qstep, 0)
    per = nwo // min(KVBUF, ngrp)

    def group(g, _):
        slot = lax.rem(g, KVBUF)

        def go(n):
            for c in kv_copies(g, slot, n):
                c.wait()
            w = n * crow
            lane = lax.broadcasted_iota(jnp.int32, (nh, w), 1)
            rq = [pl.ds(pl.multiple_of((g * SEQ + s) * nh, nh), nh) for s in range(SEQ)]
            for s in range(SEQ):
                q = qs[rq[s], :].astype(BF16)
                k = kb[slot, s, 0:w, :]
                ss[s * nh:(s + 1) * nh, 0:w] = lax.dot_general(
                    q, k, (((1,), (1,)), ((), ())), preferred_element_type=F32)
            for s in range(SEQ):
                sc = ss[s * nh:(s + 1) * nh, 0:w] * (hd ** -0.5) + bias[:, 0:w]
                sc = jnp.where(lane < lens[g * SEQ + s] * kvh, sc, NEG)
                m = jnp.max(sc, axis=1, keepdims=True)
                p = jnp.exp(sc - m)
                ps[s * nh:(s + 1) * nh, 0:w] = (p * (1.0 / jnp.sum(p, axis=1, keepdims=True))).astype(BF16)
            for s in range(SEQ):
                o = jnp.dot(ps[s * nh:(s + 1) * nh, 0:w], vb[slot, s, 0:w, :], preferred_element_type=F32)
                os[rq[s], :] = o.astype(BF16).astype(F32)
        by_class(g, go)
        pl.when(g + KVBUF < ngrp)(lambda: start_kv(g + KVBUF))

        @pl.when(g + KVBUF >= ngrp)
        def _():
            for i in range(per):
                wo_copy((g + KVBUF - ngrp) * per + i).start()
        return 0

    lax.fori_loop(0, ngrp, group, 0)

    for j in range(nh):
        ob[:, j * hd:(j + 1) * hd] = os[pl.ds(j, b, stride=nh), :].astype(BF16)

    def ostep(i, _):
        wo_copy(i).wait()
        c = pl.ds(pl.multiple_of(i * co, co), co)
        attn = jnp.dot(ob[...], wob[:, c], preferred_element_type=F32)
        hf[:, c] = (x[:, c].astype(F32) + attn).astype(BF16)
        return 0

    lax.fori_loop(0, nwo, ostep, 0)
    h = hf[...]
    h_out[...] = h
    u_out[...] = _rms(h, ln2[...])


def _attention(x, kv_k, kv_v, lens, idx, gates, ln1, ln2, wq, wo):
    b, d = x.shape
    _, l, kvh, hd = kv_k.shape
    hdim = wq.shape[1]
    nh = hdim // hd
    rows = l * kvh
    kk = kv_k.reshape(b, rows, hd)
    vv = kv_v.reshape(b, rows, hd)
    return pl.pallas_call(
        _attn_kernel,
        name="attn",
        out_shape=(pltpu.VMEM((b, d), BF16), pltpu.VMEM((b, d), BF16), pltpu.VMEM((2 * idx.shape[1], 128), F32)),
        in_specs=[_sm(), _vm(), _vm(), _vm(), _vm(), _vm(), _any(), _any(), _any(), _any()],
        out_specs=(_vm(), _vm(), _vm()),
        scratch_shapes=[
            pltpu.VMEM((d, hdim), BF16),
            pltpu.VMEM((hdim, d), BF16),
            pltpu.VMEM((KVBUF, SEQ, rows, hd), BF16),
            pltpu.VMEM((KVBUF, SEQ, rows, hd), BF16),
            pltpu.VMEM((b * nh, hd), F32),
            pltpu.VMEM((b * nh, hd), F32),
            pltpu.VMEM((b, hdim), BF16),
            pltpu.VMEM((nh, rows), F32),
            pltpu.VMEM((b, d), BF16),
            pltpu.VMEM((SEQ * nh, rows), F32),
            pltpu.VMEM((SEQ * nh, rows), BF16),
            pltpu.SemaphoreType.DMA((8,)),
            pltpu.SemaphoreType.DMA((8,)),
            pltpu.SemaphoreType.DMA((KVBUF,)),
            pltpu.SemaphoreType.DMA((KVBUF,)),
        ],
        compiler_params=pltpu.CompilerParams(vmem_limit_bytes=VLIM),
    )(lens, x, ln1, ln2, idx.T, gates.T, kk, vv, wq, wo)


def _places():
    cy = lax.axis_index("ey")
    cx = lax.axis_index("ex")
    xn = cy + 1 - 2 * lax.rem(cy, 2)
    yn = lax.rem(cy + 2, 4)
    dg = 3 - cy
    return cy, cx, (xn, yn, dg)


def _barrier(cy, cx, others):
    bar = pltpu.get_barrier_semaphore()
    for o in others:
        pl.semaphore_signal(bar, inc=1, device_id=(o, cx), device_id_type=MESH)
    pl.semaphore_signal(bar, inc=1, device_id=(cy, 1 - cx), device_id_type=MESH)
    pl.semaphore_wait(bar, len(others) + 1)


WBUF = 4
TILE = 128
SMALL = 64
LANES = 16
STEP8 = 8


def _silu_mul(z1, z3):
    return (z1 * jax.nn.sigmoid(z1) * z3).astype(BF16)


def _slot_copies(w1, w3, w2, b1, b3, b2, sem, e, slot):
    return (pltpu.make_async_copy(w1.at[e], b1.at[slot], sem.at[0, slot]),
            pltpu.make_async_copy(w3.at[e], b3.at[slot], sem.at[1, slot]),
            pltpu.make_async_copy(w2.at[e], b2.at[slot], sem.at[2, slot]))


def _gather_kernel(u, pk, w1, w3, w2, ua, toks, wgts, cols, b1, b3, b2,
                   pka, tmap, ps_sem, pr_sem, s_sem, r_sem, fs_sem, fr_sem, os_sem, or_sem, w_sem):
    blk, d = u.shape
    ntok = 8 * blk
    ne = w1.shape[0]
    top = 8
    cap = blk - blk // 8
    half = blk // 2
    cy, cx, others = _places()
    xn, yn, dg = others
    me = 2 * cy + cx

    ahead = [_slot_copies(w1, w3, w2, b1, b3, b2, w_sem, e, e) for e in range(WBUF)]
    for cs in ahead:
        for c in cs:
            c.start()

    _barrier(cy, cx, others)

    def table(src, slot, dev, i):
        return pltpu.make_async_remote_copy(
            src_ref=src, dst_ref=pka.at[slot], send_sem=ps_sem.at[i], recv_sem=pr_sem.at[i],
            device_id=dev, device_id_type=MESH)

    def rows(k):
        return pl.ds(k * half, half)

    def part(src, slot, k, dev, ss, rs, i):
        return pltpu.make_async_remote_copy(
            src_ref=src, dst_ref=ua.at[slot, rows(k)], send_sem=ss.at[i, k], recv_sem=rs.at[i, k],
            device_id=dev, device_id_type=MESH)

    partner = (cy, 1 - cx)
    for i in range(3):
        table(pk, me, (others[i], cx), i).start()
    table(pk, me, partner, 3).start()
    direct = [(1, 0), (0, 1), (1, 1), (0, 0)]
    for i, k in direct:
        part(u.at[rows(k)], me, k, (others[i], cx), s_sem, r_sem, i).start()
    for k in range(2):
        part(u.at[rows(k)], me, k, partner, os_sem, or_sem, 0).start()
    ua[me] = u[...]
    pka[me] = pk[...]

    for i in range(3):
        slot = 2 * others[i] + cx
        table(pk, slot, (others[i], cx), i).wait_recv()
        table(pka.at[slot], slot, partner, 4 + i).start()
    for i in range(3):
        slot = 2 * others[i] + cx
        table(pka.at[slot], slot, partner, 4 + i).wait()
        table(pk, me, (others[i], cx), i).wait_send()
    table(pk, me, partner, 3).wait()

    def tables():
        tmap[...] = jnp.concatenate([pka[k, :, 0:blk] for k in range(8)], axis=1)
        ids = (me * ne + lax.broadcasted_iota(jnp.int32, (ne, ntok), 0)).astype(F32)
        member = jnp.zeros((ne, ntok), F32)
        gate = jnp.zeros((ne, ntok), F32)
        for j in range(top):
            hit = tmap[j:j + 1, :] == ids
            member = member + jnp.where(hit, 1.0, 0.0)
            gate = gate + jnp.where(hit, tmap[top + j:top + j + 1, :], 0.0)
        ti = lax.broadcasted_iota(jnp.int32, (ntok, ntok), 0)
        tj = lax.broadcasted_iota(jnp.int32, (ntok, ntok), 1)
        tri = ti < tj
        tri_b = (tri & (ti // blk == tj // blk)).astype(F32).astype(BF16)
        rank = jnp.dot(member.astype(BF16), tri_b, preferred_element_type=F32)
        keep = jnp.where(rank < cap, member, 0.0)
        pos = jnp.dot(keep.astype(BF16), tri.astype(F32).astype(BF16), preferred_element_type=F32)
        pkeep = jnp.where(keep > 0, pos, -1.0)
        gkeep = gate * keep
        both = jnp.concatenate([gkeep, jnp.zeros((128 - ne, ntok), F32)], axis=0)
        cols[...] = jnp.transpose(both)
        place = lax.broadcasted_iota(jnp.int32, (SMALL, ntok), 0).astype(F32)
        tok = lax.broadcasted_iota(jnp.int32, (SMALL, ntok), 1).astype(F32) - ntok
        lane = lax.broadcasted_iota(jnp.int32, (SMALL, 128), 1)
        lists = jnp.zeros((SMALL, 128), F32)
        for e in range(ne):
            hit = pkeep[e:e + 1, :] == place
            t = jnp.sum(jnp.where(hit, tok, 0.0), axis=1, keepdims=True)
            g = jnp.sum(jnp.where(hit, gkeep[e:e + 1, :], 0.0), axis=1, keepdims=True)
            lists = lists + jnp.where(lane == e, t, 0.0) + jnp.where(lane == ne + e, g, 0.0)
        lists = jnp.transpose(jnp.concatenate([lists, jnp.zeros((128 - SMALL, 128), F32)], axis=0))
        count = jnp.sum(keep, axis=1, keepdims=True)
        last = lax.broadcasted_iota(jnp.int32, (ne, 128), 1) == 127
        toks[...] = jnp.where(last, count, lists[0:ne, :] + ntok).astype(jnp.int32)
        wgts[...] = lists[ne:2 * ne, :]

    def take(slot, k, dev, i):
        part(u.at[rows(k)], slot, k, dev, s_sem, r_sem, i).wait_recv()
        part(ua.at[slot, rows(k)], slot, k, partner, fs_sem, fr_sem, i).start()

    sx, sy, sd = 2 * xn + cx, 2 * yn + cx, 2 * dg + cx
    relay = {0: (sy, xn), 1: (sx, yn)}

    def across(k):
        slot, dev = relay[k]
        return part(ua.at[slot, rows(k)], slot, k, (dev, cx), s_sem, r_sem, 2)

    tables()
    take(sy, 0, (yn, cx), 1)
    across(0).start()
    take(sx, 1, (xn, cx), 0)
    across(1).start()
    take(sy, 1, (yn, cx), 1)
    take(sx, 0, (xn, cx), 0)
    for k in range(2):
        take(sd, k, (dg, cx), 2)
    for i, slot in ((1, sy), (0, sx), (2, sd)):
        for k in range(2):
            part(ua.at[slot, rows(k)], slot, k, partner, fs_sem, fr_sem, i).wait()
    for k in range(2):
        part(u.at[rows(k)], me, k, partner, os_sem, or_sem, 0).wait()
        across(k).wait_send()
        for i in range(2):
            part(u.at[rows(k)], me, k, (others[i], cx), s_sem, r_sem, i).wait_send()
    for cs in ahead:
        for c in cs:
            c.wait()


def _all_gather(u, pk, w1, w3, w2):
    b, d = u.shape
    ne, _, f = w1.shape
    return pl.pallas_call(
        _gather_kernel,
        name="gather",
        out_shape=(pltpu.VMEM((8, b, d), BF16),
                   jax.ShapeDtypeStruct((ne, 128), jnp.int32),
                   jax.ShapeDtypeStruct((ne, 128), F32),
                   pltpu.VMEM((8 * b, 128), F32),
                   pltpu.VMEM((WBUF, d, f), BF16),
                   pltpu.VMEM((WBUF, d, f), BF16),
                   pltpu.VMEM((WBUF, f, d), BF16)),
        in_specs=[_vm(), _vm()] + [_hbm()] * 3,
        out_specs=(_vm(),) * 7,
        scratch_shapes=[
            pltpu.VMEM((8, pk.shape[0], 128), F32),
            pltpu.VMEM((pk.shape[0], 8 * b), F32),
            pltpu.SemaphoreType.DMA((7,)),
            pltpu.SemaphoreType.DMA((7,)),
            pltpu.SemaphoreType.DMA((3, 2)),
            pltpu.SemaphoreType.DMA((3, 2)),
            pltpu.SemaphoreType.DMA((3, 2)),
            pltpu.SemaphoreType.DMA((3, 2)),
            pltpu.SemaphoreType.DMA((1, 2)),
            pltpu.SemaphoreType.DMA((1, 2)),
            pltpu.SemaphoreType.DMA((3, WBUF)),
        ],
        compiler_params=pltpu.CompilerParams(
            collective_id=0, has_side_effects=True, vmem_limit_bytes=4 * 1024 * 1024),
    )(u, pk, w1, w3, w2)


def _expert_kernel(toks, wgts, ua, cols, i1, i3, i2, w1, w3, w2, acc, b1, b3, b2,
                   ua3, x3, r3, xt, gt, rt, gsc, order, seat, sem):
    del i1, i3, i2
    ntok, d = ua.shape
    ne = w1.shape[0]
    f = w1.shape[2]
    fc = 256
    dc = 512

    def copies(e, slot):
        return _slot_copies(w1, w3, w2, b1, b3, b2, sem, e, slot)

    spread = [5, 9, 12, 7, 10, 4, 6, 8, 11, 13, 14, 15]
    for k in range(ne - WBUF):
        seat[k] = spread[k]
    for e in range(ne):
        if e < WBUF:
            order[e] = e
        else:
            rank = jnp.int32(0)
            for o in range(WBUF, ne):
                if o != e:
                    ahead = toks[o, 127] >= toks[e, 127] if o < e else toks[o, 127] > toks[e, 127]
                    rank = rank + ahead.astype(jnp.int32)
            order[seat[rank]] = e

    for c in range(LANES):
        ua3[pl.ds(c, ntok, stride=LANES), :] = ua[:, c * 128:(c + 1) * 128].astype(F32)
    ua3[ntok * LANES:, :] = jnp.zeros((STEP8 * LANES, 128), F32)

    def zero(i, _):
        acc[pl.ds(pl.multiple_of(i * 256, 256), 256), :] = jnp.zeros((256, 128), F32)
        return 0
    lax.fori_loop(0, ntok * LANES // 256, zero, 0)
    acc[ntok * LANES:, :] = jnp.zeros((STEP8 * LANES, 128), F32)

    def hidden(slot, m):
        for c in range(f // fc):
            s = slice(c * fc, (c + 1) * fc)
            z1 = jnp.dot(xt[0:m, :], b1[slot, :, s], preferred_element_type=F32)
            z3 = jnp.dot(xt[0:m, :], b3[slot, :, s], preferred_element_type=F32)
            gt[0:m, s] = _silu_mul(z1, z3)

    def result(slot, m, c):
        return jnp.dot(gt[0:m, :], b2[slot, :, c * dc:(c + 1) * dc], preferred_element_type=F32).astype(BF16)

    def at(t):
        return pl.ds(pl.multiple_of(t * LANES, LANES), LANES)

    def expert(step, _):
        slot = lax.rem(step, WBUF)
        e = order[step]

        @pl.when(step >= WBUF)
        def _():
            for c in copies(e, slot):
                c.wait()
        n = toks[e, 127]

        @pl.when((n > 0) & (n <= SMALL))
        def _():
            steps = (n + STEP8 - 1) // STEP8

            def fetch(i, _):
                for k in range(STEP8):
                    m = i * STEP8 + k
                    x3[at(m), :] = ua3[at(toks[e, m]), :]
                return 0
            lax.fori_loop(0, steps, fetch, 0)
            for c in range(LANES):
                xt[0:SMALL, c * 128:(c + 1) * 128] = x3[pl.ds(c, SMALL, stride=LANES), :].astype(BF16)
            hidden(slot, SMALL)
            for c in range(d // dc):
                y = result(slot, SMALL, c).astype(F32)
                for j in range(dc // 128):
                    r3[pl.ds(c * (dc // 128) + j, SMALL, stride=LANES), :] = y[:, j * 128:(j + 1) * 128]

            def add(i, _):
                where = [at(toks[e, i * STEP8 + k]) for k in range(STEP8)]
                new = [acc[where[k], :] + wgts[e, i * STEP8 + k] * r3[at(i * STEP8 + k), :] for k in range(STEP8)]
                for k in range(STEP8):
                    acc[where[k], :] = new[k]
                return 0
            lax.fori_loop(0, steps, add, 0)

        @pl.when(n > SMALL)
        def _():
            lane = lax.broadcasted_iota(jnp.int32, (ntok, 128), 1)
            gsc[...] = jnp.broadcast_to(
                jnp.sum(jnp.where(lane == e, cols[...], 0.0), axis=1, keepdims=True), (ntok, 128))

            def dense(t, _):
                rows = pl.ds(pl.multiple_of(t * TILE, TILE), TILE)
                xt[...] = ua[rows, :]
                hidden(slot, TILE)
                for c in range(d // dc):
                    rt[:, c * dc:(c + 1) * dc] = result(slot, TILE, c)
                g = gsc[rows, :]
                for c in range(LANES):
                    where = pl.ds(t * (TILE * LANES) + c, TILE, stride=LANES)
                    acc[where, :] = acc[where, :] + g * rt[:, c * 128:(c + 1) * 128].astype(F32)
                return 0
            lax.fori_loop(0, ntok // TILE, dense, 0)

        @pl.when(step + WBUF < ne)
        def _():
            for c in copies(order[step + WBUF], slot):
                c.start()
        return 0

    lax.fori_loop(0, ne, expert, 0)


def _experts(toks, wgts, ua, cols, i1, i3, i2, w1, w3, w2):
    ntok, d = ua.shape
    ne, _, f = w1.shape
    return pl.pallas_call(
        _expert_kernel,
        name="experts",
        out_shape=(pltpu.VMEM(((ntok + STEP8) * LANES, 128), F32),
                   pltpu.VMEM((WBUF, d, f), BF16),
                   pltpu.VMEM((WBUF, d, f), BF16),
                   pltpu.VMEM((WBUF, f, d), BF16)),
        in_specs=[_sm()] * 2 + [_vm()] * 5 + [_hbm()] * 3,
        out_specs=(_vm(),) * 4,
        input_output_aliases={4: 1, 5: 2, 6: 3},
        scratch_shapes=[
            pltpu.VMEM(((ntok + STEP8) * LANES, 128), F32),
            pltpu.VMEM((SMALL * LANES, 128), F32),
            pltpu.VMEM((SMALL * LANES, 128), F32),
            pltpu.VMEM((TILE, d), BF16),
            pltpu.VMEM((TILE, f), BF16),
            pltpu.VMEM((TILE, d), BF16),
            pltpu.VMEM((ntok, 128), F32),
            pltpu.SMEM((ne,), jnp.int32),
            pltpu.SMEM((ne,), jnp.int32),
            pltpu.SemaphoreType.DMA((3, WBUF)),
        ],
        compiler_params=pltpu.CompilerParams(vmem_limit_bytes=8 * 1024 * 1024),
    )(toks, wgts, ua, cols, i1, i3, i2, w1, w3, w2)[0]


CH = 4


def _return_kernel(acc, h, u, ws1, ws3, ws2, y, rbuf, sbuf, abuf, tbuf, zbuf, tot, hs, gt, v1, v3, v2,
                   ds_sem, dr_sem, s_sem, r_sem, ts_sem, tr_sem, v_sem):
    cy, cx, others = _places()
    xn, yn, dg = others
    b, d = h.shape
    f = gt.shape[1]
    per = b // CH
    w = per * LANES
    n1 = xn * (1 - cx) + yn * cx
    n2 = yn * (1 - cx) + xn * cx

    shared = (pltpu.make_async_copy(ws1, v1, v_sem.at[0]),
              pltpu.make_async_copy(ws3, v3, v_sem.at[1]),
              pltpu.make_async_copy(ws2, v2, v_sem.at[2]))
    for c in shared:
        c.start()
    _barrier(cy, cx, others)

    def piece(k, core, c):
        return pl.ds((2 * k + core) * (b * LANES) + c * w, w)

    def pair(c, k):
        return pltpu.make_async_remote_copy(
            src_ref=acc.at[piece(k, 1 - cx, c)], dst_ref=rbuf.at[c, k],
            send_sem=ds_sem.at[c, k], recv_sem=dr_sem.at[c, k],
            device_id=(cy, 1 - cx), device_id_type=MESH)

    def first(c, i):
        return pltpu.make_async_remote_copy(
            src_ref=sbuf.at[c, dg if i else n1], dst_ref=abuf.at[c, i],
            send_sem=s_sem.at[c, i], recv_sem=r_sem.at[c, i],
            device_id=(n1, cx), device_id_type=MESH)

    def second(c):
        return pltpu.make_async_remote_copy(
            src_ref=tbuf.at[c], dst_ref=zbuf.at[c], send_sem=ts_sem.at[c], recv_sem=tr_sem.at[c],
            device_id=(n2, cx), device_id_type=MESH)

    for c in range(CH):
        for k in range(4):
            pair(c, k).start()
    for c in range(CH):
        for k in range(4):
            pair(c, k).wait_recv()
            sbuf[c, k] = acc[piece(k, cx, c), :] + rbuf[c, k]
        for i in (1, 0):
            first(c, i).start()

    for c in shared:
        c.wait()
    for c in range(f // 256):
        s = slice(c * 256, (c + 1) * 256)
        z1 = jnp.dot(u[...], v1[:, s], preferred_element_type=F32)
        z3 = jnp.dot(u[...], v3[:, s], preferred_element_type=F32)
        gt[:, s] = _silu_mul(z1, z3)
    for c in range(d // 512):
        s = slice(c * 512, (c + 1) * 512)
        hs[:, s] = h[:, s].astype(F32) + jnp.dot(gt[...], v2[:, s], preferred_element_type=F32)

    for c in range(CH):
        first(c, 1).wait_recv()
        tbuf[c] = sbuf[c, n2] + abuf[c, 1]
        second(c).start()
    for c in range(CH):
        first(c, 0).wait_recv()
        second(c).wait_recv()
        tot[...] = sbuf[c, cy] + (abuf[c, 0] + zbuf[c])
        r = slice(c * per, (c + 1) * per)
        for j in range(LANES):
            s = slice(j * 128, (j + 1) * 128)
            y[r, s] = (hs[r, s] + tot[pl.ds(j, per, stride=LANES), :]).astype(BF16)
    for c in range(CH):
        for k in range(4):
            pair(c, k).wait_send()
        for i in range(2):
            first(c, i).wait_send()
        second(c).wait_send()


def _return(acc, h, u, ws1, ws3, ws2):
    b, d = h.shape
    f = ws1.shape[1]
    w = b // CH * LANES
    return pl.pallas_call(
        _return_kernel,
        name="giveback",
        out_shape=jax.ShapeDtypeStruct((b, d), BF16),
        in_specs=[_vm()] * 3 + [_hbm()] * 3,
        out_specs=_vm(),
        scratch_shapes=[
            pltpu.VMEM((CH, 4, w, 128), F32),
            pltpu.VMEM((CH, 4, w, 128), F32),
            pltpu.VMEM((CH, 2, w, 128), F32),
            pltpu.VMEM((CH, w, 128), F32),
            pltpu.VMEM((CH, w, 128), F32),
            pltpu.VMEM((w, 128), F32),
            pltpu.VMEM((b, d), F32),
            pltpu.VMEM((b, f), BF16),
            pltpu.VMEM((d, f), BF16),
            pltpu.VMEM((d, f), BF16),
            pltpu.VMEM((f, d), BF16),
            pltpu.SemaphoreType.DMA((CH, 4)),
            pltpu.SemaphoreType.DMA((CH, 4)),
            pltpu.SemaphoreType.DMA((CH, 2)),
            pltpu.SemaphoreType.DMA((CH, 2)),
            pltpu.SemaphoreType.DMA((CH,)),
            pltpu.SemaphoreType.DMA((CH,)),
            pltpu.SemaphoreType.DMA((3,)),
        ],
        compiler_params=pltpu.CompilerParams(
            collective_id=1, has_side_effects=True, vmem_limit_bytes=20 * 1024 * 1024),
    )(acc, h, u, ws1, ws3, ws2)


def solution(mesh):
    def body(x, kv_k, kv_v, lens, idx, gates, ln1, wq, wo, ln2, ws1, ws3, ws2, w1, w3, w2):
        b, d = x.shape
        h, u, pk = _attention(x, kv_k, kv_v, lens, idx, gates, ln1, ln2, wq, wo)
        ua, toks, wgts, cols, b1, b3, b2 = _all_gather(u, pk, w1, w3, w2)
        acc = _experts(toks, wgts, ua.reshape(8 * b, d), cols, b1, b3, b2, w1, w3, w2)
        return _return(acc, h, u, ws1, ws3, ws2)

    rows = P(GRP)
    rep = P()
    return jax.shard_map(
        body, mesh=mesh,
        in_specs=(rows, rows, rows, rows, rows, rows, rep, rep, rep, rep, rep, rep, rep, rows, rows, rows),
        out_specs=rows, check_vma=False)
```

```python
import functools

import jax
import jax.numpy as jnp
from jax import lax
from jax.experimental import pallas as pl
from jax.experimental.pallas import tpu as pltpu
from jax.sharding import PartitionSpec as P

EPS = 1e-6
GRP = ("ey", "ex")
MESH = pl.DeviceIdType.MESH
NEG = -1e30
F32 = jnp.float32
BF16 = jnp.bfloat16
VLIM = 55 * 1024 * 1024


def _vm():
    return pl.BlockSpec(memory_space=pltpu.VMEM)


def _sm():
    return pl.BlockSpec(memory_space=pltpu.SMEM)


def _hbm():
    return pl.BlockSpec(memory_space=pltpu.HBM)


def _any():
    return pl.BlockSpec(memory_space=pl.ANY)


def _rms(v, w):
    v32 = v.astype(F32)
    r = lax.rsqrt(jnp.mean(v32 * v32, axis=-1, keepdims=True) + EPS)
    return (v32 * r * w.astype(F32)).astype(BF16)


SEQ = 8
KVBUF = 4
STEP = 64


def _attn_kernel(lens, x, ln1, ln2, idx, gates, kk, vv, wq, wo, h_out, u_out, pk_out,
                 wqb, wob, kb, vb, qs, os, ob, bias, hf, ss, ps, wq_sem, wo_sem, k_sem, v_sem):
    b, d = x.shape
    heads_dim = wqb.shape[1]
    hd = 128
    nh = heads_dim // hd
    rows = kk.shape[1]
    kvh = 4
    seqlen = rows // kvh
    ncls = seqlen // STEP
    crow = STEP * kvh
    ngrp = b // SEQ
    nwq = wq_sem.shape[0]
    nwo = wo_sem.shape[0]
    cq = heads_dim // nwq
    co = d // nwo

    def wq_copy(i):
        c = pl.ds(pl.multiple_of(i * cq, cq), cq)
        return pltpu.make_async_copy(wq.at[:, c], wqb.at[:, c], wq_sem.at[i])

    def wo_copy(i):
        c = pl.ds(pl.multiple_of(i * co, co), co)
        return pltpu.make_async_copy(wo.at[:, c], wob.at[:, c], wo_sem.at[i])

    def gmax(g):
        m = lens[g * SEQ]
        for s in range(1, SEQ):
            m = jnp.maximum(m, lens[g * SEQ + s])
        return m

    def kv_copies(g, slot, n):
        src = (pl.ds(g * SEQ, SEQ), pl.ds(0, n * crow))
        dst = (slot, slice(None), pl.ds(0, n * crow))
        return (pltpu.make_async_copy(kk.at[src], kb.at[dst], k_sem.at[slot]),
                pltpu.make_async_copy(vv.at[src], vb.at[dst], v_sem.at[slot]))

    def by_class(g, f):
        cls = (gmax(g) + STEP - 1) // STEP
        for n in range(1, ncls + 1):
            pl.when(cls == n)(functools.partial(f, n))

    def start_kv(g):
        slot = lax.rem(g, KVBUF)

        def go(n):
            for c in kv_copies(g, slot, n):
                c.start()
        by_class(g, go)

    for i in range(nwq):
        wq_copy(i).start()
    lax.fori_loop(0, min(KVBUF, ngrp), lambda g, _: (start_kv(g), 0)[1], 0)
    table = jnp.concatenate([idx[...].astype(F32), gates[...]], axis=0)
    pk_out[...] = jnp.concatenate([table, jnp.zeros((table.shape[0], 128 - b), F32)], axis=1)
    col = lax.broadcasted_iota(jnp.int32, (nh, rows), 1)
    row = lax.broadcasted_iota(jnp.int32, (nh, rows), 0)
    bias[...] = jnp.where(lax.rem(col, kvh) == row // (nh // kvh), 0.0, NEG)

    a = _rms(x[...], ln1[...])

    def qstep(i, _):
        wq_copy(i).wait()
        w = wqb[:, pl.ds(pl.multiple_of(i * cq, cq), cq)]
        q = jnp.dot(a, w, preferred_element_type=F32).astype(BF16).astype(F32)
        for j in range(cq // hd):
            qs[pl.ds(i * (cq // hd) + j, b, stride=nh), :] = q[:, j * hd:(j + 1) * hd]
        return 0

    lax.fori_loop(0, nwq, qstep, 0)
    per = nwo // min(KVBUF, ngrp)

    def group(g, _):
        slot = lax.rem(g, KVBUF)

        def go(n):
            for c in kv_copies(g, slot, n):
                c.wait()
            w = n * crow
            lane = lax.broadcasted_iota(jnp.int32, (nh, w), 1)
            rq = [pl.ds(pl.multiple_of((g * SEQ + s) * nh, nh), nh) for s in range(SEQ)]
            for s in range(SEQ):
                q = qs[rq[s], :].astype(BF16)
                k = kb[slot, s, 0:w, :]
                ss[s * nh:(s + 1) * nh, 0:w] = lax.dot_general(
                    q, k, (((1,), (1,)), ((), ())), preferred_element_type=F32)
            for s in range(SEQ):
                sc = ss[s * nh:(s + 1) * nh, 0:w] * (hd ** -0.5) + bias[:, 0:w]
                sc = jnp.where(lane < lens[g * SEQ + s] * kvh, sc, NEG)
                m = jnp.max(sc, axis=1, keepdims=True)
                p = jnp.exp(sc - m)
                ps[s * nh:(s + 1) * nh, 0:w] = (p * (1.0 / jnp.sum(p, axis=1, keepdims=True))).astype(BF16)
            for s in range(SEQ):
                o = jnp.dot(ps[s * nh:(s + 1) * nh, 0:w], vb[slot, s, 0:w, :], preferred_element_type=F32)
                os[rq[s], :] = o.astype(BF16).astype(F32)
        by_class(g, go)
        pl.when(g + KVBUF < ngrp)(lambda: start_kv(g + KVBUF))

        @pl.when(g + KVBUF >= ngrp)
        def _():
            for i in range(per):
                wo_copy((g + KVBUF - ngrp) * per + i).start()
        return 0

    lax.fori_loop(0, ngrp, group, 0)

    for j in range(nh):
        ob[:, j * hd:(j + 1) * hd] = os[pl.ds(j, b, stride=nh), :].astype(BF16)

    def ostep(i, _):
        wo_copy(i).wait()
        c = pl.ds(pl.multiple_of(i * co, co), co)
        attn = jnp.dot(ob[...], wob[:, c], preferred_element_type=F32)
        hf[:, c] = (x[:, c].astype(F32) + attn).astype(BF16)
        return 0

    lax.fori_loop(0, nwo, ostep, 0)
    h = hf[...]
    h_out[...] = h
    u_out[...] = _rms(h, ln2[...])


def _attention(x, kv_k, kv_v, lens, idx, gates, ln1, ln2, wq, wo):
    b, d = x.shape
    _, l, kvh, hd = kv_k.shape
    hdim = wq.shape[1]
    nh = hdim // hd
    rows = l * kvh
    kk = kv_k.reshape(b, rows, hd)
    vv = kv_v.reshape(b, rows, hd)
    return pl.pallas_call(
        _attn_kernel,
        name="attn",
        out_shape=(pltpu.VMEM((b, d), BF16), pltpu.VMEM((b, d), BF16), pltpu.VMEM((2 * idx.shape[1], 128), F32)),
        in_specs=[_sm(), _vm(), _vm(), _vm(), _vm(), _vm(), _any(), _any(), _any(), _any()],
        out_specs=(_vm(), _vm(), _vm()),
        scratch_shapes=[
            pltpu.VMEM((d, hdim), BF16),
            pltpu.VMEM((hdim, d), BF16),
            pltpu.VMEM((KVBUF, SEQ, rows, hd), BF16),
            pltpu.VMEM((KVBUF, SEQ, rows, hd), BF16),
            pltpu.VMEM((b * nh, hd), F32),
            pltpu.VMEM((b * nh, hd), F32),
            pltpu.VMEM((b, hdim), BF16),
            pltpu.VMEM((nh, rows), F32),
            pltpu.VMEM((b, d), BF16),
            pltpu.VMEM((SEQ * nh, rows), F32),
            pltpu.VMEM((SEQ * nh, rows), BF16),
            pltpu.SemaphoreType.DMA((8,)),
            pltpu.SemaphoreType.DMA((8,)),
            pltpu.SemaphoreType.DMA((KVBUF,)),
            pltpu.SemaphoreType.DMA((KVBUF,)),
        ],
        compiler_params=pltpu.CompilerParams(vmem_limit_bytes=VLIM),
    )(lens, x, ln1, ln2, idx.T, gates.T, kk, vv, wq, wo)


def _places():
    cy = lax.axis_index("ey")
    cx = lax.axis_index("ex")
    xn = cy + 1 - 2 * lax.rem(cy, 2)
    yn = lax.rem(cy + 2, 4)
    dg = 3 - cy
    return cy, cx, (xn, yn, dg)


def _barrier(cy, cx, others):
    bar = pltpu.get_barrier_semaphore()
    for o in others:
        pl.semaphore_signal(bar, inc=1, device_id=(o, cx), device_id_type=MESH)
    pl.semaphore_signal(bar, inc=1, device_id=(cy, 1 - cx), device_id_type=MESH)
    pl.semaphore_wait(bar, len(others) + 1)


WBUF = 4
TILE = 128
SMALL = 64
LANES = 16
PITCH = 17
STEP8 = 8


def _silu_mul(z1, z3):
    return (z1 * jax.nn.sigmoid(z1) * z3).astype(BF16)


def _slot_copies(w1, w3, w2, b1, b3, b2, sem, e, slot):
    return (pltpu.make_async_copy(w1.at[e], b1.at[slot], sem.at[0, slot]),
            pltpu.make_async_copy(w3.at[e], b3.at[slot], sem.at[1, slot]),
            pltpu.make_async_copy(w2.at[e], b2.at[slot], sem.at[2, slot]))


def _gather_kernel(u, pk, w1, w3, w2, ua, toks, wgts, cols, b1, b3, b2,
                   pka, tmap, ps_sem, pr_sem, s_sem, r_sem, fs_sem, fr_sem, os_sem, or_sem, w_sem):
    blk, d = u.shape
    ntok = 8 * blk
    ne = w1.shape[0]
    top = 8
    cap = blk - blk // 8
    half = blk // 2
    cy, cx, others = _places()
    xn, yn, dg = others
    me = 2 * cy + cx

    ahead = [_slot_copies(w1, w3, w2, b1, b3, b2, w_sem, e, e) for e in range(WBUF)]
    for cs in ahead:
        for c in cs:
            c.start()

    _barrier(cy, cx, others)

    def table(src, slot, dev, i):
        return pltpu.make_async_remote_copy(
            src_ref=src, dst_ref=pka.at[slot], send_sem=ps_sem.at[i], recv_sem=pr_sem.at[i],
            device_id=dev, device_id_type=MESH)

    def rows(k):
        return pl.ds(k * half, half)

    def part(src, slot, k, dev, ss, rs, i):
        return pltpu.make_async_remote_copy(
            src_ref=src, dst_ref=ua.at[slot, rows(k)], send_sem=ss.at[i, k], recv_sem=rs.at[i, k],
            device_id=dev, device_id_type=MESH)

    partner = (cy, 1 - cx)
    for i in range(3):
        table(pk, me, (others[i], cx), i).start()
    table(pk, me, partner, 3).start()
    direct = [(1, 0), (0, 1), (1, 1), (0, 0)]
    for i, k in direct:
        part(u.at[rows(k)], me, k, (others[i], cx), s_sem, r_sem, i).start()
    for k in range(2):
        part(u.at[rows(k)], me, k, partner, os_sem, or_sem, 0).start()
    ua[me] = u[...]
    pka[me] = pk[...]

    for i in range(3):
        slot = 2 * others[i] + cx
        table(pk, slot, (others[i], cx), i).wait_recv()
        table(pka.at[slot], slot, partner, 4 + i).start()
    for i in range(3):
        slot = 2 * others[i] + cx
        table(pka.at[slot], slot, partner, 4 + i).wait()
        table(pk, me, (others[i], cx), i).wait_send()
    table(pk, me, partner, 3).wait()

    def tables():
        tmap[...] = jnp.concatenate([pka[k, :, 0:blk] for k in range(8)], axis=1)
        ids = (me * ne + lax.broadcasted_iota(jnp.int32, (ne, ntok), 0)).astype(F32)
        member = jnp.zeros((ne, ntok), F32)
        gate = jnp.zeros((ne, ntok), F32)
        for j in range(top):
            hit = tmap[j:j + 1, :] == ids
            member = member + jnp.where(hit, 1.0, 0.0)
            gate = gate + jnp.where(hit, tmap[top + j:top + j + 1, :], 0.0)
        ti = lax.broadcasted_iota(jnp.int32, (ntok, ntok), 0)
        tj = lax.broadcasted_iota(jnp.int32, (ntok, ntok), 1)
        tri = ti < tj
        tri_b = (tri & (ti // blk == tj // blk)).astype(F32).astype(BF16)
        rank = jnp.dot(member.astype(BF16), tri_b, preferred_element_type=F32)
        keep = jnp.where(rank < cap, member, 0.0)
        pos = jnp.dot(keep.astype(BF16), tri.astype(F32).astype(BF16), preferred_element_type=F32)
        pkeep = jnp.where(keep > 0, pos, -1.0)
        gkeep = gate * keep
        both = jnp.concatenate([gkeep, jnp.zeros((128 - ne, ntok), F32)], axis=0)
        cols[...] = jnp.transpose(both)
        place = lax.broadcasted_iota(jnp.int32, (SMALL, ntok), 0).astype(F32)
        tok = lax.broadcasted_iota(jnp.int32, (SMALL, ntok), 1).astype(F32) - ntok
        lane = lax.broadcasted_iota(jnp.int32, (SMALL, 128), 1)
        lists = jnp.zeros((SMALL, 128), F32)
        for e in range(ne):
            hit = pkeep[e:e + 1, :] == place
            t = jnp.sum(jnp.where(hit, tok, 0.0), axis=1, keepdims=True)
            g = jnp.sum(jnp.where(hit, gkeep[e:e + 1, :], 0.0), axis=1, keepdims=True)
            lists = lists + jnp.where(lane == e, t, 0.0) + jnp.where(lane == ne + e, g, 0.0)
        lists = jnp.transpose(jnp.concatenate([lists, jnp.zeros((128 - SMALL, 128), F32)], axis=0))
        count = jnp.sum(keep, axis=1, keepdims=True)
        last = lax.broadcasted_iota(jnp.int32, (ne, 128), 1) == 127
        toks[...] = jnp.where(last, count, lists[0:ne, :] + ntok).astype(jnp.int32)
        wgts[...] = lists[ne:2 * ne, :]

    def take(slot, k, dev, i):
        part(u.at[rows(k)], slot, k, dev, s_sem, r_sem, i).wait_recv()
        part(ua.at[slot, rows(k)], slot, k, partner, fs_sem, fr_sem, i).start()

    sx, sy, sd = 2 * xn + cx, 2 * yn + cx, 2 * dg + cx
    relay = {0: (sy, xn), 1: (sx, yn)}

    def across(k):
        slot, dev = relay[k]
        return part(ua.at[slot, rows(k)], slot, k, (dev, cx), s_sem, r_sem, 2)

    tables()
    take(sy, 0, (yn, cx), 1)
    across(0).start()
    take(sx, 1, (xn, cx), 0)
    across(1).start()
    take(sy, 1, (yn, cx), 1)
    take(sx, 0, (xn, cx), 0)
    for k in range(2):
        take(sd, k, (dg, cx), 2)
    for i, slot in ((1, sy), (0, sx), (2, sd)):
        for k in range(2):
            part(ua.at[slot, rows(k)], slot, k, partner, fs_sem, fr_sem, i).wait()
    for k in range(2):
        part(u.at[rows(k)], me, k, partner, os_sem, or_sem, 0).wait()
        across(k).wait_send()
        for i in range(2):
            part(u.at[rows(k)], me, k, (others[i], cx), s_sem, r_sem, i).wait_send()
    for cs in ahead:
        for c in cs:
            c.wait()


def _all_gather(u, pk, w1, w3, w2):
    b, d = u.shape
    ne, _, f = w1.shape
    return pl.pallas_call(
        _gather_kernel,
        name="gather",
        out_shape=(pltpu.VMEM((8, b, d), BF16),
                   jax.ShapeDtypeStruct((ne, 128), jnp.int32),
                   jax.ShapeDtypeStruct((ne, 128), F32),
                   pltpu.VMEM((8 * b, 128), F32),
                   pltpu.VMEM((WBUF, d, f), BF16),
                   pltpu.VMEM((WBUF, d, f), BF16),
                   pltpu.VMEM((WBUF, f, d), BF16)),
        in_specs=[_vm(), _vm()] + [_hbm()] * 3,
        out_specs=(_vm(),) * 7,
        scratch_shapes=[
            pltpu.VMEM((8, pk.shape[0], 128), F32),
            pltpu.VMEM((pk.shape[0], 8 * b), F32),
            pltpu.SemaphoreType.DMA((7,)),
            pltpu.SemaphoreType.DMA((7,)),
            pltpu.SemaphoreType.DMA((3, 2)),
            pltpu.SemaphoreType.DMA((3, 2)),
            pltpu.SemaphoreType.DMA((3, 2)),
            pltpu.SemaphoreType.DMA((3, 2)),
            pltpu.SemaphoreType.DMA((1, 2)),
            pltpu.SemaphoreType.DMA((1, 2)),
            pltpu.SemaphoreType.DMA((3, WBUF)),
        ],
        compiler_params=pltpu.CompilerParams(
            collective_id=0, has_side_effects=True, vmem_limit_bytes=4 * 1024 * 1024),
    )(u, pk, w1, w3, w2)


def _expert_kernel(toks, wgts, ua, cols, b1, b3, b2, w1, w3, w2, acc, o1, o3, o2,
                   ua3, x3, r3, xt, gt, gsc, order, seat, sem):
    del o1, o3, o2
    ntok, d = ua.shape
    ne = w1.shape[0]
    f = w1.shape[2]
    fc = 256
    dc = 512

    def copies(e, slot):
        return _slot_copies(w1, w3, w2, b1, b3, b2, sem, e, slot)

    spread = [5, 9, 12, 7, 10, 4, 6, 8, 11, 13, 14, 15]
    for k in range(ne - WBUF):
        seat[k] = spread[k]
    for e in range(ne):
        if e < WBUF:
            order[e] = e
        else:
            rank = jnp.int32(0)
            for o in range(WBUF, ne):
                if o != e:
                    ahead = toks[o, 127] >= toks[e, 127] if o < e else toks[o, 127] > toks[e, 127]
                    rank = rank + ahead.astype(jnp.int32)
            order[seat[rank]] = e

    for c in range(LANES):
        ua3[pl.ds(c, ntok, stride=PITCH), :] = ua[:, c * 128:(c + 1) * 128].astype(F32)
    ua3[ntok * PITCH:, :] = jnp.zeros((STEP8 * PITCH, 128), F32)

    def zero(i, _):
        acc[pl.ds(pl.multiple_of(i * 256, 256), 256), :] = jnp.zeros((256, 128), F32)
        return 0
    lax.fori_loop(0, ntok * LANES // 256, zero, 0)
    acc[ntok * LANES:, :] = jnp.zeros((STEP8 * LANES, 128), F32)

    def hidden(slot, m):
        for c in range(f // fc):
            s = slice(c * fc, (c + 1) * fc)
            z1 = jnp.dot(xt[0:m, :], b1[slot, :, s], preferred_element_type=F32)
            z3 = jnp.dot(xt[0:m, :], b3[slot, :, s], preferred_element_type=F32)
            gt[0:m, s] = _silu_mul(z1, z3)

    def results(slot, m):
        for c in range(d // dc):
            y = jnp.dot(gt[0:m, :], b2[slot, :, c * dc:(c + 1) * dc], preferred_element_type=F32)
            y = y.astype(BF16).astype(F32)
            for j in range(dc // 128):
                r3[pl.ds(c * (dc // 128) + j, m, stride=PITCH), :] = y[:, j * 128:(j + 1) * 128]

    def at(t):
        return pl.ds(pl.multiple_of(t * LANES, LANES), LANES)

    def wide(t):
        return pl.ds(t * PITCH, LANES)

    def expert(step, _):
        slot = lax.rem(step, WBUF)
        e = order[step]

        @pl.when(step >= WBUF)
        def _():
            for c in copies(e, slot):
                c.wait()
        n = toks[e, 127]

        @pl.when((n > 0) & (n <= SMALL))
        def _():
            steps = (n + STEP8 - 1) // STEP8

            def fetch(i, _):
                for k in range(STEP8):
                    m = i * STEP8 + k
                    x3[wide(m), :] = ua3[wide(toks[e, m]), :]
                return 0
            lax.fori_loop(0, steps, fetch, 0)
            for c in range(LANES):
                xt[0:SMALL, c * 128:(c + 1) * 128] = x3[pl.ds(c, SMALL, stride=PITCH), :].astype(BF16)
            hidden(slot, SMALL)
            results(slot, SMALL)

            def add(i, _):
                where = [at(toks[e, i * STEP8 + k]) for k in range(STEP8)]
                new = [acc[where[k], :] + wgts[e, i * STEP8 + k] * r3[wide(i * STEP8 + k), :] for k in range(STEP8)]
                for k in range(STEP8):
                    acc[where[k], :] = new[k]
                return 0
            lax.fori_loop(0, steps, add, 0)

        @pl.when(n > SMALL)
        def _():
            lane = lax.broadcasted_iota(jnp.int32, (ntok, 128), 1)
            gsc[...] = jnp.broadcast_to(
                jnp.sum(jnp.where(lane == e, cols[...], 0.0), axis=1, keepdims=True), (ntok, 128))

            def dense(t, _):
                rows = pl.ds(pl.multiple_of(t * TILE, TILE), TILE)
                xt[...] = ua[rows, :]
                hidden(slot, TILE)
                results(slot, TILE)

                def add(i, _):
                    for k in range(STEP8):
                        m = i * STEP8 + k
                        one = at(t * TILE + m)
                        g = gsc[pl.ds(t * TILE + m, 1), :]
                        acc[one, :] = acc[one, :] + g * r3[wide(m), :]
                    return 0
                lax.fori_loop(0, TILE // STEP8, add, 0)
                return 0
            lax.fori_loop(0, ntok // TILE, dense, 0)

        @pl.when(step + WBUF < ne)
        def _():
            for c in copies(order[step + WBUF], slot):
                c.start()
        return 0

    lax.fori_loop(0, ne, expert, 0)


def _experts(toks, wgts, ua, cols, i1, i3, i2, w1, w3, w2):
    ntok, d = ua.shape
    ne, _, f = w1.shape
    return pl.pallas_call(
        _expert_kernel,
        name="experts",
        out_shape=(pltpu.VMEM(((ntok + STEP8) * LANES, 128), F32),
                   pltpu.VMEM((WBUF, d, f), BF16),
                   pltpu.VMEM((WBUF, d, f), BF16),
                   pltpu.VMEM((WBUF, f, d), BF16)),
        in_specs=[_sm()] * 2 + [_vm()] * 5 + [_hbm()] * 3,
        out_specs=(_vm(),) * 4,
        input_output_aliases={4: 1, 5: 2, 6: 3},
        scratch_shapes=[
            pltpu.VMEM(((ntok + STEP8) * PITCH, 128), F32),
            pltpu.VMEM((SMALL * PITCH, 128), F32),
            pltpu.VMEM((TILE * PITCH, 128), F32),
            pltpu.VMEM((TILE, d), BF16),
            pltpu.VMEM((TILE, f), BF16),
            pltpu.VMEM((ntok, 128), F32),
            pltpu.SMEM((ne,), jnp.int32),
            pltpu.SMEM((ne,), jnp.int32),
            pltpu.SemaphoreType.DMA((3, WBUF)),
        ],
        compiler_params=pltpu.CompilerParams(vmem_limit_bytes=9 * 1024 * 1024),
    )(toks, wgts, ua, cols, i1, i3, i2, w1, w3, w2)[0]


CH = 4


def _return_kernel(acc, h, u, ws1, ws3, ws2, y, rbuf, sbuf, abuf, tbuf, zbuf, tot, hs, gt, v1, v3, v2,
                   ds_sem, dr_sem, s_sem, r_sem, ts_sem, tr_sem, v_sem):
    cy, cx, others = _places()
    xn, yn, dg = others
    b, d = h.shape
    f = gt.shape[1]
    per = b // CH
    w = per * LANES
    n1 = xn * (1 - cx) + yn * cx
    n2 = yn * (1 - cx) + xn * cx

    shared = (pltpu.make_async_copy(ws1, v1, v_sem.at[0]),
              pltpu.make_async_copy(ws3, v3, v_sem.at[1]),
              pltpu.make_async_copy(ws2, v2, v_sem.at[2]))
    for c in shared:
        c.start()
    _barrier(cy, cx, others)

    def piece(k, core, c):
        return pl.ds((2 * k + core) * (b * LANES) + c * w, w)

    def pair(c, k):
        return pltpu.make_async_remote_copy(
            src_ref=acc.at[piece(k, 1 - cx, c)], dst_ref=rbuf.at[c, k],
            send_sem=ds_sem.at[c, k], recv_sem=dr_sem.at[c, k],
            device_id=(cy, 1 - cx), device_id_type=MESH)

    def first(c, i):
        return pltpu.make_async_remote_copy(
            src_ref=sbuf.at[c, dg if i else n1], dst_ref=abuf.at[c, i],
            send_sem=s_sem.at[c, i], recv_sem=r_sem.at[c, i],
            device_id=(n1, cx), device_id_type=MESH)

    def second(c):
        return pltpu.make_async_remote_copy(
            src_ref=tbuf.at[c], dst_ref=zbuf.at[c], send_sem=ts_sem.at[c], recv_sem=tr_sem.at[c],
            device_id=(n2, cx), device_id_type=MESH)

    for c in range(CH):
        for k in range(4):
            pair(c, k).start()
    for c in range(CH):
        for k in range(4):
            pair(c, k).wait_recv()
            sbuf[c, k] = acc[piece(k, cx, c), :] + rbuf[c, k]
        for i in (1, 0):
            first(c, i).start()

    for c in shared:
        c.wait()
    for c in range(f // 256):
        s = slice(c * 256, (c + 1) * 256)
        z1 = jnp.dot(u[...], v1[:, s], preferred_element_type=F32)
        z3 = jnp.dot(u[...], v3[:, s], preferred_element_type=F32)
        gt[:, s] = _silu_mul(z1, z3)
    for c in range(d // 512):
        s = slice(c * 512, (c + 1) * 512)
        hs[:, s] = h[:, s].astype(F32) + jnp.dot(gt[...], v2[:, s], preferred_element_type=F32)

    for c in range(CH):
        first(c, 1).wait_recv()
        tbuf[c] = sbuf[c, n2] + abuf[c, 1]
        second(c).start()
    for c in range(CH):
        first(c, 0).wait_recv()
        second(c).wait_recv()
        tot[...] = sbuf[c, cy] + (abuf[c, 0] + zbuf[c])
        r = slice(c * per, (c + 1) * per)
        for j in range(LANES):
            s = slice(j * 128, (j + 1) * 128)
            y[r, s] = (hs[r, s] + tot[pl.ds(j, per, stride=LANES), :]).astype(BF16)
    for c in range(CH):
        for k in range(4):
            pair(c, k).wait_send()
        for i in range(2):
            first(c, i).wait_send()
        second(c).wait_send()


def _return(acc, h, u, ws1, ws3, ws2):
    b, d = h.shape
    f = ws1.shape[1]
    w = b // CH * LANES
    return pl.pallas_call(
        _return_kernel,
        name="giveback",
        out_shape=jax.ShapeDtypeStruct((b, d), BF16),
        in_specs=[_vm()] * 3 + [_hbm()] * 3,
        out_specs=_vm(),
        scratch_shapes=[
            pltpu.VMEM((CH, 4, w, 128), F32),
            pltpu.VMEM((CH, 4, w, 128), F32),
            pltpu.VMEM((CH, 2, w, 128), F32),
            pltpu.VMEM((CH, w, 128), F32),
            pltpu.VMEM((CH, w, 128), F32),
            pltpu.VMEM((w, 128), F32),
            pltpu.VMEM((b, d), F32),
            pltpu.VMEM((b, f), BF16),
            pltpu.VMEM((d, f), BF16),
            pltpu.VMEM((d, f), BF16),
            pltpu.VMEM((f, d), BF16),
            pltpu.SemaphoreType.DMA((CH, 4)),
            pltpu.SemaphoreType.DMA((CH, 4)),
            pltpu.SemaphoreType.DMA((CH, 2)),
            pltpu.SemaphoreType.DMA((CH, 2)),
            pltpu.SemaphoreType.DMA((CH,)),
            pltpu.SemaphoreType.DMA((CH,)),
            pltpu.SemaphoreType.DMA((3,)),
        ],
        compiler_params=pltpu.CompilerParams(
            collective_id=1, has_side_effects=True, vmem_limit_bytes=20 * 1024 * 1024),
    )(acc, h, u, ws1, ws3, ws2)


def solution(mesh):
    def body(x, kv_k, kv_v, lens, idx, gates, ln1, wq, wo, ln2, ws1, ws3, ws2, w1, w3, w2):
        b, d = x.shape
        h, u, pk = _attention(x, kv_k, kv_v, lens, idx, gates, ln1, ln2, wq, wo)
        ua, toks, wgts, cols, b1, b3, b2 = _all_gather(u, pk, w1, w3, w2)
        acc = _experts(toks, wgts, ua.reshape(8 * b, d), cols, b1, b3, b2, w1, w3, w2)
        return _return(acc, h, u, ws1, ws3, ws2)

    rows = P(GRP)
    rep = P()
    return jax.shard_map(
        body, mesh=mesh,
        in_specs=(rows, rows, rows, rows, rows, rows, rep, rep, rep, rep, rep, rep, rep, rows, rows, rows),
        out_specs=rows, check_vma=False)
```

```python
import functools

import jax
import jax.numpy as jnp
from jax import lax
from jax.experimental import pallas as pl
from jax.experimental.pallas import tpu as pltpu
from jax.sharding import PartitionSpec as P

EPS = 1e-6
GRP = ("ey", "ex")
MESH = pl.DeviceIdType.MESH
NEG = -1e30
F32 = jnp.float32
BF16 = jnp.bfloat16
VLIM = 55 * 1024 * 1024


def _vm():
    return pl.BlockSpec(memory_space=pltpu.VMEM)


def _sm():
    return pl.BlockSpec(memory_space=pltpu.SMEM)


def _hbm():
    return pl.BlockSpec(memory_space=pltpu.HBM)


def _any():
    return pl.BlockSpec(memory_space=pl.ANY)


def _rms(v, w):
    v32 = v.astype(F32)
    r = lax.rsqrt(jnp.mean(v32 * v32, axis=-1, keepdims=True) + EPS)
    return (v32 * r * w.astype(F32)).astype(BF16)


SEQ = 8
KVBUF = 4
STEP = 64


def _attn_kernel(lens, x, ln1, ln2, idx, gates, kk, vv, wq, wo, h_out, u_out, pk_out,
                 wqb, wob, kb, vb, qs, os, ob, bias, hf, ss, ps, wq_sem, wo_sem, k_sem, v_sem):
    b, d = x.shape
    heads_dim = wqb.shape[1]
    hd = 128
    nh = heads_dim // hd
    rows = kk.shape[1]
    kvh = 4
    seqlen = rows // kvh
    ncls = seqlen // STEP
    crow = STEP * kvh
    ngrp = b // SEQ
    nwq = wq_sem.shape[0]
    nwo = wo_sem.shape[0]
    cq = heads_dim // nwq
    co = d // nwo

    def wq_copy(i):
        c = pl.ds(pl.multiple_of(i * cq, cq), cq)
        return pltpu.make_async_copy(wq.at[:, c], wqb.at[:, c], wq_sem.at[i])

    def wo_copy(i):
        c = pl.ds(pl.multiple_of(i * co, co), co)
        return pltpu.make_async_copy(wo.at[:, c], wob.at[:, c], wo_sem.at[i])

    def gmax(g):
        m = lens[g * SEQ]
        for s in range(1, SEQ):
            m = jnp.maximum(m, lens[g * SEQ + s])
        return m

    def kv_copies(g, slot, n):
        src = (pl.ds(g * SEQ, SEQ), pl.ds(0, n * crow))
        dst = (slot, slice(None), pl.ds(0, n * crow))
        return (pltpu.make_async_copy(kk.at[src], kb.at[dst], k_sem.at[slot]),
                pltpu.make_async_copy(vv.at[src], vb.at[dst], v_sem.at[slot]))

    def by_class(g, f):
        cls = (gmax(g) + STEP - 1) // STEP
        for n in range(1, ncls + 1):
            pl.when(cls == n)(functools.partial(f, n))

    def start_kv(g):
        slot = lax.rem(g, KVBUF)

        def go(n):
            for c in kv_copies(g, slot, n):
                c.start()
        by_class(g, go)

    for i in range(nwq):
        wq_copy(i).start()
    lax.fori_loop(0, min(KVBUF, ngrp), lambda g, _: (start_kv(g), 0)[1], 0)
    table = jnp.concatenate([idx[...].astype(F32), gates[...]], axis=0)
    pk_out[...] = jnp.concatenate([table, jnp.zeros((table.shape[0], 128 - b), F32)], axis=1)
    col = lax.broadcasted_iota(jnp.int32, (nh, rows), 1)
    row = lax.broadcasted_iota(jnp.int32, (nh, rows), 0)
    bias[...] = jnp.where(lax.rem(col, kvh) == row // (nh // kvh), 0.0, NEG)

    a = _rms(x[...], ln1[...])

    def qstep(i, _):
        wq_copy(i).wait()
        w = wqb[:, pl.ds(pl.multiple_of(i * cq, cq), cq)]
        q = jnp.dot(a, w, preferred_element_type=F32).astype(BF16).astype(F32)
        for j in range(cq // hd):
            qs[pl.ds(i * (cq // hd) + j, b, stride=nh), :] = q[:, j * hd:(j + 1) * hd]
        return 0

    lax.fori_loop(0, nwq, qstep, 0)
    per = nwo // min(KVBUF, ngrp)

    def group(g, _):
        slot = lax.rem(g, KVBUF)

        def go(n):
            for c in kv_copies(g, slot, n):
                c.wait()
            w = n * crow
            lane = lax.broadcasted_iota(jnp.int32, (nh, w), 1)
            rq = [pl.ds(pl.multiple_of((g * SEQ + s) * nh, nh), nh) for s in range(SEQ)]
            for s in range(SEQ):
                q = qs[rq[s], :].astype(BF16)
                k = kb[slot, s, 0:w, :]
                ss[s * nh:(s + 1) * nh, 0:w] = lax.dot_general(
                    q, k, (((1,), (1,)), ((), ())), preferred_element_type=F32)
            for s in range(SEQ):
                sc = ss[s * nh:(s + 1) * nh, 0:w] * (hd ** -0.5) + bias[:, 0:w]
                sc = jnp.where(lane < lens[g * SEQ + s] * kvh, sc, NEG)
                m = jnp.max(sc, axis=1, keepdims=True)
                p = jnp.exp(sc - m)
                ps[s * nh:(s + 1) * nh, 0:w] = (p * (1.0 / jnp.sum(p, axis=1, keepdims=True))).astype(BF16)
            for s in range(SEQ):
                o = jnp.dot(ps[s * nh:(s + 1) * nh, 0:w], vb[slot, s, 0:w, :], preferred_element_type=F32)
                os[rq[s], :] = o.astype(BF16).astype(F32)
        by_class(g, go)
        pl.when(g + KVBUF < ngrp)(lambda: start_kv(g + KVBUF))

        @pl.when(g + KVBUF >= ngrp)
        def _():
            for i in range(per):
                wo_copy((g + KVBUF - ngrp) * per + i).start()
        return 0

    lax.fori_loop(0, ngrp, group, 0)

    for j in range(nh):
        ob[:, j * hd:(j + 1) * hd] = os[pl.ds(j, b, stride=nh), :].astype(BF16)

    def ostep(i, _):
        wo_copy(i).wait()
        c = pl.ds(pl.multiple_of(i * co, co), co)
        attn = jnp.dot(ob[...], wob[:, c], preferred_element_type=F32)
        hf[:, c] = (x[:, c].astype(F32) + attn).astype(BF16)
        return 0

    lax.fori_loop(0, nwo, ostep, 0)
    h = hf[...]
    h_out[...] = h
    u_out[...] = _rms(h, ln2[...])


def _attention(x, kv_k, kv_v, lens, idx, gates, ln1, ln2, wq, wo):
    b, d = x.shape
    _, l, kvh, hd = kv_k.shape
    hdim = wq.shape[1]
    nh = hdim // hd
    rows = l * kvh
    kk = kv_k.reshape(b, rows, hd)
    vv = kv_v.reshape(b, rows, hd)
    return pl.pallas_call(
        _attn_kernel,
        name="attn",
        out_shape=(pltpu.VMEM((b, d), BF16), pltpu.VMEM((b, d), BF16), pltpu.VMEM((2 * idx.shape[1], 128), F32)),
        in_specs=[_sm(), _vm(), _vm(), _vm(), _vm(), _vm(), _any(), _any(), _any(), _any()],
        out_specs=(_vm(), _vm(), _vm()),
        scratch_shapes=[
            pltpu.VMEM((d, hdim), BF16),
            pltpu.VMEM((hdim, d), BF16),
            pltpu.VMEM((KVBUF, SEQ, rows, hd), BF16),
            pltpu.VMEM((KVBUF, SEQ, rows, hd), BF16),
            pltpu.VMEM((b * nh, hd), F32),
            pltpu.VMEM((b * nh, hd), F32),
            pltpu.VMEM((b, hdim), BF16),
            pltpu.VMEM((nh, rows), F32),
            pltpu.VMEM((b, d), BF16),
            pltpu.VMEM((SEQ * nh, rows), F32),
            pltpu.VMEM((SEQ * nh, rows), BF16),
            pltpu.SemaphoreType.DMA((8,)),
            pltpu.SemaphoreType.DMA((8,)),
            pltpu.SemaphoreType.DMA((KVBUF,)),
            pltpu.SemaphoreType.DMA((KVBUF,)),
        ],
        compiler_params=pltpu.CompilerParams(vmem_limit_bytes=VLIM),
    )(lens, x, ln1, ln2, idx.T, gates.T, kk, vv, wq, wo)


def _places():
    cy = lax.axis_index("ey")
    cx = lax.axis_index("ex")
    xn = cy + 1 - 2 * lax.rem(cy, 2)
    yn = lax.rem(cy + 2, 4)
    dg = 3 - cy
    return cy, cx, (xn, yn, dg)


def _barrier(cy, cx, others):
    bar = pltpu.get_barrier_semaphore()
    for o in others:
        pl.semaphore_signal(bar, inc=1, device_id=(o, cx), device_id_type=MESH)
    pl.semaphore_signal(bar, inc=1, device_id=(cy, 1 - cx), device_id_type=MESH)
    pl.semaphore_wait(bar, len(others) + 1)


WBUF = 4
TILE = 128
SMALL = 64
LANES = 16
PITCH = 17
STEP8 = 8


def _silu_mul(z1, z3):
    return (z1 * jax.nn.sigmoid(z1) * z3).astype(BF16)


def _slot_copies(w1, w3, w2, b1, b3, b2, sem, e, slot):
    return (pltpu.make_async_copy(w1.at[e], b1.at[slot], sem.at[0, slot]),
            pltpu.make_async_copy(w3.at[e], b3.at[slot], sem.at[1, slot]),
            pltpu.make_async_copy(w2.at[e], b2.at[slot], sem.at[2, slot]))


def _gather_kernel(u, pk, w1, w3, w2, ua, toks, wgts, cols, b1, b3, b2,
                   pka, tmap, ps_sem, pr_sem, s_sem, r_sem, fs_sem, fr_sem, os_sem, or_sem, w_sem):
    blk, d = u.shape
    ntok = 8 * blk
    ne = w1.shape[0]
    top = 8
    cap = blk - blk // 8
    half = blk // 2
    cy, cx, others = _places()
    xn, yn, dg = others
    me = 2 * cy + cx

    ahead = [_slot_copies(w1, w3, w2, b1, b3, b2, w_sem, e, e) for e in range(WBUF)]
    for cs in ahead:
        for c in cs:
            c.start()

    _barrier(cy, cx, others)

    def table(src, slot, dev, i):
        return pltpu.make_async_remote_copy(
            src_ref=src, dst_ref=pka.at[slot], send_sem=ps_sem.at[i], recv_sem=pr_sem.at[i],
            device_id=dev, device_id_type=MESH)

    def rows(k):
        return pl.ds(k * half, half)

    def part(src, slot, k, dev, ss, rs, i):
        return pltpu.make_async_remote_copy(
            src_ref=src, dst_ref=ua.at[slot, rows(k)], send_sem=ss.at[i, k], recv_sem=rs.at[i, k],
            device_id=dev, device_id_type=MESH)

    partner = (cy, 1 - cx)
    for i in range(3):
        table(pk, me, (others[i], cx), i).start()
    table(pk, me, partner, 3).start()
    direct = [(1, 0), (0, 1), (1, 1), (0, 0)]
    for i, k in direct:
        part(u.at[rows(k)], me, k, (others[i], cx), s_sem, r_sem, i).start()
    for k in range(2):
        part(u.at[rows(k)], me, k, partner, os_sem, or_sem, 0).start()
    ua[me] = u[...]
    pka[me] = pk[...]

    for i in range(3):
        slot = 2 * others[i] + cx
        table(pk, slot, (others[i], cx), i).wait_recv()
        table(pka.at[slot], slot, partner, 4 + i).start()
    def tables():
        tmap[...] = jnp.concatenate([pka[k, :, 0:blk] for k in range(8)], axis=1)
        ids = (me * ne + lax.broadcasted_iota(jnp.int32, (ne, ntok), 0)).astype(F32)
        member = jnp.zeros((ne, ntok), F32)
        gate = jnp.zeros((ne, ntok), F32)
        for j in range(top):
            hit = tmap[j:j + 1, :] == ids
            member = member + jnp.where(hit, 1.0, 0.0)
            gate = gate + jnp.where(hit, tmap[top + j:top + j + 1, :], 0.0)
        ti = lax.broadcasted_iota(jnp.int32, (ntok, ntok), 0)
        tj = lax.broadcasted_iota(jnp.int32, (ntok, ntok), 1)
        tri = ti < tj
        tri_b = (tri & (ti // blk == tj // blk)).astype(F32).astype(BF16)
        rank = jnp.dot(member.astype(BF16), tri_b, preferred_element_type=F32)
        keep = jnp.where(rank < cap, member, 0.0)
        pos = jnp.dot(keep.astype(BF16), tri.astype(F32).astype(BF16), preferred_element_type=F32)
        pkeep = jnp.where(keep > 0, pos, -1.0)
        gkeep = gate * keep
        both = jnp.concatenate([gkeep, jnp.zeros((128 - ne, ntok), F32)], axis=0)
        cols[...] = jnp.transpose(both)
        place = lax.broadcasted_iota(jnp.int32, (SMALL, ntok), 0).astype(F32)
        tok = lax.broadcasted_iota(jnp.int32, (SMALL, ntok), 1).astype(F32) - ntok
        lane = lax.broadcasted_iota(jnp.int32, (SMALL, 128), 1)
        lists = jnp.zeros((SMALL, 128), F32)
        for e in range(ne):
            hit = pkeep[e:e + 1, :] == place
            t = jnp.sum(jnp.where(hit, tok, 0.0), axis=1, keepdims=True)
            g = jnp.sum(jnp.where(hit, gkeep[e:e + 1, :], 0.0), axis=1, keepdims=True)
            lists = lists + jnp.where(lane == e, t, 0.0) + jnp.where(lane == ne + e, g, 0.0)
        lists = jnp.transpose(jnp.concatenate([lists, jnp.zeros((128 - SMALL, 128), F32)], axis=0))
        count = jnp.sum(keep, axis=1, keepdims=True)
        last = lax.broadcasted_iota(jnp.int32, (ne, 128), 1) == 127
        toks[...] = jnp.where(last, count, lists[0:ne, :] + ntok).astype(jnp.int32)
        wgts[...] = lists[ne:2 * ne, :]

    def take(slot, k, dev, i):
        part(u.at[rows(k)], slot, k, dev, s_sem, r_sem, i).wait_recv()
        part(ua.at[slot, rows(k)], slot, k, partner, fs_sem, fr_sem, i).start()

    sx, sy, sd = 2 * xn + cx, 2 * yn + cx, 2 * dg + cx
    relay = {0: (sy, xn), 1: (sx, yn)}

    def across(k):
        slot, dev = relay[k]
        return part(ua.at[slot, rows(k)], slot, k, (dev, cx), s_sem, r_sem, 2)

    take(sy, 0, (yn, cx), 1)
    across(0).start()
    take(sx, 1, (xn, cx), 0)
    across(1).start()
    for i in range(3):
        slot = 2 * others[i] + cx
        table(pka.at[slot], slot, partner, 4 + i).wait()
        table(pk, me, (others[i], cx), i).wait_send()
    table(pk, me, partner, 3).wait()
    tables()
    take(sy, 1, (yn, cx), 1)
    take(sx, 0, (xn, cx), 0)
    for k in range(2):
        take(sd, k, (dg, cx), 2)
    for i, slot in ((1, sy), (0, sx), (2, sd)):
        for k in range(2):
            part(ua.at[slot, rows(k)], slot, k, partner, fs_sem, fr_sem, i).wait()
    for k in range(2):
        part(u.at[rows(k)], me, k, partner, os_sem, or_sem, 0).wait()
        across(k).wait_send()
        for i in range(2):
            part(u.at[rows(k)], me, k, (others[i], cx), s_sem, r_sem, i).wait_send()
    for cs in ahead:
        for c in cs:
            c.wait()


def _all_gather(u, pk, w1, w3, w2):
    b, d = u.shape
    ne, _, f = w1.shape
    return pl.pallas_call(
        _gather_kernel,
        name="gather",
        out_shape=(pltpu.VMEM((8, b, d), BF16),
                   jax.ShapeDtypeStruct((ne, 128), jnp.int32),
                   jax.ShapeDtypeStruct((ne, 128), F32),
                   pltpu.VMEM((8 * b, 128), F32),
                   pltpu.VMEM((WBUF, d, f), BF16),
                   pltpu.VMEM((WBUF, d, f), BF16),
                   pltpu.VMEM((WBUF, f, d), BF16)),
        in_specs=[_vm(), _vm()] + [_hbm()] * 3,
        out_specs=(_vm(),) * 7,
        scratch_shapes=[
            pltpu.VMEM((8, pk.shape[0], 128), F32),
            pltpu.VMEM((pk.shape[0], 8 * b), F32),
            pltpu.SemaphoreType.DMA((7,)),
            pltpu.SemaphoreType.DMA((7,)),
            pltpu.SemaphoreType.DMA((3, 2)),
            pltpu.SemaphoreType.DMA((3, 2)),
            pltpu.SemaphoreType.DMA((3, 2)),
            pltpu.SemaphoreType.DMA((3, 2)),
            pltpu.SemaphoreType.DMA((1, 2)),
            pltpu.SemaphoreType.DMA((1, 2)),
            pltpu.SemaphoreType.DMA((3, WBUF)),
        ],
        compiler_params=pltpu.CompilerParams(
            collective_id=0, has_side_effects=True, vmem_limit_bytes=4 * 1024 * 1024),
    )(u, pk, w1, w3, w2)


def _expert_kernel(toks, wgts, ua, cols, b1, b3, b2, w1, w3, w2, acc, o1, o3, o2,
                   ua3, x3, r3, xt, gt, gsc, order, seat, sem):
    del o1, o3, o2
    ntok, d = ua.shape
    ne = w1.shape[0]
    f = w1.shape[2]
    fc = 256
    dc = 512

    def copies(e, slot):
        return _slot_copies(w1, w3, w2, b1, b3, b2, sem, e, slot)

    spread = [5, 9, 12, 7, 10, 4, 6, 8, 11, 13, 14, 15]
    for k in range(ne - WBUF):
        seat[k] = spread[k]
    for e in range(ne):
        if e < WBUF:
            order[e] = e
        else:
            rank = jnp.int32(0)
            for o in range(WBUF, ne):
                if o != e:
                    ahead = toks[o, 127] >= toks[e, 127] if o < e else toks[o, 127] > toks[e, 127]
                    rank = rank + ahead.astype(jnp.int32)
            order[seat[rank]] = e

    for c in range(LANES):
        ua3[pl.ds(c, ntok, stride=PITCH), :] = ua[:, c * 128:(c + 1) * 128].astype(F32)
    ua3[ntok * PITCH:, :] = jnp.zeros((STEP8 * PITCH, 128), F32)

    def zero(i, _):
        acc[pl.ds(pl.multiple_of(i * 256, 256), 256), :] = jnp.zeros((256, 128), F32)
        return 0
    lax.fori_loop(0, ntok * LANES // 256, zero, 0)
    acc[ntok * LANES:, :] = jnp.zeros((STEP8 * LANES, 128), F32)

    def hidden(slot, m):
        for c in range(f // fc):
            s = slice(c * fc, (c + 1) * fc)
            z1 = jnp.dot(xt[0:m, :], b1[slot, :, s], preferred_element_type=F32)
            z3 = jnp.dot(xt[0:m, :], b3[slot, :, s], preferred_element_type=F32)
            gt[0:m, s] = _silu_mul(z1, z3)

    def results(slot, m):
        for c in range(d // dc):
            y = jnp.dot(gt[0:m, :], b2[slot, :, c * dc:(c + 1) * dc], preferred_element_type=F32)
            y = y.astype(BF16).astype(F32)
            for j in range(dc // 128):
                r3[pl.ds(c * (dc // 128) + j, m, stride=PITCH), :] = y[:, j * 128:(j + 1) * 128]

    def at(t):
        return pl.ds(pl.multiple_of(t * LANES, LANES), LANES)

    def wide(t):
        return pl.ds(t * PITCH, LANES)

    def expert(step, _):
        slot = lax.rem(step, WBUF)
        e = order[step]

        @pl.when(step >= WBUF)
        def _():
            for c in copies(e, slot):
                c.wait()
        n = toks[e, 127]

        @pl.when((n > 0) & (n <= SMALL))
        def _():
            steps = (n + STEP8 - 1) // STEP8

            def fetch(i, _):
                for k in range(STEP8):
                    m = i * STEP8 + k
                    x3[wide(m), :] = ua3[wide(toks[e, m]), :]
                return 0
            lax.fori_loop(0, steps, fetch, 0)
            for c in range(LANES):
                xt[0:SMALL, c * 128:(c + 1) * 128] = x3[pl.ds(c, SMALL, stride=PITCH), :].astype(BF16)
            hidden(slot, SMALL)
            results(slot, SMALL)

            def add(i, _):
                where = [at(toks[e, i * STEP8 + k]) for k in range(STEP8)]
                new = [acc[where[k], :] + wgts[e, i * STEP8 + k] * r3[wide(i * STEP8 + k), :] for k in range(STEP8)]
                for k in range(STEP8):
                    acc[where[k], :] = new[k]
                return 0
            lax.fori_loop(0, steps, add, 0)

        @pl.when(n > SMALL)
        def _():
            lane = lax.broadcasted_iota(jnp.int32, (ntok, 128), 1)
            gsc[...] = jnp.broadcast_to(
                jnp.sum(jnp.where(lane == e, cols[...], 0.0), axis=1, keepdims=True), (ntok, 128))

            def dense(t, _):
                rows = pl.ds(pl.multiple_of(t * TILE, TILE), TILE)
                xt[...] = ua[rows, :]
                hidden(slot, TILE)
                results(slot, TILE)

                def add(i, _):
                    for k in range(STEP8):
                        m = i * STEP8 + k
                        one = at(t * TILE + m)
                        g = gsc[pl.ds(t * TILE + m, 1), :]
                        acc[one, :] = acc[one, :] + g * r3[wide(m), :]
                    return 0
                lax.fori_loop(0, TILE // STEP8, add, 0)
                return 0
            lax.fori_loop(0, ntok // TILE, dense, 0)

        @pl.when(step + WBUF < ne)
        def _():
            for c in copies(order[step + WBUF], slot):
                c.start()
        return 0

    lax.fori_loop(0, ne, expert, 0)


def _experts(toks, wgts, ua, cols, i1, i3, i2, w1, w3, w2):
    ntok, d = ua.shape
    ne, _, f = w1.shape
    return pl.pallas_call(
        _expert_kernel,
        name="experts",
        out_shape=(pltpu.VMEM(((ntok + STEP8) * LANES, 128), F32),
                   pltpu.VMEM((WBUF, d, f), BF16),
                   pltpu.VMEM((WBUF, d, f), BF16),
                   pltpu.VMEM((WBUF, f, d), BF16)),
        in_specs=[_sm()] * 2 + [_vm()] * 5 + [_hbm()] * 3,
        out_specs=(_vm(),) * 4,
        input_output_aliases={4: 1, 5: 2, 6: 3},
        scratch_shapes=[
            pltpu.VMEM(((ntok + STEP8) * PITCH, 128), F32),
            pltpu.VMEM((SMALL * PITCH, 128), F32),
            pltpu.VMEM((TILE * PITCH, 128), F32),
            pltpu.VMEM((TILE, d), BF16),
            pltpu.VMEM((TILE, f), BF16),
            pltpu.VMEM((ntok, 128), F32),
            pltpu.SMEM((ne,), jnp.int32),
            pltpu.SMEM((ne,), jnp.int32),
            pltpu.SemaphoreType.DMA((3, WBUF)),
        ],
        compiler_params=pltpu.CompilerParams(vmem_limit_bytes=9 * 1024 * 1024),
    )(toks, wgts, ua, cols, i1, i3, i2, w1, w3, w2)[0]


CH = 4


def _return_kernel(acc, h, u, ws1, ws3, ws2, y, rbuf, sbuf, abuf, tbuf, zbuf, tot, hs, gt, v1, v3, v2,
                   ds_sem, dr_sem, s_sem, r_sem, ts_sem, tr_sem, v_sem):
    cy, cx, others = _places()
    xn, yn, dg = others
    b, d = h.shape
    f = gt.shape[1]
    per = b // CH
    w = per * LANES
    n1 = xn * (1 - cx) + yn * cx
    n2 = yn * (1 - cx) + xn * cx

    shared = (pltpu.make_async_copy(ws1, v1, v_sem.at[0]),
              pltpu.make_async_copy(ws3, v3, v_sem.at[1]),
              pltpu.make_async_copy(ws2, v2, v_sem.at[2]))
    for c in shared:
        c.start()
    _barrier(cy, cx, others)

    def piece(k, core, c):
        return pl.ds((2 * k + core) * (b * LANES) + c * w, w)

    def pair(c, k):
        return pltpu.make_async_remote_copy(
            src_ref=acc.at[piece(k, 1 - cx, c)], dst_ref=rbuf.at[c, k],
            send_sem=ds_sem.at[c, k], recv_sem=dr_sem.at[c, k],
            device_id=(cy, 1 - cx), device_id_type=MESH)

    def first(c, i):
        return pltpu.make_async_remote_copy(
            src_ref=sbuf.at[c, dg if i else n1], dst_ref=abuf.at[c, i],
            send_sem=s_sem.at[c, i], recv_sem=r_sem.at[c, i],
            device_id=(n1, cx), device_id_type=MESH)

    def second(c):
        return pltpu.make_async_remote_copy(
            src_ref=tbuf.at[c], dst_ref=zbuf.at[c], send_sem=ts_sem.at[c], recv_sem=tr_sem.at[c],
            device_id=(n2, cx), device_id_type=MESH)

    for c in range(CH):
        for k in range(4):
            pair(c, k).start()
    for c in range(CH):
        for k in range(4):
            pair(c, k).wait_recv()
            sbuf[c, k] = acc[piece(k, cx, c), :] + rbuf[c, k]
        for i in (1, 0):
            first(c, i).start()

    for c in shared:
        c.wait()
    for c in range(f // 256):
        s = slice(c * 256, (c + 1) * 256)
        z1 = jnp.dot(u[...], v1[:, s], preferred_element_type=F32)
        z3 = jnp.dot(u[...], v3[:, s], preferred_element_type=F32)
        gt[:, s] = _silu_mul(z1, z3)
    for c in range(d // 512):
        s = slice(c * 512, (c + 1) * 512)
        hs[:, s] = h[:, s].astype(F32) + jnp.dot(gt[...], v2[:, s], preferred_element_type=F32)

    for c in range(CH):
        first(c, 1).wait_recv()
        tbuf[c] = sbuf[c, n2] + abuf[c, 1]
        second(c).start()
    for c in range(CH):
        first(c, 0).wait_recv()
        second(c).wait_recv()
        tot[...] = sbuf[c, cy] + (abuf[c, 0] + zbuf[c])
        r = slice(c * per, (c + 1) * per)
        for j in range(LANES):
            s = slice(j * 128, (j + 1) * 128)
            y[r, s] = (hs[r, s] + tot[pl.ds(j, per, stride=LANES), :]).astype(BF16)
    for c in range(CH):
        for k in range(4):
            pair(c, k).wait_send()
        for i in range(2):
            first(c, i).wait_send()
        second(c).wait_send()


def _return(acc, h, u, ws1, ws3, ws2):
    b, d = h.shape
    f = ws1.shape[1]
    w = b // CH * LANES
    return pl.pallas_call(
        _return_kernel,
        name="giveback",
        out_shape=jax.ShapeDtypeStruct((b, d), BF16),
        in_specs=[_vm()] * 3 + [_hbm()] * 3,
        out_specs=_vm(),
        scratch_shapes=[
            pltpu.VMEM((CH, 4, w, 128), F32),
            pltpu.VMEM((CH, 4, w, 128), F32),
            pltpu.VMEM((CH, 2, w, 128), F32),
            pltpu.VMEM((CH, w, 128), F32),
            pltpu.VMEM((CH, w, 128), F32),
            pltpu.VMEM((w, 128), F32),
            pltpu.VMEM((b, d), F32),
            pltpu.VMEM((b, f), BF16),
            pltpu.VMEM((d, f), BF16),
            pltpu.VMEM((d, f), BF16),
            pltpu.VMEM((f, d), BF16),
            pltpu.SemaphoreType.DMA((CH, 4)),
            pltpu.SemaphoreType.DMA((CH, 4)),
            pltpu.SemaphoreType.DMA((CH, 2)),
            pltpu.SemaphoreType.DMA((CH, 2)),
            pltpu.SemaphoreType.DMA((CH,)),
            pltpu.SemaphoreType.DMA((CH,)),
            pltpu.SemaphoreType.DMA((3,)),
        ],
        compiler_params=pltpu.CompilerParams(
            collective_id=1, has_side_effects=True, vmem_limit_bytes=20 * 1024 * 1024),
    )(acc, h, u, ws1, ws3, ws2)


def solution(mesh):
    def body(x, kv_k, kv_v, lens, idx, gates, ln1, wq, wo, ln2, ws1, ws3, ws2, w1, w3, w2):
        b, d = x.shape
        h, u, pk = _attention(x, kv_k, kv_v, lens, idx, gates, ln1, ln2, wq, wo)
        ua, toks, wgts, cols, b1, b3, b2 = _all_gather(u, pk, w1, w3, w2)
        acc = _experts(toks, wgts, ua.reshape(8 * b, d), cols, b1, b3, b2, w1, w3, w2)
        return _return(acc, h, u, ws1, ws3, ws2)

    rows = P(GRP)
    rep = P()
    return jax.shard_map(
        body, mesh=mesh,
        in_specs=(rows, rows, rows, rows, rows, rows, rep, rep, rep, rep, rep, rep, rep, rows, rows, rows),
        out_specs=rows, check_vma=False)
```

```python
import functools

import jax
import jax.numpy as jnp
from jax import lax
from jax.experimental import pallas as pl
from jax.experimental.pallas import tpu as pltpu
from jax.sharding import PartitionSpec as P

EPS = 1e-6
GRP = ("ey", "ex")
MESH = pl.DeviceIdType.MESH
NEG = -1e30
F32 = jnp.float32
BF16 = jnp.bfloat16
VLIM = 55 * 1024 * 1024


def _vm():
    return pl.BlockSpec(memory_space=pltpu.VMEM)


def _sm():
    return pl.BlockSpec(memory_space=pltpu.SMEM)


def _hbm():
    return pl.BlockSpec(memory_space=pltpu.HBM)


def _any():
    return pl.BlockSpec(memory_space=pl.ANY)


def _rms(v, w):
    v32 = v.astype(F32)
    r = lax.rsqrt(jnp.mean(v32 * v32, axis=-1, keepdims=True) + EPS)
    return (v32 * r * w.astype(F32)).astype(BF16)


SEQ = 8
KVBUF = 4
STEP = 64


def _attn_kernel(lens, x, ln1, ln2, idx, gates, kk, vv, wq, wo, h_out, u_out, pk_out,
                 wqb, wob, kb, vb, qs, os, ob, bias, hf, ss, ps, wq_sem, wo_sem, k_sem, v_sem):
    b, d = x.shape
    heads_dim = wqb.shape[1]
    hd = 128
    nh = heads_dim // hd
    rows = kk.shape[1]
    kvh = 4
    seqlen = rows // kvh
    ncls = seqlen // STEP
    crow = STEP * kvh
    ngrp = b // SEQ
    nwq = wq_sem.shape[0]
    nwo = wo_sem.shape[0]
    cq = heads_dim // nwq
    co = d // nwo

    def wq_copy(i):
        c = pl.ds(pl.multiple_of(i * cq, cq), cq)
        return pltpu.make_async_copy(wq.at[:, c], wqb.at[:, c], wq_sem.at[i])

    def wo_copy(i):
        c = pl.ds(pl.multiple_of(i * co, co), co)
        return pltpu.make_async_copy(wo.at[:, c], wob.at[:, c], wo_sem.at[i])

    def gmax(g):
        m = lens[g * SEQ]
        for s in range(1, SEQ):
            m = jnp.maximum(m, lens[g * SEQ + s])
        return m

    def kv_copies(g, slot, n):
        src = (pl.ds(g * SEQ, SEQ), pl.ds(0, n * crow))
        dst = (slot, slice(None), pl.ds(0, n * crow))
        return (pltpu.make_async_copy(kk.at[src], kb.at[dst], k_sem.at[slot]),
                pltpu.make_async_copy(vv.at[src], vb.at[dst], v_sem.at[slot]))

    def by_class(g, f):
        cls = (gmax(g) + STEP - 1) // STEP
        for n in range(1, ncls + 1):
            pl.when(cls == n)(functools.partial(f, n))

    def start_kv(g):
        slot = lax.rem(g, KVBUF)

        def go(n):
            for c in kv_copies(g, slot, n):
                c.start()
        by_class(g, go)

    for i in range(nwq):
        wq_copy(i).start()
    lax.fori_loop(0, min(KVBUF, ngrp), lambda g, _: (start_kv(g), 0)[1], 0)
    table = jnp.concatenate([idx[...].astype(F32), gates[...]], axis=0)
    pk_out[...] = jnp.concatenate([table, jnp.zeros((table.shape[0], 128 - b), F32)], axis=1)
    col = lax.broadcasted_iota(jnp.int32, (nh, rows), 1)
    row = lax.broadcasted_iota(jnp.int32, (nh, rows), 0)
    bias[...] = jnp.where(lax.rem(col, kvh) == row // (nh // kvh), 0.0, NEG)

    a = _rms(x[...], ln1[...])

    def qstep(i, _):
        wq_copy(i).wait()
        w = wqb[:, pl.ds(pl.multiple_of(i * cq, cq), cq)]
        q = jnp.dot(a, w, preferred_element_type=F32).astype(BF16).astype(F32)
        for j in range(cq // hd):
            qs[pl.ds(i * (cq // hd) + j, b, stride=nh), :] = q[:, j * hd:(j + 1) * hd]
        return 0

    lax.fori_loop(0, nwq, qstep, 0)
    per = nwo // min(KVBUF, ngrp)

    def group(g, _):
        slot = lax.rem(g, KVBUF)

        def go(n):
            for c in kv_copies(g, slot, n):
                c.wait()
            w = n * crow
            lane = lax.broadcasted_iota(jnp.int32, (nh, w), 1)
            rq = [pl.ds(pl.multiple_of((g * SEQ + s) * nh, nh), nh) for s in range(SEQ)]
            for s in range(SEQ):
                q = qs[rq[s], :].astype(BF16)
                k = kb[slot, s, 0:w, :]
                ss[s * nh:(s + 1) * nh, 0:w] = lax.dot_general(
                    q, k, (((1,), (1,)), ((), ())), preferred_element_type=F32)
            for s in range(SEQ):
                sc = ss[s * nh:(s + 1) * nh, 0:w] * (hd ** -0.5) + bias[:, 0:w]
                sc = jnp.where(lane < lens[g * SEQ + s] * kvh, sc, NEG)
                m = jnp.max(sc, axis=1, keepdims=True)
                p = jnp.exp(sc - m)
                ps[s * nh:(s + 1) * nh, 0:w] = (p * (1.0 / jnp.sum(p, axis=1, keepdims=True))).astype(BF16)
            for s in range(SEQ):
                o = jnp.dot(ps[s * nh:(s + 1) * nh, 0:w], vb[slot, s, 0:w, :], preferred_element_type=F32)
                os[rq[s], :] = o.astype(BF16).astype(F32)
        by_class(g, go)
        pl.when(g + KVBUF < ngrp)(lambda: start_kv(g + KVBUF))

        @pl.when(g + KVBUF >= ngrp)
        def _():
            for i in range(per):
                wo_copy((g + KVBUF - ngrp) * per + i).start()
        return 0

    lax.fori_loop(0, ngrp, group, 0)

    for j in range(nh):
        ob[:, j * hd:(j + 1) * hd] = os[pl.ds(j, b, stride=nh), :].astype(BF16)

    def ostep(i, _):
        wo_copy(i).wait()
        c = pl.ds(pl.multiple_of(i * co, co), co)
        attn = jnp.dot(ob[...], wob[:, c], preferred_element_type=F32)
        hf[:, c] = (x[:, c].astype(F32) + attn).astype(BF16)
        return 0

    lax.fori_loop(0, nwo, ostep, 0)
    h = hf[...]
    h_out[...] = h
    u_out[...] = _rms(h, ln2[...])


def _attention(x, kv_k, kv_v, lens, idx, gates, ln1, ln2, wq, wo):
    b, d = x.shape
    _, l, kvh, hd = kv_k.shape
    hdim = wq.shape[1]
    nh = hdim // hd
    rows = l * kvh
    kk = kv_k.reshape(b, rows, hd)
    vv = kv_v.reshape(b, rows, hd)
    return pl.pallas_call(
        _attn_kernel,
        name="attn",
        out_shape=(pltpu.VMEM((b, d), BF16), pltpu.VMEM((b, d), BF16), pltpu.VMEM((2 * idx.shape[1], 128), F32)),
        in_specs=[_sm(), _vm(), _vm(), _vm(), _vm(), _vm(), _any(), _any(), _any(), _any()],
        out_specs=(_vm(), _vm(), _vm()),
        scratch_shapes=[
            pltpu.VMEM((d, hdim), BF16),
            pltpu.VMEM((hdim, d), BF16),
            pltpu.VMEM((KVBUF, SEQ, rows, hd), BF16),
            pltpu.VMEM((KVBUF, SEQ, rows, hd), BF16),
            pltpu.VMEM((b * nh, hd), F32),
            pltpu.VMEM((b * nh, hd), F32),
            pltpu.VMEM((b, hdim), BF16),
            pltpu.VMEM((nh, rows), F32),
            pltpu.VMEM((b, d), BF16),
            pltpu.VMEM((SEQ * nh, rows), F32),
            pltpu.VMEM((SEQ * nh, rows), BF16),
            pltpu.SemaphoreType.DMA((8,)),
            pltpu.SemaphoreType.DMA((8,)),
            pltpu.SemaphoreType.DMA((KVBUF,)),
            pltpu.SemaphoreType.DMA((KVBUF,)),
        ],
        compiler_params=pltpu.CompilerParams(vmem_limit_bytes=VLIM),
    )(lens, x, ln1, ln2, idx.T, gates.T, kk, vv, wq, wo)


def _places():
    cy = lax.axis_index("ey")
    cx = lax.axis_index("ex")
    xn = cy + 1 - 2 * lax.rem(cy, 2)
    yn = lax.rem(cy + 2, 4)
    dg = 3 - cy
    return cy, cx, (xn, yn, dg)


def _barrier(cy, cx, others):
    bar = pltpu.get_barrier_semaphore()
    for o in others:
        pl.semaphore_signal(bar, inc=1, device_id=(o, cx), device_id_type=MESH)
    pl.semaphore_signal(bar, inc=1, device_id=(cy, 1 - cx), device_id_type=MESH)
    pl.semaphore_wait(bar, len(others) + 1)


WBUF = 4
TILE = 128
WIDE = 256
SMALL = 64
LANES = 16
PITCH = 17
STEP8 = 8


def _silu_mul(z1, z3):
    return (z1 * jax.nn.sigmoid(z1) * z3).astype(BF16)


def _slot_copies(w1, w3, w2, b1, b3, b2, sem, e, slot):
    return (pltpu.make_async_copy(w1.at[e], b1.at[slot], sem.at[0, slot]),
            pltpu.make_async_copy(w3.at[e], b3.at[slot], sem.at[1, slot]),
            pltpu.make_async_copy(w2.at[e], b2.at[slot], sem.at[2, slot]))


def _gather_kernel(u, pk, w1, w3, w2, ua, toks, wgts, cols, b1, b3, b2,
                   pka, tmap, ps_sem, pr_sem, s_sem, r_sem, fs_sem, fr_sem, os_sem, or_sem, w_sem):
    blk, d = u.shape
    ntok = 8 * blk
    ne = w1.shape[0]
    top = 8
    cap = blk - blk // 8
    half = blk // 2
    cy, cx, others = _places()
    xn, yn, dg = others
    me = 2 * cy + cx

    ahead = [_slot_copies(w1, w3, w2, b1, b3, b2, w_sem, e, e) for e in range(WBUF)]
    for cs in ahead:
        for c in cs:
            c.start()

    _barrier(cy, cx, others)

    def table(src, slot, dev, i):
        return pltpu.make_async_remote_copy(
            src_ref=src, dst_ref=pka.at[slot], send_sem=ps_sem.at[i], recv_sem=pr_sem.at[i],
            device_id=dev, device_id_type=MESH)

    def rows(k):
        return pl.ds(k * half, half)

    def part(src, slot, k, dev, ss, rs, i):
        return pltpu.make_async_remote_copy(
            src_ref=src, dst_ref=ua.at[slot, rows(k)], send_sem=ss.at[i, k], recv_sem=rs.at[i, k],
            device_id=dev, device_id_type=MESH)

    partner = (cy, 1 - cx)
    for i in range(3):
        table(pk, me, (others[i], cx), i).start()
    table(pk, me, partner, 3).start()
    direct = [(1, 0), (0, 1), (1, 1), (0, 0)]
    for i, k in direct:
        part(u.at[rows(k)], me, k, (others[i], cx), s_sem, r_sem, i).start()
    for k in range(2):
        part(u.at[rows(k)], me, k, partner, os_sem, or_sem, 0).start()
    ua[me] = u[...]
    pka[me] = pk[...]

    for i in range(3):
        slot = 2 * others[i] + cx
        table(pk, slot, (others[i], cx), i).wait_recv()
        table(pka.at[slot], slot, partner, 4 + i).start()
    def tables():
        tmap[...] = jnp.concatenate([pka[k, :, 0:blk] for k in range(8)], axis=1)
        ids = (me * ne + lax.broadcasted_iota(jnp.int32, (ne, ntok), 0)).astype(F32)
        member = jnp.zeros((ne, ntok), F32)
        gate = jnp.zeros((ne, ntok), F32)
        for j in range(top):
            hit = tmap[j:j + 1, :] == ids
            member = member + jnp.where(hit, 1.0, 0.0)
            gate = gate + jnp.where(hit, tmap[top + j:top + j + 1, :], 0.0)
        ti = lax.broadcasted_iota(jnp.int32, (ntok, ntok), 0)
        tj = lax.broadcasted_iota(jnp.int32, (ntok, ntok), 1)
        tri = ti < tj
        tri_b = (tri & (ti // blk == tj // blk)).astype(F32).astype(BF16)
        rank = jnp.dot(member.astype(BF16), tri_b, preferred_element_type=F32)
        keep = jnp.where(rank < cap, member, 0.0)
        pos = jnp.dot(keep.astype(BF16), tri.astype(F32).astype(BF16), preferred_element_type=F32)
        pkeep = jnp.where(keep > 0, pos, -1.0)
        gkeep = gate * keep
        both = jnp.concatenate([gkeep, jnp.zeros((128 - ne, ntok), F32)], axis=0)
        cols[...] = jnp.transpose(both)
        place = lax.broadcasted_iota(jnp.int32, (SMALL, ntok), 0).astype(F32)
        tok = lax.broadcasted_iota(jnp.int32, (SMALL, ntok), 1).astype(F32) - ntok
        lane = lax.broadcasted_iota(jnp.int32, (SMALL, 128), 1)
        lists = jnp.zeros((SMALL, 128), F32)
        for e in range(ne):
            hit = pkeep[e:e + 1, :] == place
            t = jnp.sum(jnp.where(hit, tok, 0.0), axis=1, keepdims=True)
            g = jnp.sum(jnp.where(hit, gkeep[e:e + 1, :], 0.0), axis=1, keepdims=True)
            lists = lists + jnp.where(lane == e, t, 0.0) + jnp.where(lane == ne + e, g, 0.0)
        lists = jnp.transpose(jnp.concatenate([lists, jnp.zeros((128 - SMALL, 128), F32)], axis=0))
        count = jnp.sum(keep, axis=1, keepdims=True)
        last = lax.broadcasted_iota(jnp.int32, (ne, 128), 1) == 127
        toks[...] = jnp.where(last, count, lists[0:ne, :] + ntok).astype(jnp.int32)
        wgts[...] = lists[ne:2 * ne, :]

    def take(slot, k, dev, i):
        part(u.at[rows(k)], slot, k, dev, s_sem, r_sem, i).wait_recv()
        part(ua.at[slot, rows(k)], slot, k, partner, fs_sem, fr_sem, i).start()

    sx, sy, sd = 2 * xn + cx, 2 * yn + cx, 2 * dg + cx
    relay = {0: (sy, xn), 1: (sx, yn)}

    def across(k):
        slot, dev = relay[k]
        return part(ua.at[slot, rows(k)], slot, k, (dev, cx), s_sem, r_sem, 2)

    take(sy, 0, (yn, cx), 1)
    across(0).start()
    take(sx, 1, (xn, cx), 0)
    across(1).start()
    for i in range(3):
        slot = 2 * others[i] + cx
        table(pka.at[slot], slot, partner, 4 + i).wait()
        table(pk, me, (others[i], cx), i).wait_send()
    table(pk, me, partner, 3).wait()
    tables()
    take(sy, 1, (yn, cx), 1)
    take(sx, 0, (xn, cx), 0)
    for k in range(2):
        take(sd, k, (dg, cx), 2)
    for i, slot in ((1, sy), (0, sx), (2, sd)):
        for k in range(2):
            part(ua.at[slot, rows(k)], slot, k, partner, fs_sem, fr_sem, i).wait()
    for k in range(2):
        part(u.at[rows(k)], me, k, partner, os_sem, or_sem, 0).wait()
        across(k).wait_send()
        for i in range(2):
            part(u.at[rows(k)], me, k, (others[i], cx), s_sem, r_sem, i).wait_send()
    for cs in ahead:
        for c in cs:
            c.wait()


def _all_gather(u, pk, w1, w3, w2):
    b, d = u.shape
    ne, _, f = w1.shape
    return pl.pallas_call(
        _gather_kernel,
        name="gather",
        out_shape=(pltpu.VMEM((8, b, d), BF16),
                   jax.ShapeDtypeStruct((ne, 128), jnp.int32),
                   jax.ShapeDtypeStruct((ne, 128), F32),
                   pltpu.VMEM((8 * b, 128), F32),
                   pltpu.VMEM((WBUF, d, f), BF16),
                   pltpu.VMEM((WBUF, d, f), BF16),
                   pltpu.VMEM((WBUF, f, d), BF16)),
        in_specs=[_vm(), _vm()] + [_hbm()] * 3,
        out_specs=(_vm(),) * 7,
        scratch_shapes=[
            pltpu.VMEM((8, pk.shape[0], 128), F32),
            pltpu.VMEM((pk.shape[0], 8 * b), F32),
            pltpu.SemaphoreType.DMA((7,)),
            pltpu.SemaphoreType.DMA((7,)),
            pltpu.SemaphoreType.DMA((3, 2)),
            pltpu.SemaphoreType.DMA((3, 2)),
            pltpu.SemaphoreType.DMA((3, 2)),
            pltpu.SemaphoreType.DMA((3, 2)),
            pltpu.SemaphoreType.DMA((1, 2)),
            pltpu.SemaphoreType.DMA((1, 2)),
            pltpu.SemaphoreType.DMA((3, WBUF)),
        ],
        compiler_params=pltpu.CompilerParams(
            collective_id=0, has_side_effects=True, vmem_limit_bytes=4 * 1024 * 1024),
    )(u, pk, w1, w3, w2)


def _expert_kernel(toks, wgts, ua, cols, b1, b3, b2, w1, w3, w2, acc, o1, o3, o2,
                   ua3, x3, r3, xt, gt, gsc, order, seat, sem):
    del o1, o3, o2
    ntok, d = ua.shape
    ne = w1.shape[0]
    f = w1.shape[2]
    fc = 256
    dc = 512

    def copies(e, slot):
        return _slot_copies(w1, w3, w2, b1, b3, b2, sem, e, slot)

    spread = [5, 9, 12, 7, 10, 4, 6, 8, 11, 13, 14, 15]
    for k in range(ne - WBUF):
        seat[k] = spread[k]
    for e in range(ne):
        if e < WBUF:
            order[e] = e
        else:
            rank = jnp.int32(0)
            for o in range(WBUF, ne):
                if o != e:
                    ahead = toks[o, 127] >= toks[e, 127] if o < e else toks[o, 127] > toks[e, 127]
                    rank = rank + ahead.astype(jnp.int32)
            order[seat[rank]] = e

    for c in range(LANES):
        ua3[pl.ds(c, ntok, stride=PITCH), :] = ua[:, c * 128:(c + 1) * 128].astype(F32)
    ua3[ntok * PITCH:, :] = jnp.zeros((STEP8 * PITCH, 128), F32)

    def zero(i, _):
        acc[pl.ds(pl.multiple_of(i * 256, 256), 256), :] = jnp.zeros((256, 128), F32)
        return 0
    lax.fori_loop(0, ntok * LANES // 256, zero, 0)
    acc[ntok * LANES:, :] = jnp.zeros((STEP8 * LANES, 128), F32)

    def hidden(slot, m, x):
        for c in range(f // fc):
            s = slice(c * fc, (c + 1) * fc)
            z1 = jnp.dot(x(), b1[slot, :, s], preferred_element_type=F32)
            z3 = jnp.dot(x(), b3[slot, :, s], preferred_element_type=F32)
            gt[0:m, s] = _silu_mul(z1, z3)

    def results(slot, m, at0):
        for c in range(d // dc):
            y = jnp.dot(gt[at0:at0 + m, :], b2[slot, :, c * dc:(c + 1) * dc], preferred_element_type=F32)
            y = y.astype(BF16).astype(F32)
            for j in range(dc // 128):
                r3[pl.ds(c * (dc // 128) + j, m, stride=PITCH), :] = y[:, j * 128:(j + 1) * 128]

    def at(t):
        return pl.ds(pl.multiple_of(t * LANES, LANES), LANES)

    def wide(t):
        return pl.ds(t * PITCH, LANES)

    def expert(step, _):
        slot = lax.rem(step, WBUF)
        e = order[step]

        @pl.when(step >= WBUF)
        def _():
            for c in copies(e, slot):
                c.wait()
        n = toks[e, 127]

        def small(size):
            steps = (n + STEP8 - 1) // STEP8

            def fetch(i, _):
                for k in range(STEP8):
                    m = i * STEP8 + k
                    x3[wide(m), :] = ua3[wide(toks[e, m]), :]
                return 0
            lax.fori_loop(0, steps, fetch, 0)
            for c in range(LANES):
                xt[0:size, c * 128:(c + 1) * 128] = x3[pl.ds(c, size, stride=PITCH), :].astype(BF16)
            hidden(slot, size, lambda: xt[0:size, :])
            results(slot, size, 0)

            def add(i, _):
                where = [at(toks[e, i * STEP8 + k]) for k in range(STEP8)]
                new = [acc[where[k], :] + wgts[e, i * STEP8 + k] * r3[wide(i * STEP8 + k), :] for k in range(STEP8)]
                for k in range(STEP8):
                    acc[where[k], :] = new[k]
                return 0
            lax.fori_loop(0, steps, add, 0)

        pl.when((n > 0) & (n <= SMALL // 2))(lambda: small(SMALL // 2))
        pl.when((n > SMALL // 2) & (n <= SMALL))(lambda: small(SMALL))

        @pl.when(n > SMALL)
        def _():
            lane = lax.broadcasted_iota(jnp.int32, (ntok, 128), 1)
            gsc[...] = jnp.broadcast_to(
                jnp.sum(jnp.where(lane == e, cols[...], 0.0), axis=1, keepdims=True), (ntok, 128))

            def dense(t, _):
                rows = pl.ds(pl.multiple_of(t * WIDE, WIDE), WIDE)
                hidden(slot, WIDE, lambda: ua[rows, :])
                for part in range(WIDE // TILE):
                    results(slot, TILE, part * TILE)

                    def add(i, _):
                        for k in range(STEP8):
                            m = i * STEP8 + k
                            one = at(t * WIDE + part * TILE + m)
                            g = gsc[pl.ds(t * WIDE + part * TILE + m, 1), :]
                            acc[one, :] = acc[one, :] + g * r3[wide(m), :]
                        return 0
                    lax.fori_loop(0, TILE // STEP8, add, 0)
                return 0
            lax.fori_loop(0, ntok // WIDE, dense, 0)

        @pl.when(step + WBUF < ne)
        def _():
            for c in copies(order[step + WBUF], slot):
                c.start()
        return 0

    lax.fori_loop(0, ne, expert, 0)


def _experts(toks, wgts, ua, cols, i1, i3, i2, w1, w3, w2):
    ntok, d = ua.shape
    ne, _, f = w1.shape
    return pl.pallas_call(
        _expert_kernel,
        name="experts",
        out_shape=(pltpu.VMEM(((ntok + STEP8) * LANES, 128), F32),
                   pltpu.VMEM((WBUF, d, f), BF16),
                   pltpu.VMEM((WBUF, d, f), BF16),
                   pltpu.VMEM((WBUF, f, d), BF16)),
        in_specs=[_sm()] * 2 + [_vm()] * 5 + [_hbm()] * 3,
        out_specs=(_vm(),) * 4,
        input_output_aliases={4: 1, 5: 2, 6: 3},
        scratch_shapes=[
            pltpu.VMEM(((ntok + STEP8) * PITCH, 128), F32),
            pltpu.VMEM((SMALL * PITCH, 128), F32),
            pltpu.VMEM((TILE * PITCH, 128), F32),
            pltpu.VMEM((SMALL, d), BF16),
            pltpu.VMEM((WIDE, f), BF16),
            pltpu.VMEM((ntok, 128), F32),
            pltpu.SMEM((ne,), jnp.int32),
            pltpu.SMEM((ne,), jnp.int32),
            pltpu.SemaphoreType.DMA((3, WBUF)),
        ],
        compiler_params=pltpu.CompilerParams(vmem_limit_bytes=9 * 1024 * 1024),
    )(toks, wgts, ua, cols, i1, i3, i2, w1, w3, w2)[0]


CH = 4


def _return_kernel(acc, h, u, ws1, ws3, ws2, y, rbuf, sbuf, abuf, tbuf, zbuf, tot, hs, gt, v1, v3, v2,
                   ds_sem, dr_sem, s_sem, r_sem, ts_sem, tr_sem, v_sem):
    cy, cx, others = _places()
    xn, yn, dg = others
    b, d = h.shape
    f = gt.shape[1]
    per = b // CH
    w = per * LANES
    n1 = xn * (1 - cx) + yn * cx
    n2 = yn * (1 - cx) + xn * cx

    shared = (pltpu.make_async_copy(ws1, v1, v_sem.at[0]),
              pltpu.make_async_copy(ws3, v3, v_sem.at[1]),
              pltpu.make_async_copy(ws2, v2, v_sem.at[2]))
    for c in shared:
        c.start()
    _barrier(cy, cx, others)

    def piece(k, core, c):
        return pl.ds((2 * k + core) * (b * LANES) + c * w, w)

    def pair(c, k):
        return pltpu.make_async_remote_copy(
            src_ref=acc.at[piece(k, 1 - cx, c)], dst_ref=rbuf.at[c, k],
            send_sem=ds_sem.at[c, k], recv_sem=dr_sem.at[c, k],
            device_id=(cy, 1 - cx), device_id_type=MESH)

    def first(c, i):
        return pltpu.make_async_remote_copy(
            src_ref=sbuf.at[c, dg if i else n1], dst_ref=abuf.at[c, i],
            send_sem=s_sem.at[c, i], recv_sem=r_sem.at[c, i],
            device_id=(n1, cx), device_id_type=MESH)

    def second(c):
        return pltpu.make_async_remote_copy(
            src_ref=tbuf.at[c], dst_ref=zbuf.at[c], send_sem=ts_sem.at[c], recv_sem=tr_sem.at[c],
            device_id=(n2, cx), device_id_type=MESH)

    for c in range(CH):
        for k in range(4):
            pair(c, k).start()
    for c in range(CH):
        for k in range(4):
            pair(c, k).wait_recv()
            sbuf[c, k] = acc[piece(k, cx, c), :] + rbuf[c, k]
        for i in (1, 0):
            first(c, i).start()

    for c in shared:
        c.wait()
    for c in range(f // 256):
        s = slice(c * 256, (c + 1) * 256)
        z1 = jnp.dot(u[...], v1[:, s], preferred_element_type=F32)
        z3 = jnp.dot(u[...], v3[:, s], preferred_element_type=F32)
        gt[:, s] = _silu_mul(z1, z3)
    for c in range(d // 512):
        s = slice(c * 512, (c + 1) * 512)
        hs[:, s] = h[:, s].astype(F32) + jnp.dot(gt[...], v2[:, s], preferred_element_type=F32)

    for c in range(CH):
        first(c, 1).wait_recv()
        tbuf[c] = sbuf[c, n2] + abuf[c, 1]
        second(c).start()
    for c in range(CH):
        first(c, 0).wait_recv()
        second(c).wait_recv()
        tot[...] = sbuf[c, cy] + (abuf[c, 0] + zbuf[c])
        r = slice(c * per, (c + 1) * per)
        for j in range(LANES):
            s = slice(j * 128, (j + 1) * 128)
            y[r, s] = (hs[r, s] + tot[pl.ds(j, per, stride=LANES), :]).astype(BF16)
    for c in range(CH):
        for k in range(4):
            pair(c, k).wait_send()
        for i in range(2):
            first(c, i).wait_send()
        second(c).wait_send()


def _return(acc, h, u, ws1, ws3, ws2):
    b, d = h.shape
    f = ws1.shape[1]
    w = b // CH * LANES
    return pl.pallas_call(
        _return_kernel,
        name="giveback",
        out_shape=jax.ShapeDtypeStruct((b, d), BF16),
        in_specs=[_vm()] * 3 + [_hbm()] * 3,
        out_specs=_vm(),
        scratch_shapes=[
            pltpu.VMEM((CH, 4, w, 128), F32),
            pltpu.VMEM((CH, 4, w, 128), F32),
            pltpu.VMEM((CH, 2, w, 128), F32),
            pltpu.VMEM((CH, w, 128), F32),
            pltpu.VMEM((CH, w, 128), F32),
            pltpu.VMEM((w, 128), F32),
            pltpu.VMEM((b, d), F32),
            pltpu.VMEM((b, f), BF16),
            pltpu.VMEM((d, f), BF16),
            pltpu.VMEM((d, f), BF16),
            pltpu.VMEM((f, d), BF16),
            pltpu.SemaphoreType.DMA((CH, 4)),
            pltpu.SemaphoreType.DMA((CH, 4)),
            pltpu.SemaphoreType.DMA((CH, 2)),
            pltpu.SemaphoreType.DMA((CH, 2)),
            pltpu.SemaphoreType.DMA((CH,)),
            pltpu.SemaphoreType.DMA((CH,)),
            pltpu.SemaphoreType.DMA((3,)),
        ],
        compiler_params=pltpu.CompilerParams(
            collective_id=1, has_side_effects=True, vmem_limit_bytes=20 * 1024 * 1024),
    )(acc, h, u, ws1, ws3, ws2)


def solution(mesh):
    def body(x, kv_k, kv_v, lens, idx, gates, ln1, wq, wo, ln2, ws1, ws3, ws2, w1, w3, w2):
        b, d = x.shape
        h, u, pk = _attention(x, kv_k, kv_v, lens, idx, gates, ln1, ln2, wq, wo)
        ua, toks, wgts, cols, b1, b3, b2 = _all_gather(u, pk, w1, w3, w2)
        acc = _experts(toks, wgts, ua.reshape(8 * b, d), cols, b1, b3, b2, w1, w3, w2)
        return _return(acc, h, u, ws1, ws3, ws2)

    rows = P(GRP)
    rep = P()
    return jax.shard_map(
        body, mesh=mesh,
        in_specs=(rows, rows, rows, rows, rows, rows, rep, rep, rep, rep, rep, rep, rep, rows, rows, rows),
        out_specs=rows, check_vma=False)
```
